128 devices in a mesh: dp: 8 (over z, core), cp: 16 (over x, y).
Axes of the slice: x: 4, y: 4, z: 4, core: 2. Of those that a mesh axis runs over, the one named last changes fastest.
Arguments:
- row_owner: int32 [16384, 1], P(('dp', 'cp')), may hold values from 0 to 127; in each aligned block of 128 rows (0 to 127, 128 to 255, ...) at most 4 rows name the same one
- slot_row: int32 [16384], P(('dp', 'cp')), may hold values from 0 to 2559
- hot_table: bfloat16 [65536, 512], P(('dp', 'cp')), may hold values from -6 to 6
- cold_table: bfloat16 [262144, 128], P(('dp', 'cp')), may hold values from -6 to 6
- cold_projection: bfloat16 [128, 512], replicated, may hold values from -0.5 to 0.5
- joined_weight: bfloat16 [512, 2048], replicated, may hold values from -0.25 to 0.25
- output_weight: bfloat16 [512, 512], replicated, may hold values from -0.25 to 0.25
- cotangent: bfloat16 [16384, 512], P(('dp', 'cp')), may hold values from -6 to 6
Outputs:
- layer_out: bfloat16 [16384, 512], P(('dp', 'cp'))
- hot_gradient: float32 [65536, 512], P(('dp', 'cp'))
- cold_gradient: float32 [262144, 128], P(('dp', 'cp'))
- projection_gradient: float32 [128, 512], replicated
- joined_gradient: float32 [512, 2048], replicated
- output_gradient: float32 [512, 512], replicated
The draws below stay inside these ranges and needn't reach their ends.
Inputs may be any that keep to these rules, and one draw needn't show every extreme that they name: `row_owner`: in each aligned block of 128 rows (the rows of one device) no owner is named by more than 4 rows.
All inputs are finite; a program needn't handle non-finite values.
Results may differ from the reference program's by a relative error of at most 0.013.
Values may be sent and summed in bfloat16 or wider, within the bound.
A program may use at most 128 MiB of HBM per device.

```python
import math
import jax
import jax.numpy as jnp
import numpy as np
from jax import lax

D = 512
HEADS = 8
HEAD = 64
COLD_W = 128
TOK_DEV = 128
HOT_DEV = 512
COLD_DEV = 2048
LENGTH = 2048
TOKENS = 16384
CAP = 4
HOT_ALL = 65536
COLD_ALL = 262144
N_DP = 8
DEVICES = 128


def touch_ends(values, rng, least, top_value):
    longest = values.shape.index(max(values.shape))
    spots = []
    for shift in (0, 1):
        where = [jax.random.randint(jax.random.fold_in(rng, axis), (), 0, length) for axis, length in enumerate(values.shape)]
        where[longest] = (where[longest] + shift) % values.shape[longest]
        spots.append(tuple(where))
    return values.at[spots[0]].set(least).at[spots[1]].set(top_value)


def steps_of(own_key, extent, pieces, low, high):
    def one(axis_at, parts):
        draws = jax.random.uniform(jax.random.fold_in(jax.random.fold_in(own_key, 6), axis_at), (parts,), jnp.float32, low / len(pieces), high / len(pieces))
        return jnp.repeat(jnp.exp(draws), extent[axis_at] // parts).reshape((-1,) + (1,) * (len(extent) - axis_at - 1))

    gain = one(*pieces[0])
    for cut in pieces[1:]:
        gain = gain * one(*cut)
    return gain


def deal_out(stream_key, own, number, rows, amount, top, bound, skew):
    ranking = jax.random.permutation(stream_key, amount)
    heavy_load, common = shares(amount, rows * top, bound, skew, True), shares(amount, rows * top, bound, skew, False)
    places = jnp.arange(amount)

    def named(tallies, rotation):
        used = int((tallies > 0).sum())
        fixed = max(1, used // 4)
        passed = fixed + (places - fixed + rotation * (used - fixed)) % max(1, amount - fixed)
        return jnp.zeros((amount,), jnp.int32).at[ranking[jnp.where(places < fixed, places, passed)]].set(jnp.asarray(tallies, jnp.int32))

    tallies = jnp.where(number % 4 == 0, named(heavy_load, number // 4), named(common, number - number // 4 - 1))
    mixed = jax.random.permutation(jax.random.fold_in(own, 3), amount)
    donor, receiver = mixed[0:amount // 2 * 2:2], mixed[1:amount // 2 * 2:2]
    room = jnp.minimum(tallies[donor] - 1, bound - tallies[receiver]) // 2
    room = jnp.where((donor == ranking[0]) | (receiver == ranking[0]) | (tallies[receiver] == 0), 0, jnp.maximum(room, 0))
    passed = jax.random.randint(jax.random.fold_in(own, 4), (amount // 2,), 0, 1 << 20) % (room + 1)
    tallies = tallies.at[donor].add(-passed).at[receiver].add(passed)
    labels = jnp.searchsorted(jnp.cumsum(tallies), jnp.arange(rows * top), side="right").astype(jnp.int32)
    listing = labels.reshape(top, rows).T
    listing = listing[jax.random.permutation(jax.random.fold_in(own, 1), rows)]
    rotation = jax.random.randint(jax.random.fold_in(own, 2), (rows, 1), 0, top)
    return jnp.take_along_axis(listing, (jnp.arange(top)[None, :] + rotation) % top, axis=1)


def shares(count, total, bound, lean, full):
    portions = [(1 << 20) // math.isqrt(rank ** lean) + 1 for rank in range(1, count + 1)]
    largest = bound if full else min(bound, max(-(-total // count), total * portions[0] // sum(portions)))
    least = 1 if total - largest >= count - 1 else 0
    holding, spare = [largest] + [least] * (count - 1), total - largest - least * (count - 1)
    while spare > 0:
        free = [i for i in range(1, count) if holding[i] < largest] or [i for i in range(1, count) if holding[i] < bound]
        whole, remaining = sum([portions[i] for i in free]), spare
        for i in free:
            more = min(bound - holding[i], max(1, remaining * portions[i] // whole), spare)
            holding[i] = holding[i] + more
            spare = spare - more
    return np.array(holding)


def normal_values(stream_key, dims, width, bound, split=(), kind=jnp.bfloat16):
    values = width * jax.random.normal(stream_key, dims, jnp.float32)
    if split:
        values = values * steps_of(stream_key, dims, split, -0.22, 0.18)
    return jnp.clip(values, -bound, bound).astype(kind)


def setup_inputs(seed: int = 0) -> dict:
    key_list = jax.random.split(jax.random.key(seed), 9)
    row_owner_keys = jax.random.split(jax.random.fold_in(key_list[0], 1), TOKENS // TOK_DEV)
    row_owner_turns = jax.random.permutation(jax.random.fold_in(key_list[0], 3), TOKENS // TOK_DEV)
    row_owner = jax.vmap(lambda own, number: deal_out(jax.random.fold_in(key_list[0], 2), own, number, TOK_DEV, DEVICES, 1, CAP, 2))(row_owner_keys, row_owner_turns).reshape((TOKENS, 1))
    slot_row = touch_ends(jax.random.randint(key_list[1], (TOKENS,), 0, HOT_DEV + COLD_DEV), jax.random.fold_in(key_list[1], 1), 0, (HOT_DEV + COLD_DEV) - 1).astype(jnp.int32)
    hot_table = normal_values(key_list[2], (HOT_ALL, D), 1.0, 6.0, ((0, 128),))
    cold_table = normal_values(key_list[3], (COLD_ALL, COLD_W), 1.0, 6.0, ((0, 128),))
    cold_projection = normal_values(key_list[4], (COLD_W, D), COLD_W ** -0.5, 0.5)
    joined_weight = normal_values(key_list[5], (D, 4 * D), D ** -0.5, 0.25)
    output_weight = normal_values(key_list[6], (D, D), D ** -0.5, 0.25)
    cotangent = normal_values(key_list[7], (TOKENS, D), 1.0, 6.0, ((0, 128),))
    return {"row_owner": row_owner, "slot_row": slot_row, "hot_table": hot_table, "cold_table": cold_table, "cold_projection": cold_projection, "joined_weight": joined_weight, "output_weight": output_weight, "cotangent": cotangent}


EPSILON = 1e-05

def silu_slope(values):
    sigmoid_v = jax.nn.sigmoid(values)
    return sigmoid_v * (1.0 + values * (1.0 - sigmoid_v))

def layer_normalize(values):
    average = lax.optimization_barrier(jnp.mean(values, axis=-1, keepdims=True))
    centred = values - average
    inverse = lax.rsqrt(lax.optimization_barrier(jnp.mean(centred * centred, axis=-1, keepdims=True)) + EPSILON)
    return (centred * inverse, inverse)

def normalize_back(gradient, normed, inverse):
    first_term = lax.optimization_barrier(jnp.mean(gradient, axis=-1, keepdims=True))
    second_term = lax.optimization_barrier(jnp.mean(gradient * normed, axis=-1, keepdims=True))
    return (gradient - first_term - normed * second_term) * inverse

def rounded_float(values):
    return lax.optimization_barrier(values.astype(jnp.bfloat16)).astype(jnp.float32)

def sequence_forward(query_heads, key_heads, value_heads):
    block_rows = min(LENGTH, 512)
    score_scale = 1.0 / math.sqrt(HEAD)
    key_index = jnp.arange(LENGTH, dtype=jnp.int32)
    key_float = key_heads.astype(jnp.float32)
    value_float = value_heads.astype(jnp.float32)

    def one_block(counter):
        offset = counter * block_rows
        query_block = lax.dynamic_slice_in_dim(query_heads, offset, block_rows, 0).astype(jnp.float32)
        scores = jnp.einsum('qhd,khd->hqk', query_block, key_float) * score_scale
        query_index = offset + jnp.arange(block_rows, dtype=jnp.int32)
        allowed = (key_index[None, :] <= query_index[:, None])[None]
        weights = rounded_float(jnp.where(allowed, jax.nn.silu(scores), 0.0))
        return jnp.einsum('hqk,khd->qhd', weights, value_float)
    result = lax.map(one_block, jnp.arange(LENGTH // block_rows, dtype=jnp.int32))
    return result.reshape(LENGTH, HEADS * HEAD)

def sequence_backward(query_heads, key_heads, value_heads, delta_heads):
    block_rows = min(LENGTH, 512)
    score_scale = 1.0 / math.sqrt(HEAD)
    key_index = jnp.arange(LENGTH, dtype=jnp.int32)
    key_float = key_heads.astype(jnp.float32)
    value_float = value_heads.astype(jnp.float32)

    def one_block(carried, counter):
        key_sum, value_sum = carried
        offset = counter * block_rows
        query_block = lax.dynamic_slice_in_dim(query_heads, offset, block_rows, 0).astype(jnp.float32)
        delta_block = lax.dynamic_slice_in_dim(delta_heads, offset, block_rows, 0).astype(jnp.float32)
        scores = jnp.einsum('qhd,khd->hqk', query_block, key_float) * score_scale
        query_index = offset + jnp.arange(block_rows, dtype=jnp.int32)
        allowed = (key_index[None, :] <= query_index[:, None])[None]
        weights = rounded_float(jnp.where(allowed, jax.nn.silu(scores), 0.0))
        delta_weights = jnp.einsum('qhd,khd->hqk', delta_block, value_float)
        delta_scores = rounded_float(jnp.where(allowed, delta_weights * silu_slope(scores) * score_scale, 0.0))
        query_part = jnp.einsum('hqk,khd->qhd', delta_scores, key_float)
        key_sum = key_sum + jnp.einsum('hqk,qhd->khd', delta_scores, query_block)
        value_sum = value_sum + jnp.einsum('hqk,qhd->khd', weights, delta_block)
        return ((key_sum, value_sum), query_part)
    empty_heads = jnp.zeros((LENGTH, HEADS, HEAD), jnp.float32)
    (key_sum, value_sum), query_parts = lax.scan(one_block, (empty_heads, empty_heads), jnp.arange(LENGTH // block_rows, dtype=jnp.int32))
    return (query_parts.reshape(LENGTH, HEADS * HEAD), key_sum.reshape(LENGTH, HEADS * HEAD), value_sum.reshape(LENGTH, HEADS * HEAD))

def reference(row_owner, slot_row, hot_table, cold_table, cold_projection, joined_weight, output_weight, cotangent):
    owners = row_owner[:, 0]
    is_hot = slot_row < HOT_DEV
    is_cold = jnp.logical_not(is_hot)
    hot_index = jnp.where(is_hot, owners * HOT_DEV + slot_row, 0).astype(jnp.int32)
    cold_index = jnp.where(is_hot, 0, owners * COLD_DEV + slot_row - HOT_DEV).astype(jnp.int32)
    hot_rows = hot_table[hot_index]
    cold_rows = cold_table[cold_index]
    cold_embed = jnp.dot(cold_rows, cold_projection, preferred_element_type=jnp.float32)
    embedded = jnp.where(is_hot[:, None], hot_rows.astype(jnp.float32), cold_embed)
    normed, inverse = layer_normalize(embedded)
    normed_low = normed.astype(jnp.bfloat16)
    hidden = jnp.dot(normed_low, joined_weight, preferred_element_type=jnp.float32)
    active = jax.nn.silu(hidden).astype(jnp.bfloat16)
    gate_part = active[:, :D]
    shaped = active[:, D:].reshape(N_DP, LENGTH, 3, HEADS, HEAD)
    value_rows = shaped[:, :, 0]
    query_rows = shaped[:, :, 1]
    key_rows = shaped[:, :, 2]
    attended = lax.map(lambda items: sequence_forward(*items), (query_rows, key_rows, value_rows)).reshape(TOKENS, D)
    mixed, inverse_mix = layer_normalize(attended)
    gated = (mixed * gate_part.astype(jnp.float32)).astype(jnp.bfloat16)
    branch = jnp.dot(gated, output_weight, preferred_element_type=jnp.float32)
    layer_out = (embedded + branch).astype(jnp.bfloat16)
    delta_gated = jnp.dot(cotangent, output_weight.T, preferred_element_type=jnp.float32)
    delta_gate = delta_gated * mixed
    delta_attended = normalize_back(delta_gated * gate_part.astype(jnp.float32), mixed, inverse_mix).astype(jnp.bfloat16)
    delta_heads = delta_attended.reshape(N_DP, LENGTH, HEADS, HEAD)
    delta_query, delta_key, delta_value = lax.map(lambda items: sequence_backward(*items), (query_rows, key_rows, value_rows, delta_heads))
    delta_active = jnp.concatenate([delta_gate, delta_value.reshape(TOKENS, D), delta_query.reshape(TOKENS, D), delta_key.reshape(TOKENS, D)], axis=1)
    delta_hidden = (delta_active * silu_slope(hidden)).astype(jnp.bfloat16)
    delta_normed = jnp.dot(delta_hidden, joined_weight.T, preferred_element_type=jnp.float32)
    delta_embed = normalize_back(delta_normed, normed, inverse) + cotangent.astype(jnp.float32)
    hot_gradient = jnp.zeros((HOT_ALL, D), jnp.float32).at[hot_index].add(jnp.where(is_hot[:, None], delta_embed, 0.0))
    cold_event = jnp.dot(delta_embed, cold_projection.astype(jnp.float32).T, precision=lax.Precision.HIGHEST)
    cold_gradient = jnp.zeros((COLD_ALL, COLD_W), jnp.float32).at[cold_index].add(jnp.where(is_cold[:, None], cold_event, 0.0))
    norm_scale = TOKENS ** (-0.5)
    cold_float = jnp.where(is_cold[:, None], cold_rows.astype(jnp.float32), 0.0)
    projection_gradient = jnp.dot(cold_float.T, delta_embed, precision=lax.Precision.HIGHEST) * norm_scale
    joined_gradient = jnp.dot(normed_low.T, delta_hidden, preferred_element_type=jnp.float32) * norm_scale
    output_gradient = jnp.dot(gated.T, cotangent, preferred_element_type=jnp.float32) * norm_scale
    return (layer_out, hot_gradient, cold_gradient, projection_gradient, joined_gradient, output_gradient)
```

```python
import math

import jax
import jax.numpy as jnp
from jax import lax
from jax.experimental import pallas as pl
from jax.experimental.pallas import tpu as pltpu
from jax.sharding import PartitionSpec as P

MESH = pl.DeviceIdType.MESH
BF = jnp.bfloat16
F32 = jnp.float32
I32 = jnp.int32
EPSILON = 1e-05

D = 512
HEADS = 8
HEAD = 64
TOK = 128
CAP = 4
HOT = 512
COLD = 2048
COLD_W = 128
N_DP = 8
N_CP = 16
DEVICES = N_DP * N_CP
SLOT = 16
SLOTS = DEVICES * SLOT
SHIFT = 4096
CHUNK = 256
PAIRS = HEADS * (HEADS + 1) // 2
W_ROWS = 4 * D + D + COLD_W
HALF_ROWS = W_ROWS // 2
COLOR_ROWS = HALF_ROWS // 3
PART_ROWS = COLOR_ROWS // 4


def nn(a, b):
    return jnp.dot(a, b, preferred_element_type=F32)


def nt(a, b, precision=None):
    return lax.dot_general(
        a, b, (((1,), (1,)), ((), ())), preferred_element_type=F32, precision=precision
    )


def sigmoid(v):
    return 0.5 * jnp.tanh(0.5 * v) + 0.5


def silu_slope(v):
    sig = sigmoid(v)
    return sig + v * sig * (1.0 - sig)


def iota(shape, dim):
    return lax.broadcasted_iota(I32, shape, dim)


def turned(v):
    return v.astype(F32).T


def column_norm(v):
    average = jnp.mean(v, axis=0, keepdims=True)
    centred = v - average
    inverse = lax.rsqrt(jnp.mean(centred * centred, axis=0, keepdims=True) + EPSILON)
    return centred * inverse, inverse


def column_norm_back(g, y, inverse):
    first = jnp.mean(g, axis=0, keepdims=True)
    second = jnp.mean(g * y, axis=0, keepdims=True)
    return (g - first - y * second) * inverse


def step_kernel(
    code_col, code_row, hot, cold, proj, joined, wout, cot,
    layer_out, rows_out, req_out, sums_out,
    ids_all, pick32, pick16, row_in, emb_nat, normed_t, inv_ref, cold_t, joined_t,
    hidden_t, active_t, dgated_t, cot_t, slots_1h,
    k_in, v_in, q_in, w_keep, slope_keep, att_out, att_in, da_out, da_in,
    dq_acc, dq_out, dk_out, dv_out, dq_in, dk_in, dv_in, dh_t, pack_ref, grad_out, grad_in,
    rows_buf, w_ref, r0, u1, r1, u2, r2, r3, g2, total,
    send, recv, ar_send, ar_recv, out_sem,
):
    dp, cp = lax.axis_index("dp"), lax.axis_index("cp")
    me = dp * N_CP + cp
    z, core, x, y = dp // 2, dp % 2, cp // 4, cp % 4
    head = cp // 2
    half = ((cp + 1) // 2) % 2

    def far(k):
        pz, pc = (z + k // 32) % 4, (core + (k // 16) % 2) % 2
        px, py = (x + (k // 4) % 4) % 4, (y + k % 4) % 4
        return pz * 2 + pc, px * 4 + py

    def remote(src, dst, send_sem, recv_sem, to):
        return pltpu.make_async_remote_copy(
            src_ref=src, dst_ref=dst, send_sem=send_sem, recv_sem=recv_sem,
            device_id=to, device_id_type=MESH,
        )

    def wait_sent(ref, i):
        remote(ref, ref, send.at[i], recv.at[i], (dp, cp)).wait_send()

    def wait_got(ref, i):
        remote(ref, ref, send.at[i], recv.at[i], (dp, cp)).wait_recv()

    def rows64(h):
        return pl.ds(pl.multiple_of(h * HEAD, HEAD), HEAD)

    def tile(o):
        return pl.ds(pl.multiple_of(o * SLOT, SLOT), SLOT)

    barrier = pltpu.get_barrier_semaphore()

    def greet(k, carry):
        pl.semaphore_signal(barrier, inc=1, device_id=far(k), device_id_type=MESH)
        return carry

    lax.fori_loop(1, DEVICES, greet, 0)
    pl.semaphore_wait(barrier, DEVICES - 1)

    def send_ids(k, carry):
        remote(code_row, ids_all.at[me], send.at[0], recv.at[0], far(k)).start()
        return carry

    lax.fori_loop(1, DEVICES, send_ids, 0)
    ids_all[pl.ds(me, 1)] = code_row[...].reshape(1, 1, TOK)

    owner_col, slot_col = code_col[...] // SHIFT, code_col[...] % SHIFT
    owner_row, slot_row = code_row[...] // SHIFT, code_row[...] % SHIFT
    same = owner_col == owner_row
    before_row = same & (iota((TOK, TOK), 0) < iota((TOK, TOK), 1))
    rank_row = jnp.sum(jnp.where(before_row, 1, 0), axis=0, keepdims=True)
    before_col = same & (iota((TOK, TOK), 1) < iota((TOK, TOK), 0))
    rank_col = jnp.sum(
        jnp.where(before_col, 1.0, 0.0), axis=1, keepdims=True
    ).astype(I32)
    place_col = owner_col * SLOT + rank_col
    place_row = owner_row * SLOT + rank_row
    for f in range(4):
        slots_1h[:, f * TOK : (f + 1) * TOK] = jnp.where(
            iota((SLOTS, TOK), 0) == place_row + CAP * f, 1.0, 0.0
        ).astype(BF)
    for b in range(4):
        joined_t[b * D : (b + 1) * D, :] = turned(joined[:, b * D : (b + 1) * D]).astype(BF)
    cot_t[...] = turned(cot[...])
    dgated_t[...] = nn(wout[...], cot_t[...].astype(BF))

    wait_got(ids_all.at[pl.ds(0, DEVICES - 1)], 0)
    wait_sent(ids_all.at[pl.ds(0, DEVICES - 1)], 0)

    ids = ids_all[:, 0, :]
    asked = (ids // SHIFT) == me
    slot_plus = ((ids % SHIFT) + 1).astype(F32)
    upper = jnp.where(iota((TOK, TOK), 0) < iota((TOK, TOK), 1), 1.0, 0.0).astype(BF)
    earlier = nn(jnp.where(asked, 1.0, 0.0).astype(BF), upper)
    lane_hot = iota((DEVICES, HOT), 1).astype(F32) + 1.0
    lane_cold = iota((DEVICES, COLD), 1).astype(F32) + (HOT + 1.0)
    asks = []
    for c in range(CAP):
        ask = jnp.where(asked & (earlier == float(c)), slot_plus, 0.0)
        asks.append(ask)
        wanted = jnp.sum(ask, axis=1, keepdims=True)
        hot_rows = nn(jnp.where(lane_hot == wanted, 1.0, 0.0).astype(BF), hot[...])
        cold_rows = nn(jnp.where(lane_cold == wanted, 1.0, 0.0).astype(BF), cold[...])
        for f in range(4):
            piece = hot_rows[:, f * 128 : (f + 1) * 128]
            if f == 0:
                piece = piece + cold_rows
            pick32[pl.ds(CAP * f + c, DEVICES, stride=SLOT), :] = piece
    pick16[...] = pick32[...].astype(BF)

    def send_rows(k, carry):
        to = far(k)
        remote(
            pick16.at[tile(to[0] * N_CP + to[1])], row_in.at[tile(me)], send.at[1], recv.at[1], to
        ).start()
        return carry

    lax.fori_loop(1, DEVICES, send_rows, 0)
    row_in[tile(me), :] = pick16[tile(me), :]
    req_out[...] = jnp.zeros(req_out.shape, I32)
    for c in range(CAP):
        wanted_row = jnp.sum(asks[c].T, axis=0, keepdims=True)
        req_out[c : c + 1, :] = wanted_row.astype(I32) - 1

    wait_got(row_in.at[pl.ds(0, SLOTS - SLOT)], 1)
    wait_sent(row_in.at[pl.ds(0, SLOTS - SLOT)], 1)

    fetched = []
    for f in range(4):
        take = jnp.where(iota((TOK, SLOTS), 1) == place_col + CAP * f, 1.0, 0.0).astype(BF)
        fetched.append(nn(take, row_in[...]))
    cold_vec = fetched[0]
    cold_embed = nn(cold_vec.astype(BF), proj[...])
    hot_col = slot_col < HOT
    embedded = jnp.where(hot_col, jnp.concatenate(fetched, axis=1), cold_embed)
    emb_nat[...] = embedded
    cold_t[...] = jnp.where(slot_row < HOT, 0.0, cold_vec.T)
    normed, inverse = column_norm(embedded.T)
    normed_t[...] = normed
    inv_ref[...] = jnp.broadcast_to(inverse, inv_ref.shape)
    normed_low = normed.astype(BF)
    for b in (3, 1, 2, 0):
        hid = nn(joined_t[b * D : (b + 1) * D, :], normed_low)
        hidden_t[b * D : (b + 1) * D, :] = hid
        active_t[b * D : (b + 1) * D, :] = (hid * sigmoid(hid)).astype(BF)

    def k_rows(h):
        return pl.ds(pl.multiple_of(3 * D + h * HEAD, HEAD), HEAD)

    def v_rows(h):
        return pl.ds(pl.multiple_of(D + h * HEAD, HEAD), HEAD)

    def q_rows(h):
        return pl.ds(pl.multiple_of(2 * D + h * HEAD, HEAD), HEAD)

    def send_kv(j, carry):
        pcp = ((x + j // 4) % 4) * 4 + (y + j % 4) % 4
        remote(active_t.at[k_rows(pcp // 2)], k_in.at[cp], send.at[2], recv.at[2], (dp, pcp)).start()
        remote(active_t.at[v_rows(pcp // 2)], v_in.at[cp], send.at[3], recv.at[3], (dp, pcp)).start()
        return carry

    def same_half(d):
        h = (head + d) % HEADS
        return h, (dp, 2 * h + (half + h) % 2)

    def send_q(d, carry):
        h, to = same_half(d)
        remote(active_t.at[q_rows(h)], q_in.at[head], send.at[4], recv.at[4], to).start()
        return carry

    lax.fori_loop(1, N_CP, send_kv, 0)
    lax.fori_loop(1, HEADS, send_q, 0)
    k_in[pl.ds(cp, 1)] = active_t[k_rows(head), :].reshape(1, HEAD, TOK)
    v_in[pl.ds(cp, 1)] = active_t[v_rows(head), :].reshape(1, HEAD, TOK)
    q_in[pl.ds(head, 1)] = active_t[q_rows(head), :].reshape(1, HEAD, TOK)
    wait_got(k_in.at[pl.ds(0, N_CP - 1)], 2)
    wait_got(v_in.at[pl.ds(0, N_CP - 1)], 3)
    wait_got(q_in.at[pl.ds(0, HEADS - 1)], 4)

    def block_of(i):
        return 4 * (i // 2) + (half if i % 2 == 0 else 3 - half)

    def pair(ref, c):
        return jnp.concatenate([ref[2 * c], ref[2 * c + 1]], axis=1)

    for i in range(HEADS):
        q_nat = turned(q_in[i]).astype(BF)
        total_t = jnp.zeros((HEAD, TOK), F32)
        for c in range(i + 1):
            s = nn(q_nat, pair(k_in, c)) * (1.0 / math.sqrt(HEAD))
            sig = sigmoid(s)
            w = s * sig
            slope = (sig + w * (1.0 - sig)) * (1.0 / math.sqrt(HEAD))
            if c == i:
                ok = (iota((TOK, CHUNK), 1) + c * CHUNK) <= (
                    iota((TOK, CHUNK), 0) + block_of(i) * TOK
                )
                w = jnp.where(ok, w, 0.0)
                slope = jnp.where(ok, slope, 0.0)
            w = w.astype(BF)
            at = i * (i + 1) // 2 + c
            w_keep[at] = w
            slope_keep[at] = slope
            total_t = total_t + nt(pair(v_in, c), w)
        att_out[i] = total_t.astype(BF)

        @pl.when(head != i)
        def _():
            remote(
                att_out.at[i], att_in.at[rows64(head)], send.at[5], recv.at[5], (dp, block_of(i))
            ).start()

    att_in[rows64(head), :] = att_out[pl.ds(head, 1)].reshape(HEAD, TOK)
    wait_got(att_in.at[pl.ds(0, D - HEAD)], 5)

    mixed, inv_mix = column_norm(att_in[...].astype(F32))
    gate = active_t[0:D, :].astype(F32)
    gated = (mixed * gate).astype(BF)
    dgated = dgated_t[...]
    da = column_norm_back(dgated * gate, mixed, inv_mix).astype(BF)
    da_out[...] = da

    def send_da(d, carry):
        h, to = same_half(d)
        remote(da_out.at[rows64(h)], da_in.at[head], send.at[6], recv.at[6], to).start()
        return carry

    lax.fori_loop(1, HEADS, send_da, 0)
    da_in[pl.ds(head, 1)] = da_out[rows64(head), :].reshape(1, HEAD, TOK)

    low = normed_t[...].astype(BF)
    dh_gate = (dgated * mixed * silu_slope(hidden_t[0:D, :])).astype(BF)
    dh_t[0:D, :] = dh_gate
    w_ref[0:D, :] = nt(low, dh_gate).astype(BF)
    w_ref[4 * D : 5 * D, :] = nn(gated, cot[...]).astype(BF)
    branch = nn(turned(gated).astype(BF), wout[...])
    layer_out[...] = (emb_nat[...] + branch).astype(BF)

    wait_got(da_in.at[pl.ds(0, HEADS - 1)], 6)

    dq_acc[...] = jnp.zeros(dq_acc.shape, F32)
    for c in range(HEADS):
        keys, values = pair(k_in, c), pair(v_in, c)
        dk = jnp.zeros((HEAD, CHUNK), F32)
        dv = jnp.zeros((HEAD, CHUNK), F32)
        for i in range(c, HEADS):
            at = i * (i + 1) // 2 + c
            dw = nn(turned(da_in[i]).astype(BF), values)
            ds = (dw * slope_keep[at]).astype(BF)
            dq_acc[i] += nt(keys, ds)
            dk = dk + nn(q_in[i], ds)
            dv = dv + nn(da_in[i], w_keep[at])
        dk, dv = dk.astype(BF), dv.astype(BF)
        dq_out[c] = dq_acc[c].astype(BF)
        for b in range(2):
            kb = 2 * c + b
            dk_out[kb] = dk[:, b * TOK : (b + 1) * TOK]
            dv_out[kb] = dv[:, b * TOK : (b + 1) * TOK]

            @pl.when(cp != kb)
            def _():
                remote(
                    dk_out.at[kb], dk_in.at[half, rows64(head)], send.at[7], recv.at[7], (dp, kb)
                ).start()
                remote(
                    dv_out.at[kb], dv_in.at[half, rows64(head)], send.at[8], recv.at[8], (dp, kb)
                ).start()

        @pl.when(head != c)
        def _():
            remote(
                dq_out.at[c], dq_in.at[rows64(head)], send.at[9], recv.at[9], (dp, block_of(c))
            ).start()

    dq_in[rows64(head), :] = dq_out[pl.ds(head, 1)].reshape(HEAD, TOK)
    dk_in[pl.ds(half, 1), rows64(head), :] = dk_out[pl.ds(cp, 1)]
    dv_in[pl.ds(half, 1), rows64(head), :] = dv_out[pl.ds(cp, 1)]
    wait_got(dk_out.at[pl.ds(0, N_CP - 1)], 7)
    wait_got(dv_out.at[pl.ds(0, N_CP - 1)], 8)
    wait_got(dq_in.at[pl.ds(0, D - HEAD)], 9)

    def column_back(b, grad):
        dh_t[b * D : (b + 1) * D, :] = (
            grad * silu_slope(hidden_t[b * D : (b + 1) * D, :])
        ).astype(BF)

    column_back(1, dv_in[0].astype(F32) + dv_in[1].astype(F32))
    column_back(2, dq_in[...].astype(F32))
    column_back(3, dk_in[0].astype(F32) + dk_in[1].astype(F32))
    dnormed = nn(joined[...], dh_t[...])
    dembed = column_norm_back(dnormed, normed_t[...], inv_ref[0:1, :]) + cot_t[...]

    exact = lax.Precision.HIGHEST
    cold_event = lax.dot_general(
        proj[...].astype(F32), dembed, (((1,), (0,)), ((), ())),
        preferred_element_type=F32, precision=exact,
    )
    is_hot = slot_row < HOT
    for f in range(4):
        piece = dembed[f * 128 : (f + 1) * 128, :]
        pack_ref[:, f * TOK : (f + 1) * TOK] = jnp.where(
            is_hot, piece, cold_event if f == 0 else 0.0
        ).astype(BF)
    grad_out[...] = nt(slots_1h[...], pack_ref[...]).astype(BF)

    def send_grads(k, carry):
        to = far(k)
        remote(
            grad_out.at[tile(to[0] * N_CP + to[1])], grad_in.at[tile(me)],
            send.at[10], recv.at[10], to,
        ).start()
        return carry

    lax.fori_loop(1, DEVICES, send_grads, 0)
    grad_in[tile(me), :] = grad_out[tile(me), :]

    for b in range(1, 4):
        w_ref[b * D : (b + 1) * D, :] = nt(low, dh_t[b * D : (b + 1) * D, :]).astype(BF)
    w_ref[5 * D :, :] = nt(cold_t[...], dembed, exact).astype(BF)

    def half_rows(c):
        return pl.ds(pl.multiple_of(c * HALF_ROWS, 16), HALF_ROWS)

    def ar(src, dst, stage, k, to):
        return remote(src, dst, ar_send.at[stage, k], ar_recv.at[stage, k], to)

    def ar_got(ref, stage, k):
        ar(ref, ref, stage, k, (dp, cp)).wait_recv()

    def ar_sent(ref, stage, k):
        ar(ref, ref, stage, k, (dp, cp)).wait_send()

    sibling = (z * 2 + (1 - core), cp)
    place = (x, y, z)

    def along(dim, d):
        moved = [x, y, z]
        moved[dim] = (moved[dim] + d) % 4
        return moved[dim], (moved[2] * 2 + core, moved[0] * 4 + moved[1])

    ar(w_ref.at[half_rows(1 - core)], r0, 0, 0, sibling).start()
    ar_got(r0, 0, 0)
    u1[...] = (w_ref[half_rows(core), :].astype(F32) + r0[...].astype(F32)).astype(BF)
    for k in range(3):
        for d in range(1, 4):
            a, to = along(k, d)
            rows = pl.ds(pl.multiple_of(k * COLOR_ROWS + a * PART_ROWS, 16), PART_ROWS)
            ar(u1.at[rows], r1.at[k, d - 1], 1, k, to).start()
    for k in range(3):
        ar_got(r1.at[k], 1, k)
        own = pl.ds(pl.multiple_of(k * COLOR_ROWS + place[k] * PART_ROWS, 16), PART_ROWS)
        part = u1[own, :].astype(F32)
        for d in range(3):
            part = part + r1[k, d].astype(F32)
        for b in range(4):
            u2[k, b] = part[:, b * 128 : (b + 1) * 128].astype(BF)
        for d in range(1, 4):
            b, to = along((k + 1) % 3, d)
            ar(u2.at[k, b], r2.at[k, d - 1], 2, k, to).start()
    for k in range(3):
        ar_got(r2.at[k], 2, k)
        b_me, c_me = place[(k + 1) % 3], place[(k + 2) % 3]
        part = u2[k, pl.ds(b_me, 1)].reshape(PART_ROWS, 128).astype(F32)
        for d in range(3):
            part = part + r2[k, d].astype(F32)
        r3[k, pl.ds(c_me, 1)] = part.astype(BF).reshape(1, PART_ROWS, 128)
        for d in range(1, 4):
            _, to = along((k + 2) % 3, d)
            ar(r3.at[k, c_me], r3.at[k, c_me], 3, k, to).start()
    for k in range(3):
        ar_got(r3.at[k, pl.ds(0, 3)], 3, k)
        b_me = place[(k + 1) % 3]
        part = r3[k, 0].astype(F32)
        for d in range(1, 4):
            part = part + r3[k, d].astype(F32)
        g2[k, pl.ds(b_me, 1)] = part.astype(BF).reshape(1, PART_ROWS, 128)
        for d in range(1, 4):
            _, to = along((k + 1) % 3, d)
            ar(g2.at[k, b_me], g2.at[k, b_me], 4, k, to).start()
    for k in range(3):
        ar_got(g2.at[k, pl.ds(0, 3)], 4, k)
        a_me = place[k]
        for d in range(1, 4):
            _, to = along(k, d)
            ar(g2.at[k], total.at[core, k, a_me], 5, k, to).start()
        total[pl.ds(core, 1), k, pl.ds(a_me, 1)] = g2[k].reshape(1, 1, 4, PART_ROWS, 128)

    wait_got(grad_in.at[pl.ds(0, SLOTS - SLOT)], 10)
    pick32[...] = grad_in[...].astype(F32)
    for c in range(CAP):
        for f in range(4):
            rows_buf[c * DEVICES : (c + 1) * DEVICES, f * 128 : (f + 1) * 128] = pick32[
                pl.ds(CAP * f + c, DEVICES, stride=SLOT), :
            ].astype(BF)
    rows_copy = pltpu.make_async_copy(rows_buf, rows_out, out_sem.at[0])
    rows_copy.start()

    for k in range(3):
        ar_got(total.at[0, 0, pl.ds(0, 3)], 5, k)
        ar(total.at[core, k], total.at[core, k], 6, k, sibling).start()
    for k in range(3):
        ar_got(total.at[0, 0], 6, k)
    sums_copy = pltpu.make_async_copy(total, sums_out, out_sem.at[1])
    sums_copy.start()

    wait_sent(k_in.at[pl.ds(0, N_CP - 1)], 2)
    wait_sent(v_in.at[pl.ds(0, N_CP - 1)], 3)
    wait_sent(q_in.at[pl.ds(0, HEADS - 1)], 4)
    wait_sent(att_in.at[pl.ds(0, D - HEAD)], 5)
    wait_sent(da_in.at[pl.ds(0, HEADS - 1)], 6)
    wait_sent(dk_out.at[pl.ds(0, N_CP - 1)], 7)
    wait_sent(dv_out.at[pl.ds(0, N_CP - 1)], 8)
    wait_sent(dq_in.at[pl.ds(0, D - HEAD)], 9)
    wait_sent(grad_in.at[pl.ds(0, SLOTS - SLOT)], 10)
    ar_sent(r0, 0, 0)
    for k in range(3):
        ar_sent(r1.at[k], 1, k)
        ar_sent(r2.at[k], 2, k)
        ar_sent(r3.at[k, pl.ds(0, 3)], 3, k)
        ar_sent(g2.at[k, pl.ds(0, 3)], 4, k)
        ar_sent(total.at[0, 0, pl.ds(0, 3)], 5, k)
        ar_sent(total.at[0, 0], 6, k)
    rows_copy.wait()
    sums_copy.wait()


def finish_kernel(
    rows, req, sums, hot_out, cold_out, proj_out, joined_out, wout_out,
    hot_buf, cold_buf, sum_buf, sem,
):
    picked = rows[...]

    def onehot(rows_here, first):
        index = iota((rows_here, DEVICES), 0) + first
        return jnp.concatenate(
            [jnp.where(index == req[c : c + 1, :], 1.0, 0.0).astype(BF) for c in range(CAP)],
            axis=1,
        )

    copies = []

    def put(src, dst, i):
        copy = pltpu.make_async_copy(src, dst, sem.at[i])
        copy.start()
        copies.append(copy)

    scale = (TOK * DEVICES) ** -0.5
    for core in range(2):
        for k in range(3):
            for a in range(4):
                top = core * HALF_ROWS + k * COLOR_ROWS + a * PART_ROWS
                for b in range(4):
                    sum_buf[top : top + PART_ROWS, b * 128 : (b + 1) * 128] = (
                        sums[core, k, a, b].astype(F32) * scale
                    )
    for b in range(4):
        put(sum_buf.at[pl.ds(b * D, D)], joined_out.at[:, pl.ds(b * D, D)], b)
    put(sum_buf.at[pl.ds(4 * D, D)], wout_out, 4)
    put(sum_buf.at[pl.ds(5 * D, COLD_W)], proj_out, 5)
    hot_buf[...] = nn(onehot(HOT, 0), picked)
    put(hot_buf, hot_out, 6)
    low = picked[:, 0:COLD_W]
    for t in range(4):
        part = pl.ds(t * (COLD // 4), COLD // 4)
        cold_buf[part, :] = nn(onehot(COLD // 4, HOT + t * (COLD // 4)), low)
        put(cold_buf.at[part], cold_out.at[part], 7 + t)
    for copy in copies:
        copy.wait()


def vmem(n):
    return [pl.BlockSpec(memory_space=pltpu.VMEM)] * n


def anywhere(n):
    return [pl.BlockSpec(memory_space=pl.ANY)] * n


def local(row_owner, slot_row, hot, cold, proj, joined, wout, cot):
    code = row_owner[:, 0] * SHIFT + slot_row
    v = pltpu.VMEM
    layer_out, rows, req, sums = pl.pallas_call(
        step_kernel,
        out_shape=(
            jax.ShapeDtypeStruct((TOK, D), BF),
            jax.ShapeDtypeStruct((CAP * DEVICES, D), BF),
            jax.ShapeDtypeStruct((8, DEVICES), I32),
            jax.ShapeDtypeStruct((2, 3, 4, 4, PART_ROWS, 128), BF),
        ),
        in_specs=vmem(8),
        out_specs=tuple(vmem(1) + anywhere(1) + vmem(1) + anywhere(1)),
        scratch_shapes=[
            v((DEVICES, 1, TOK), I32), v((SLOTS, 128), F32), v((SLOTS, 128), BF),
            v((SLOTS, 128), BF), v((TOK, D), F32), v((D, TOK), F32), v((8, TOK), F32),
            v((COLD_W, TOK), F32), v((4 * D, D), BF),
            v((4 * D, TOK), F32), v((4 * D, TOK), BF), v((D, TOK), F32), v((D, TOK), F32),
            v((SLOTS, 4 * TOK), BF),
            v((N_CP, HEAD, TOK), BF), v((N_CP, HEAD, TOK), BF), v((HEADS, HEAD, TOK), BF),
            v((PAIRS, TOK, CHUNK), BF), v((PAIRS, TOK, CHUNK), F32),
            v((HEADS, HEAD, TOK), BF), v((D, TOK), BF), v((D, TOK), BF),
            v((HEADS, HEAD, TOK), BF),
            v((HEADS, HEAD, TOK), F32), v((HEADS, HEAD, TOK), BF),
            v((N_CP, HEAD, TOK), BF), v((N_CP, HEAD, TOK), BF),
            v((D, TOK), BF), v((2, D, TOK), BF), v((2, D, TOK), BF),
            v((4 * D, TOK), BF), v((128, 4 * TOK), BF),
            v((SLOTS, 128), BF), v((SLOTS, 128), BF), v((CAP * DEVICES, D), BF),
            v((W_ROWS, D), BF), v((HALF_ROWS, D), BF), v((HALF_ROWS, D), BF),
            v((3, 3, PART_ROWS, D), BF), v((3, 4, PART_ROWS, 128), BF),
            v((3, 3, PART_ROWS, 128), BF), v((3, 4, PART_ROWS, 128), BF),
            v((3, 4, PART_ROWS, 128), BF), v((2, 3, 4, 4, PART_ROWS, 128), BF),
            pltpu.SemaphoreType.DMA((11,)), pltpu.SemaphoreType.DMA((11,)),
            pltpu.SemaphoreType.DMA((7, 3)), pltpu.SemaphoreType.DMA((7, 3)),
            pltpu.SemaphoreType.DMA((2,)),
        ],
        compiler_params=pltpu.CompilerParams(
            collective_id=0, has_side_effects=True, vmem_limit_bytes=60 << 20
        ),
        name="step",
    )(code[:, None], code[None, :], hot, cold, proj, joined, wout, cot)
    hot_grad, cold_grad, proj_grad, joined_grad, wout_grad = pl.pallas_call(
        finish_kernel,
        out_shape=(
            jax.ShapeDtypeStruct((HOT, D), F32),
            jax.ShapeDtypeStruct((COLD, COLD_W), F32),
            jax.ShapeDtypeStruct((COLD_W, D), F32),
            jax.ShapeDtypeStruct((D, 4 * D), F32),
            jax.ShapeDtypeStruct((D, D), F32),
        ),
        in_specs=vmem(3),
        out_specs=tuple(anywhere(5)),
        scratch_shapes=[
            v((HOT, D), F32), v((COLD, COLD_W), F32), v((W_ROWS, D), F32),
            pltpu.SemaphoreType.DMA((11,)),
        ],
        compiler_params=pltpu.CompilerParams(vmem_limit_bytes=40 << 20),
        name="finish",
    )(rows, req, sums)
    return layer_out, hot_grad, cold_grad, proj_grad, joined_grad, wout_grad


def solution(mesh):
    rows = P(("dp", "cp"), None)
    return jax.shard_map(
        local,
        mesh=mesh,
        in_specs=(rows, P(("dp", "cp")), rows, rows, P(), P(), P(), rows),
        out_specs=(rows, rows, rows, P(), P(), P()),
        check_vma=False,
    )
```

```python
import math

import jax
import jax.numpy as jnp
from jax import lax
from jax.experimental import pallas as pl
from jax.experimental.pallas import tpu as pltpu
from jax.sharding import PartitionSpec as P

MESH = pl.DeviceIdType.MESH
BF = jnp.bfloat16
F32 = jnp.float32
I32 = jnp.int32
EPSILON = 1e-05

D = 512
HEADS = 8
HEAD = 64
TOK = 128
CAP = 4
HOT = 512
COLD = 2048
COLD_W = 128
N_DP = 8
N_CP = 16
DEVICES = N_DP * N_CP
SLOT = 16
SLOTS = DEVICES * SLOT
SHIFT = 4096
CHUNK = 256
PAIRS = HEADS * (HEADS + 1) // 2
W_ROWS = 4 * D + D + COLD_W
LATE = 2 * D
SETS = (
    (0, 512, (48, 48, 32), (0, 48, 96)),
    (LATE, 832, (64, 64, 80), (128, 192, 256)),
)
PART_ROWS = 336
FAR_FIRST = sorted(
    (
        (dz, dc, dx, dy)
        for dz in range(4)
        for dc in range(2)
        for dx in range(4)
        for dy in range(4)
        if dz or dc or dx or dy
    ),
    key=lambda o: (-sum(min(v, 4 - v) for v in (o[0], o[2], o[3])), sum(o) * 53 % 7, o),
)


def nn(a, b):
    return jnp.dot(a, b, preferred_element_type=F32)


def nt(a, b, precision=None):
    return lax.dot_general(
        a, b, (((1,), (1,)), ((), ())), preferred_element_type=F32, precision=precision
    )


def sigmoid(v):
    return 0.5 * jnp.tanh(0.5 * v) + 0.5


def silu_slope(v):
    sig = sigmoid(v)
    return sig + v * sig * (1.0 - sig)


def iota(shape, dim):
    return lax.broadcasted_iota(I32, shape, dim)


def turned(v):
    return v.astype(F32).T


def column_norm(v):
    average = jnp.mean(v, axis=0, keepdims=True)
    centred = v - average
    inverse = lax.rsqrt(jnp.mean(centred * centred, axis=0, keepdims=True) + EPSILON)
    return centred * inverse, inverse


def column_norm_back(g, y, inverse):
    first = jnp.mean(g, axis=0, keepdims=True)
    second = jnp.mean(g * y, axis=0, keepdims=True)
    return (g - first - y * second) * inverse


def step_kernel(
    owner_in, slot_in, hot_hbm, cold_hbm, proj_hbm, joined_hbm, wout_hbm, cot_hbm,
    layer_out, rows_out, req_out, sums_out,
    hot, cold, proj, joined, wout, cot, code_row,
    ids_all, pick32, pick16, row_in, emb_nat, normed_t, inv_ref, cold_t, joined_t,
    hidden_t, active_t, dgated_t, cot_t, slots_1h,
    k_in, v_in, q_in, w_keep, slope_keep, att_out, att_in, da_out, da_in, da_nat,
    dq_acc, dq_out, dk_out, dv_out, dq_in, dk_in, dv_in, dh_t, pack_ref, grad_out, grad_in,
    rows_buf, layer_buf, req_buf, w_ref, r0, u1, r1, u2, r2, r3, g2, total,
    send, recv, ar_send, ar_recv, local_sem,
):
    dp, cp = lax.axis_index("dp"), lax.axis_index("cp")
    me = dp * N_CP + cp
    z, core, x, y = dp // 2, dp % 2, cp // 4, cp % 4
    head = cp // 2
    half = ((cp + 1) // 2) % 2
    xs, ys, zs = ([(v + d) % 4 for d in range(4)] for v in (x, y, z))
    cores = [core, (core + 1) % 2]
    dps = [[zs[dz] * 2 + cores[dc] for dc in range(2)] for dz in range(4)]
    cps = [[xs[dx] * 4 + ys[dy] for dy in range(4)] for dx in range(4)]
    plane = [(dx, dy) for dx in range(4) for dy in range(4) if dx or dy]
    plane.sort(key=lambda o: (-(min(o[0], 4 - o[0]) + min(o[1], 4 - o[1])), (o[0] * 3 + o[1]) % 4))

    def remote(src, dst, send_sem, recv_sem, to):
        return pltpu.make_async_remote_copy(
            src_ref=src, dst_ref=dst, send_sem=send_sem, recv_sem=recv_sem,
            device_id=to, device_id_type=MESH,
        )

    def wait_sent(ref, i):
        remote(ref, ref, send.at[i], recv.at[i], (dp, cp)).wait_send()

    def wait_got(ref, i):
        remote(ref, ref, send.at[i], recv.at[i], (dp, cp)).wait_recv()

    def rows64(h):
        return pl.ds(pl.multiple_of(h * HEAD, HEAD), HEAD)

    def tile(o):
        return pl.ds(pl.multiple_of(o * SLOT, SLOT), SLOT)

    barrier = pltpu.get_barrier_semaphore()
    everyone = [(dps[dz][dc], cps[dx][dy]) for dz, dc, dx, dy in FAR_FIRST]
    for to in everyone:
        pl.semaphore_signal(barrier, inc=1, device_id=to, device_id_type=MESH)
    loads = [
        pltpu.make_async_copy(src, dst, local_sem.at[i])
        for i, (src, dst) in enumerate(
            ((joined_hbm, joined), (cot_hbm, cot), (wout_hbm, wout), (hot_hbm, hot),
             (cold_hbm, cold), (proj_hbm, proj))
        )
    ]
    for load in loads:
        load.start()
    owner_row, slot_row = owner_in[...], slot_in[...]
    code_row[...] = owner_row * SHIFT + slot_row
    pl.semaphore_wait(barrier, DEVICES - 1)

    for to in everyone:
        remote(code_row, ids_all.at[me], send.at[0], recv.at[0], to).start()
    ids_all[pl.ds(me, 1)] = code_row[...].reshape(1, 1, TOK)

    diagonal = iota((TOK, TOK), 0) == iota((TOK, TOK), 1)

    def as_column(row):
        picked = jnp.where(diagonal, row.astype(F32), 0.0)
        return jnp.sum(picked, axis=1, keepdims=True).astype(I32)

    owner_col, slot_col = as_column(owner_row), as_column(slot_row)
    before_row = (owner_col == owner_row) & (iota((TOK, TOK), 0) < iota((TOK, TOK), 1))
    rank_row = jnp.sum(jnp.where(before_row, 1, 0), axis=0, keepdims=True)
    place_row = owner_row * SLOT + rank_row
    place_col = as_column(place_row)
    for f in range(4):
        slots_1h[:, f * TOK : (f + 1) * TOK] = jnp.where(
            iota((SLOTS, TOK), 0) == place_row + CAP * f, 1.0, 0.0
        ).astype(BF)
    for load in loads[:3]:
        load.wait()
    for b in range(4):
        joined_t[b * D : (b + 1) * D, :] = turned(joined[:, b * D : (b + 1) * D]).astype(BF)
    cot_t[...] = turned(cot[...])
    dgated_t[...] = nn(wout[...], cot_t[...].astype(BF))
    for load in loads[3:]:
        load.wait()

    wait_got(ids_all.at[pl.ds(0, DEVICES - 1)], 0)

    ids = ids_all[:, 0, :]
    asked = (ids // SHIFT) == me
    slot_plus = ((ids % SHIFT) + 1).astype(F32)
    upper = jnp.where(iota((TOK, TOK), 0) < iota((TOK, TOK), 1), 1.0, 0.0).astype(BF)
    earlier = nn(jnp.where(asked, 1.0, 0.0).astype(BF), upper)
    lane_hot = iota((DEVICES, HOT), 1).astype(F32) + 1.0
    lane_cold = iota((DEVICES, COLD), 1).astype(F32) + (HOT + 1.0)
    asks = []
    for c in range(CAP):
        ask = jnp.where(asked & (earlier == float(c)), slot_plus, 0.0)
        asks.append(ask)
        wanted = jnp.sum(ask, axis=1, keepdims=True)
        hot_rows = nn(jnp.where(lane_hot == wanted, 1.0, 0.0).astype(BF), hot[...])
        cold_rows = nn(jnp.where(lane_cold == wanted, 1.0, 0.0).astype(BF), cold[...])
        for f in range(4):
            piece = hot_rows[:, f * 128 : (f + 1) * 128]
            if f == 0:
                piece = piece + cold_rows
            pick32[pl.ds(CAP * f + c, DEVICES, stride=SLOT), :] = piece
    pick16[...] = pick32[...].astype(BF)

    for to in everyone:
        remote(
            pick16.at[tile(to[0] * N_CP + to[1])], row_in.at[tile(me)], send.at[1], recv.at[1], to
        ).start()
    row_in[tile(me), :] = pick16[tile(me), :]
    req_buf[...] = jnp.zeros(req_buf.shape, I32)
    for c in range(CAP):
        wanted_row = jnp.sum(asks[c].T, axis=0, keepdims=True)
        req_buf[c : c + 1, :] = wanted_row.astype(I32) - 1
    req_copy = pltpu.make_async_copy(req_buf, req_out, local_sem.at[6])
    req_copy.start()

    wait_got(row_in.at[pl.ds(0, SLOTS - SLOT)], 1)

    fetched = []
    for f in range(4):
        take = jnp.where(iota((TOK, SLOTS), 1) == place_col + CAP * f, 1.0, 0.0).astype(BF)
        fetched.append(nn(take, row_in[...]))
    cold_vec = fetched[0]
    cold_embed = nn(cold_vec.astype(BF), proj[...])
    embedded = jnp.where(slot_col < HOT, jnp.concatenate(fetched, axis=1), cold_embed)
    emb_nat[...] = embedded
    normed, inverse = column_norm(embedded.T)
    normed_t[...] = normed
    inv_ref[...] = jnp.broadcast_to(inverse, inv_ref.shape)
    low = normed.astype(BF)

    def k_rows(h):
        return pl.ds(pl.multiple_of(3 * D + h * HEAD, HEAD), HEAD)

    def v_rows(h):
        return pl.ds(pl.multiple_of(D + h * HEAD, HEAD), HEAD)

    def q_rows(h):
        return pl.ds(pl.multiple_of(2 * D + h * HEAD, HEAD), HEAD)

    def same_half(d):
        h = (head + d) % HEADS
        return h, (dp, 2 * h + (half + h) % 2)

    def project(b):
        hid = nn(joined_t[b * D : (b + 1) * D, :], low)
        hidden_t[b * D : (b + 1) * D, :] = hid
        active_t[b * D : (b + 1) * D, :] = (hid * sigmoid(hid)).astype(BF)

    project(3)
    for dx, dy in plane:
        pcp = cps[dx][dy]
        remote(active_t.at[k_rows(pcp // 2)], k_in.at[cp], send.at[2], recv.at[2], (dp, pcp)).start()
    project(1)
    for dx, dy in plane:
        pcp = cps[dx][dy]
        remote(active_t.at[v_rows(pcp // 2)], v_in.at[cp], send.at[3], recv.at[3], (dp, pcp)).start()
    project(2)
    for d in range(1, HEADS):
        h, to = same_half(d)
        remote(active_t.at[q_rows(h)], q_in.at[head], send.at[4], recv.at[4], to).start()
    k_in[pl.ds(cp, 1)] = active_t[k_rows(head), :].reshape(1, HEAD, TOK)
    v_in[pl.ds(cp, 1)] = active_t[v_rows(head), :].reshape(1, HEAD, TOK)
    q_in[pl.ds(head, 1)] = active_t[q_rows(head), :].reshape(1, HEAD, TOK)
    project(0)
    cold_t[...] = jnp.where(slot_row < HOT, 0.0, cold_vec.T)
    wait_got(k_in.at[pl.ds(0, N_CP - 1)], 2)
    wait_got(v_in.at[pl.ds(0, N_CP - 1)], 3)
    wait_got(q_in.at[pl.ds(0, HEADS - 1)], 4)

    def block_of(i):
        return 4 * (i // 2) + (half if i % 2 == 0 else 3 - half)

    def pair(ref, c):
        return jnp.concatenate([ref[2 * c], ref[2 * c + 1]], axis=1)

    shrink = 0.5 / math.sqrt(HEAD)
    for i in range(HEADS):
        q_nat = (turned(q_in[i]) * shrink).astype(BF)
        total_t = jnp.zeros((HEAD, TOK), F32)
        for c in range(i + 1):
            s = nn(q_nat, pair(k_in, c))
            up = 1.0 + jnp.tanh(s)
            w = s * up
            slope = up + w * (2.0 - up)
            if c == i:
                ok = (iota((TOK, CHUNK), 1) + c * CHUNK) <= (
                    iota((TOK, CHUNK), 0) + block_of(i) * TOK
                )
                w = jnp.where(ok, w, 0.0)
                slope = jnp.where(ok, slope, 0.0)
            w = w.astype(BF)
            at = i * (i + 1) // 2 + c
            w_keep[at] = w
            slope_keep[at] = slope
            total_t = total_t + nt(pair(v_in, c), w)
        att_out[i] = total_t.astype(BF)

        @pl.when(head != i)
        def _():
            remote(
                att_out.at[i], att_in.at[rows64(head)], send.at[5], recv.at[5], (dp, block_of(i))
            ).start()

    att_in[rows64(head), :] = att_out[pl.ds(head, 1)].reshape(HEAD, TOK)
    wait_got(att_in.at[pl.ds(0, D - HEAD)], 5)

    mixed, inv_mix = column_norm(att_in[...].astype(F32))
    gate = active_t[0:D, :].astype(F32)
    dgated = dgated_t[...]
    da_out[...] = column_norm_back(dgated * gate, mixed, inv_mix).astype(BF)
    for d in range(1, HEADS):
        h, to = same_half(d)
        remote(da_out.at[rows64(h)], da_in.at[head], send.at[6], recv.at[6], to).start()
    da_in[pl.ds(head, 1)] = da_out[rows64(head), :].reshape(1, HEAD, TOK)

    sibling = (z * 2 + (1 - core), cp)
    place = (x, y, z)

    def along(dim, d):
        moved = [xs[0], ys[0], zs[0]]
        moved[dim] = (xs, ys, zs)[dim][d]
        return moved[dim], (moved[2] * 2 + core, moved[0] * 4 + moved[1])

    def ar(src, dst, n, stage, k, to):
        return remote(src, dst, ar_send.at[n, stage, k], ar_recv.at[n, stage, k], to)

    def ar_got(ref, n, stage, k):
        ar(ref, ref, n, stage, k, (dp, cp)).wait_recv()

    def ar_sent(ref, n, stage, k):
        ar(ref, ref, n, stage, k, (dp, cp)).wait_send()

    def core_rows(n, c, first, count):
        base, rows = SETS[n][:2]
        return pl.ds(pl.multiple_of(base + c * rows + first, 16), count)

    def set_rows(n, first, count):
        return pl.ds(SETS[n][0] // 2 + first, count)

    def stage0(n, k, first, count):
        ar(
            w_ref.at[core_rows(n, 1 - core, first, count)], r0.at[set_rows(n, first, count)],
            n, 0, k, sibling,
        ).start()

    def stage1(n, k, first, count, colors):
        at = set_rows(n, first, count)
        ar_got(r0.at[at], n, 0, k)
        u1[at, :] = (
            w_ref[core_rows(n, core, first, count), :].astype(F32) + r0[at, :].astype(F32)
        ).astype(BF)
        for color in colors:
            start1(n, color)

    def piece(n, k):
        return pl.ds(SETS[n][3][k], SETS[n][2][k])

    def u1_rows(n, k, a):
        part = SETS[n][2][k]
        return pl.ds(
            pl.multiple_of(SETS[n][0] // 2 + sum(SETS[n][2][:k]) * 4 + a * part, 16), part
        )

    def start1(n, k):
        for d in (2, 1, 3):
            a, to = along(k, d)
            ar(u1.at[u1_rows(n, k, a)], r1.at[d - 1, piece(n, k)], n, 1, k, to).start()

    def stage2(n, k):
        at = piece(n, k)
        ar_got(r1.at[:, at], n, 1, k)
        part = u1[u1_rows(n, k, place[k]), :].astype(F32)
        for d in range(3):
            part = part + r1[d, at, :].astype(F32)
        for b in range(4):
            u2[b, at, :] = part[:, b * 128 : (b + 1) * 128].astype(BF)
        for d in (2, 1, 3):
            b, to = along((k + 1) % 3, d)
            ar(u2.at[b, at], r2.at[d - 1, at], n, 2, k, to).start()

    def stage3(n, k):
        at, rows = piece(n, k), SETS[n][2][k]
        ar_got(r2.at[:, at], n, 2, k)
        b_me, c_me = place[(k + 1) % 3], place[(k + 2) % 3]
        part = u2[pl.ds(b_me, 1), at, :].astype(F32)
        for d in range(3):
            part = part + r2[d : d + 1, at, :].astype(F32)
        r3[pl.ds(c_me, 1), at, :] = part.astype(BF)
        for d in (2, 1, 3):
            _, to = along((k + 2) % 3, d)
            ar(r3.at[c_me, at], r3.at[c_me, at], n, 3, k, to).start()

    def stage4(n, k):
        at = piece(n, k)
        ar_got(r3.at[pl.ds(0, 3), at], n, 3, k)
        b_me = place[(k + 1) % 3]
        part = r3[0:1, at, :].astype(F32)
        for d in range(1, 4):
            part = part + r3[d : d + 1, at, :].astype(F32)
        g2[pl.ds(b_me, 1), at, :] = part.astype(BF)
        for d in (2, 1, 3):
            _, to = along((k + 1) % 3, d)
            ar(g2.at[b_me, at], g2.at[b_me, at], n, 4, k, to).start()

    def stage5(n, k):
        at = piece(n, k)
        ar_got(g2.at[pl.ds(0, 3), at], n, 4, k)
        a_me = place[k]
        for d in (2, 1, 3):
            _, to = along(k, d)
            ar(g2.at[:, at], total.at[core, a_me, :, at], n, 5, k, to).start()
        total[pl.ds(core, 1), pl.ds(a_me, 1), :, at, :] = g2[:, at, :].reshape(
            1, 1, 4, SETS[n][2][k], 128
        )

    def stage6(n, k):
        at = piece(n, k)
        ar_got(total.at[0, pl.ds(0, 3), :, at], n, 5, k)
        ar(total.at[core, :, :, at], total.at[core, :, :, at], n, 6, k, sibling).start()

    def stage7(n, k):
        ar_got(total.at[0, :, :, piece(n, k)], n, 6, k)

    def all_colors(stage, n):
        for k in range(3):
            stage(n, k)

    def settle(n, firsts):
        for k, count in firsts:
            ar_sent(r0.at[pl.ds(0, count)], n, 0, k)
        for k in range(3):
            at = piece(n, k)
            ar_sent(r1.at[:, at], n, 1, k)
            ar_sent(r2.at[:, at], n, 2, k)
            ar_sent(r3.at[pl.ds(0, 3), at], n, 3, k)
            ar_sent(g2.at[pl.ds(0, 3), at], n, 4, k)
            ar_sent(total.at[0, pl.ds(0, 3), :, at], n, 5, k)
            ar_sent(total.at[0, :, :, at], n, 6, k)

    gated = (mixed * gate).astype(BF)
    low = normed_t[...].astype(BF)
    dh_gate = (dgated * mixed * silu_slope(hidden_t[0:D, :])).astype(BF)
    dh_t[0:D, :] = dh_gate
    w_ref[0:D, :] = nt(low, dh_gate).astype(BF)
    w_ref[D : 2 * D, :] = nn(gated, cot[...]).astype(BF)
    stage0(0, 0, 0, D)
    branch = nn(turned(gated).astype(BF), wout[...])
    layer_buf[...] = (emb_nat[...] + branch).astype(BF)
    layer_copy = pltpu.make_async_copy(layer_buf, layer_out, local_sem.at[7])
    layer_copy.start()
    stage1(0, 0, 0, D, (0, 1, 2))

    wait_got(da_in.at[pl.ds(0, HEADS - 1)], 6)

    for i in range(HEADS):
        da_nat[i] = (turned(da_in[i]) * shrink).astype(BF)
    dq_acc[...] = jnp.zeros(dq_acc.shape, F32)
    for c in range(HEADS - 1, -1, -1):
        keys, values = pair(k_in, c), pair(v_in, c)
        dk = jnp.zeros((HEAD, CHUNK), F32)
        dv = jnp.zeros((HEAD, CHUNK), F32)
        for i in range(c, HEADS):
            at = i * (i + 1) // 2 + c
            ds = (nn(da_nat[i], values) * slope_keep[at]).astype(BF)
            dq = dq_acc[i] + nt(keys, ds)
            if c:
                dq_acc[i] = dq
            else:
                dq_out[i] = dq.astype(BF)

                @pl.when(head != i)
                def _():
                    remote(
                        dq_out.at[i], dq_in.at[rows64(head)], send.at[9], recv.at[9],
                        (dp, block_of(i)),
                    ).start()
            dk = dk + nn(q_in[i], ds)
            dv = dv + nn(da_in[i], w_keep[at])
        dk, dv = dk.astype(BF), dv.astype(BF)
        for b in range(2):
            kb = 2 * c + b
            dk_out[kb] = dk[:, b * TOK : (b + 1) * TOK]
            dv_out[kb] = dv[:, b * TOK : (b + 1) * TOK]

            @pl.when(cp != kb)
            def _():
                remote(
                    dk_out.at[kb], dk_in.at[half, rows64(head)], send.at[7], recv.at[7], (dp, kb)
                ).start()
                remote(
                    dv_out.at[kb], dv_in.at[half, rows64(head)], send.at[8], recv.at[8], (dp, kb)
                ).start()

        if c == 2:
            all_colors(stage2, 0)
        if c == 0:
            all_colors(stage3, 0)

    dq_in[rows64(head), :] = dq_out[pl.ds(head, 1)].reshape(HEAD, TOK)
    dk_in[pl.ds(half, 1), rows64(head), :] = dk_out[pl.ds(cp, 1)]
    dv_in[pl.ds(half, 1), rows64(head), :] = dv_out[pl.ds(cp, 1)]
    wait_got(dk_out.at[pl.ds(0, N_CP - 1)], 7)
    wait_got(dv_out.at[pl.ds(0, N_CP - 1)], 8)
    wait_got(dq_in.at[pl.ds(0, D - HEAD)], 9)

    def column_back(b, grad):
        dh = (grad * silu_slope(hidden_t[b * D : (b + 1) * D, :])).astype(BF)
        dh_t[b * D : (b + 1) * D, :] = dh
        grads = nt(low, dh).astype(BF)
        if b == 1:
            w_ref[LATE : LATE + D, :] = grads
        elif b == 2:
            w_ref[LATE + D : LATE + 768, :] = grads[0:256]
            w_ref[LATE + 832 : LATE + 1088, :] = grads[256:512]
        else:
            w_ref[LATE + 1088 : LATE + 1600, :] = grads

    column_back(1, dv_in[0].astype(F32) + dv_in[1].astype(F32))
    column_back(2, dq_in[...].astype(F32))
    column_back(3, dk_in[0].astype(F32) + dk_in[1].astype(F32))
    stage0(1, 0, 0, 768)
    all_colors(stage4, 0)

    dnormed = nn(joined[...], dh_t[...])
    dembed = column_norm_back(dnormed, normed_t[...], inv_ref[0:1, :]) + cot_t[...]
    exact = lax.Precision.HIGHEST
    proj_grads = nt(cold_t[...], dembed, exact).astype(BF)
    w_ref[LATE + 768 : LATE + 832, :] = proj_grads[0:64]
    w_ref[LATE + 1600 : LATE + 1664, :] = proj_grads[64:128]
    stage0(1, 1, 768, 64)
    stage1(1, 0, 0, 768, (0, 1))
    stage1(1, 1, 768, 64, (2,))

    cold_event = lax.dot_general(
        proj[...].astype(F32), dembed, (((1,), (0,)), ((), ())),
        preferred_element_type=F32, precision=exact,
    )
    is_hot = slot_row < HOT
    for f in range(4):
        part = dembed[f * 128 : (f + 1) * 128, :]
        pack_ref[:, f * TOK : (f + 1) * TOK] = jnp.where(
            is_hot, part, cold_event if f == 0 else 0.0
        ).astype(BF)
    grad_out[...] = nt(slots_1h[...], pack_ref[...]).astype(BF)
    all_colors(stage5, 0)
    for to in everyone:
        remote(
            grad_out.at[tile(to[0] * N_CP + to[1])], grad_in.at[tile(me)],
            send.at[10], recv.at[10], to,
        ).start()
    grad_in[tile(me), :] = grad_out[tile(me), :]

    all_colors(stage2, 1)
    all_colors(stage3, 1)
    all_colors(stage6, 0)
    all_colors(stage4, 1)
    all_colors(stage5, 1)

    wait_got(grad_in.at[pl.ds(0, SLOTS - SLOT)], 10)
    pick32[...] = grad_in[...].astype(F32)
    for c in range(CAP):
        for f in range(4):
            rows_buf[c * DEVICES : (c + 1) * DEVICES, f * 128 : (f + 1) * 128] = pick32[
                pl.ds(CAP * f + c, DEVICES, stride=SLOT), :
            ].astype(BF)
    rows_copy = pltpu.make_async_copy(rows_buf, rows_out, local_sem.at[8])
    rows_copy.start()
    all_colors(stage7, 0)

    wait_sent(ids_all.at[pl.ds(0, DEVICES - 1)], 0)
    wait_sent(row_in.at[pl.ds(0, SLOTS - SLOT)], 1)
    wait_sent(k_in.at[pl.ds(0, N_CP - 1)], 2)
    wait_sent(v_in.at[pl.ds(0, N_CP - 1)], 3)
    wait_sent(q_in.at[pl.ds(0, HEADS - 1)], 4)
    wait_sent(att_in.at[pl.ds(0, D - HEAD)], 5)
    wait_sent(da_in.at[pl.ds(0, HEADS - 1)], 6)
    wait_sent(dk_out.at[pl.ds(0, N_CP - 1)], 7)
    wait_sent(dv_out.at[pl.ds(0, N_CP - 1)], 8)
    wait_sent(dq_in.at[pl.ds(0, D - HEAD)], 9)
    wait_sent(grad_in.at[pl.ds(0, SLOTS - SLOT)], 10)
    settle(0, ((0, D),))
    all_colors(stage6, 1)
    near_copy = pltpu.make_async_copy(total.at[core], sums_out.at[core], local_sem.at[9])
    near_copy.start()
    all_colors(stage7, 1)
    far_copy = pltpu.make_async_copy(total.at[1 - core], sums_out.at[1 - core], local_sem.at[10])
    far_copy.start()
    settle(1, ((0, 768), (1, 64)))
    req_copy.wait()
    layer_copy.wait()
    rows_copy.wait()
    near_copy.wait()
    far_copy.wait()


def finish_kernel(
    layer_in, rows_in, req_in, sums_in,
    layer_out, hot_out, cold_out, proj_out, joined_out, wout_out,
    layer, rows, req, sums, hot_buf, cold_buf, sum_buf, in_sem, sem,
):
    loads = [
        pltpu.make_async_copy(src, dst, in_sem.at[i])
        for i, (src, dst) in enumerate(
            ((req_in, req), (rows_in, rows), (sums_in.at[0], sums.at[0]),
             (sums_in.at[1], sums.at[1]), (layer_in, layer))
        )
    ]
    for load in loads:
        load.start()
    copies = []

    def put(src, dst):
        copy = pltpu.make_async_copy(src, dst, sem.at[len(copies)])
        copy.start()
        copies.append(copy)

    loads[0].wait()
    loads[1].wait()
    picked = rows[...]

    def onehot(rows_here, first):
        index = iota((rows_here, DEVICES), 0) + first
        return jnp.concatenate(
            [jnp.where(index == req[c : c + 1, :], 1.0, 0.0).astype(BF) for c in range(CAP)],
            axis=1,
        )

    hot_buf[...] = nn(onehot(HOT, 0), picked)
    put(hot_buf, hot_out)
    low = picked[:, 0:COLD_W]
    for t in range(4):
        part = pl.ds(t * (COLD // 4), COLD // 4)
        cold_buf[part, :] = nn(onehot(COLD // 4, HOT + t * (COLD // 4)), low)
        put(cold_buf.at[part], cold_out.at[part])

    scale = (TOK * DEVICES) ** -0.5
    for core in range(2):
        loads[2 + core].wait()
        for n in range(2):
            for k in range(3):
                count, at = SETS[n][2][k], SETS[n][3][k]
                for a in range(4):
                    first = sum(SETS[n][2][:k]) * 4 + a * count
                    for source, target, length in targets(n, core, first, count):
                        for b in range(4):
                            sum_buf[target : target + length, b * 128 : (b + 1) * 128] = (
                                sums[core, a, b, at + source : at + source + length, :].astype(F32)
                                * scale
                            )
        if core == 0:
            for b in (0, 1):
                put(sum_buf.at[pl.ds(b * D, D)], joined_out.at[:, pl.ds(b * D, D)])
            loads[4].wait()
            put(layer, layer_out)
    for b in (2, 3):
        put(sum_buf.at[pl.ds(b * D, D)], joined_out.at[:, pl.ds(b * D, D)])
    put(sum_buf.at[pl.ds(4 * D, D)], wout_out)
    put(sum_buf.at[pl.ds(5 * D, COLD_W)], proj_out)
    for copy in copies:
        copy.wait()


def targets(n, core, first, count):
    if n == 0:
        return [(0, (4 * D if core else 0) + first, count)]
    runs = []
    if first < 768:
        length = min(count, 768 - first)
        runs.append((0, D + core * 768 + first, length))
    if first + count > 768:
        start = max(first, 768)
        runs.append((start - first, 5 * D + core * 64 + start - 768, first + count - start))
    return runs


def vmem(n):
    return [pl.BlockSpec(memory_space=pltpu.VMEM)] * n


def anywhere(n):
    return [pl.BlockSpec(memory_space=pl.ANY)] * n


def local(row_owner, slot_row, hot, cold, proj, joined, wout, cot):
    v = pltpu.VMEM
    layer, rows, req, sums = pl.pallas_call(
        step_kernel,
        out_shape=(
            jax.ShapeDtypeStruct((TOK, D), BF),
            jax.ShapeDtypeStruct((CAP * DEVICES, D), BF),
            jax.ShapeDtypeStruct((8, DEVICES), I32),
            jax.ShapeDtypeStruct((2, 4, 4, PART_ROWS, 128), BF),
        ),
        in_specs=vmem(2) + anywhere(6),
        out_specs=tuple(anywhere(4)),
        scratch_shapes=[
            v((HOT, D), BF), v((COLD, COLD_W), BF), v((COLD_W, D), BF), v((D, 4 * D), BF),
            v((D, D), BF), v((TOK, D), BF), v((1, TOK), I32),
            v((DEVICES, 1, TOK), I32), v((SLOTS, 128), F32), v((SLOTS, 128), BF),
            v((SLOTS, 128), BF), v((TOK, D), F32), v((D, TOK), F32), v((8, TOK), F32),
            v((COLD_W, TOK), F32), v((4 * D, D), BF),
            v((4 * D, TOK), F32), v((4 * D, TOK), BF), v((D, TOK), F32), v((D, TOK), F32),
            v((SLOTS, 4 * TOK), BF),
            v((N_CP, HEAD, TOK), BF), v((N_CP, HEAD, TOK), BF), v((HEADS, HEAD, TOK), BF),
            v((PAIRS, TOK, CHUNK), BF), v((PAIRS, TOK, CHUNK), F32),
            v((HEADS, HEAD, TOK), BF), v((D, TOK), BF), v((D, TOK), BF),
            v((HEADS, HEAD, TOK), BF), v((HEADS, TOK, HEAD), BF),
            v((HEADS, HEAD, TOK), F32), v((HEADS, HEAD, TOK), BF),
            v((N_CP, HEAD, TOK), BF), v((N_CP, HEAD, TOK), BF),
            v((D, TOK), BF), v((2, D, TOK), BF), v((2, D, TOK), BF),
            v((4 * D, TOK), BF), v((128, 4 * TOK), BF),
            v((SLOTS, 128), BF), v((SLOTS, 128), BF), v((CAP * DEVICES, D), BF),
            v((TOK, D), BF), v((8, DEVICES), I32),
            v((W_ROWS, D), BF), v((W_ROWS // 2, D), BF), v((W_ROWS // 2, D), BF),
            v((3, PART_ROWS, D), BF), v((4, PART_ROWS, 128), BF),
            v((3, PART_ROWS, 128), BF), v((4, PART_ROWS, 128), BF),
            v((4, PART_ROWS, 128), BF), v((2, 4, 4, PART_ROWS, 128), BF),
            pltpu.SemaphoreType.DMA((11,)), pltpu.SemaphoreType.DMA((11,)),
            pltpu.SemaphoreType.DMA((2, 7, 3)), pltpu.SemaphoreType.DMA((2, 7, 3)),
            pltpu.SemaphoreType.DMA((11,)),
        ],
        compiler_params=pltpu.CompilerParams(
            collective_id=0, has_side_effects=True, vmem_limit_bytes=60 << 20
        ),
        name="step",
    )(row_owner.reshape(1, TOK), slot_row.reshape(1, TOK), hot, cold, proj, joined, wout, cot)
    return pl.pallas_call(
        finish_kernel,
        out_shape=(
            jax.ShapeDtypeStruct((TOK, D), BF),
            jax.ShapeDtypeStruct((HOT, D), F32),
            jax.ShapeDtypeStruct((COLD, COLD_W), F32),
            jax.ShapeDtypeStruct((COLD_W, D), F32),
            jax.ShapeDtypeStruct((D, 4 * D), F32),
            jax.ShapeDtypeStruct((D, D), F32),
        ),
        in_specs=anywhere(4),
        out_specs=tuple(anywhere(6)),
        scratch_shapes=[
            v((TOK, D), BF), v((CAP * DEVICES, D), BF), v((8, DEVICES), I32),
            v((2, 4, 4, PART_ROWS, 128), BF),
            v((HOT, D), F32), v((COLD, COLD_W), F32), v((W_ROWS, D), F32),
            pltpu.SemaphoreType.DMA((5,)), pltpu.SemaphoreType.DMA((12,)),
        ],
        compiler_params=pltpu.CompilerParams(vmem_limit_bytes=60 << 20),
        name="finish",
    )(layer, rows, req, sums)


def solution(mesh):
    rows = P(("dp", "cp"), None)
    return jax.shard_map(
        local,
        mesh=mesh,
        in_specs=(rows, P(("dp", "cp")), rows, rows, P(), P(), P(), rows),
        out_specs=(rows, rows, rows, P(), P(), P()),
        check_vma=False,
    )
```

```python
import math

import jax
import jax.numpy as jnp
from jax import lax
from jax.experimental import pallas as pl
from jax.experimental.pallas import tpu as pltpu
from jax.sharding import PartitionSpec as P

MESH = pl.DeviceIdType.MESH
BF = jnp.bfloat16
F32 = jnp.float32
I32 = jnp.int32
EPSILON = 1e-05

D = 512
HEADS = 8
HEAD = 64
TOK = 128
CAP = 4
HOT = 512
COLD = 2048
COLD_W = 128
N_DP = 8
N_CP = 16
DEVICES = N_DP * N_CP
SLOT = 16
SLOTS = DEVICES * SLOT
SHIFT = 4096
CHUNK = 256
PAIRS = HEADS * (HEADS + 1) // 2
W_ROWS = 4 * D + D + COLD_W
LATE = 2 * D
SETS = (
    (0, 512, (48, 48, 32), (0, 48, 96)),
    (LATE, 832, (64, 64, 80), (128, 192, 256)),
)
PART_ROWS = 336
FAR_FIRST = sorted(
    (
        (dz, dc, dx, dy)
        for dz in range(4)
        for dc in range(2)
        for dx in range(4)
        for dy in range(4)
        if dz or dc or dx or dy
    ),
    key=lambda o: (-sum(min(v, 4 - v) for v in (o[0], o[2], o[3])), sum(o) * 53 % 7, o),
)


def nn(a, b):
    return jnp.dot(a, b, preferred_element_type=F32)


def nt(a, b, precision=None):
    return lax.dot_general(
        a, b, (((1,), (1,)), ((), ())), preferred_element_type=F32, precision=precision
    )


def sigmoid(v):
    return 0.5 * jnp.tanh(0.5 * v) + 0.5


def silu_slope(v):
    sig = sigmoid(v)
    return sig + v * sig * (1.0 - sig)


def iota(shape, dim):
    return lax.broadcasted_iota(I32, shape, dim)


def turned(v):
    return v.astype(F32).T


def column_norm(v):
    average = jnp.mean(v, axis=0, keepdims=True)
    centred = v - average
    inverse = lax.rsqrt(jnp.mean(centred * centred, axis=0, keepdims=True) + EPSILON)
    return centred * inverse, inverse


def column_norm_back(g, y, inverse):
    first = jnp.mean(g, axis=0, keepdims=True)
    second = jnp.mean(g * y, axis=0, keepdims=True)
    return (g - first - y * second) * inverse


def step_kernel(
    owner_in, slot_in, hot_hbm, cold_hbm, proj_hbm, joined_hbm, wout_hbm, cot_hbm,
    layer_out, rows_out, req_out, total,
    hot, cold, cold_wide, proj, joined, wout, cot, owner_ref, slot_ref, code_row,
    ids_all, pick32, pick16, row_in, take_1h, rows_got, emb_nat, normed_t, inv_ref, cold_t, joined_t,
    hidden_t, active_t, dgated_t, cot_t, slots_1h,
    k_in, v_in, q_in, kv_nat, w_keep, slope_keep, att_out, att_in, da_out, da_in,
    dk_acc, dv_acc, dq_out, dk_out, dv_out, dq_in, dk_in, dv_in, dh_t, pack_ref, grad_out, grad_in,
    w_ref, r0, u1, r1, u2, r2, r3, g2,
    send, recv, da_recv, ar_send, ar_recv, local_sem,
):
    dp, cp = lax.axis_index("dp"), lax.axis_index("cp")
    me = dp * N_CP + cp
    z, core, x, y = dp // 2, dp % 2, cp // 4, cp % 4
    head = cp // 2
    half = ((cp + 1) // 2) % 2
    xs, ys, zs = ([(v + d) % 4 for d in range(4)] for v in (x, y, z))
    cores = [core, (core + 1) % 2]
    dps = [[zs[dz] * 2 + cores[dc] for dc in range(2)] for dz in range(4)]
    cps = [[xs[dx] * 4 + ys[dy] for dy in range(4)] for dx in range(4)]
    plane = [(dx, dy) for dx in range(4) for dy in range(4) if dx or dy]
    plane.sort(key=lambda o: (-(min(o[0], 4 - o[0]) + min(o[1], 4 - o[1])), (o[0] * 3 + o[1]) % 4))

    def remote(src, dst, send_sem, recv_sem, to):
        return pltpu.make_async_remote_copy(
            src_ref=src, dst_ref=dst, send_sem=send_sem, recv_sem=recv_sem,
            device_id=to, device_id_type=MESH,
        )

    def wait_sent(ref, i):
        remote(ref, ref, send.at[i], recv.at[i], (dp, cp)).wait_send()

    def wait_got(ref, i):
        remote(ref, ref, send.at[i], recv.at[i], (dp, cp)).wait_recv()

    def rows64(h):
        return pl.ds(pl.multiple_of(h * HEAD, HEAD), HEAD)

    def tile(o):
        return pl.ds(pl.multiple_of(o * SLOT, SLOT), SLOT)

    def by_rank(tiles, rows):
        pick32[...] = tiles[...].astype(F32)
        for c in range(CAP):
            for f in range(4):
                rows[c * DEVICES : (c + 1) * DEVICES, f * 128 : (f + 1) * 128] = pick32[
                    pl.ds(CAP * f + c, DEVICES, stride=SLOT), :
                ].astype(BF)

    barrier = pltpu.get_barrier_semaphore()
    everyone = [(dps[dz][dc], cps[dx][dy]) for dz, dc, dx, dy in FAR_FIRST]
    for to in everyone:
        pl.semaphore_signal(barrier, inc=1, device_id=to, device_id_type=MESH)
    loads = [
        pltpu.make_async_copy(src, dst, local_sem.at[i])
        for i, (src, dst) in enumerate(
            ((owner_in, owner_ref), (slot_in, slot_ref), (joined_hbm, joined), (cot_hbm, cot), (wout_hbm, wout), (hot_hbm, hot),
             (cold_hbm, cold), (proj_hbm, proj))
        )
    ]
    for load in loads:
        load.start()
    for load in loads[:2]:
        load.wait()
    owner_row, slot_row = owner_ref[...], slot_ref[...]
    code_row[...] = owner_row * SHIFT + slot_row
    pl.semaphore_wait(barrier, DEVICES - 1)

    for to in everyone:
        remote(code_row, ids_all.at[me], send.at[0], recv.at[0], to).start()
    ids_all[pl.ds(me, 1)] = code_row[...].reshape(1, 1, TOK)

    diagonal = iota((TOK, TOK), 0) == iota((TOK, TOK), 1)

    def as_column(row):
        picked = jnp.where(diagonal, row.astype(F32), 0.0)
        return jnp.sum(picked, axis=1, keepdims=True).astype(I32)

    owner_col, slot_col = as_column(owner_row), as_column(slot_row)
    before_row = (owner_col == owner_row) & (iota((TOK, TOK), 0) < iota((TOK, TOK), 1))
    rank_row = jnp.sum(jnp.where(before_row, 1, 0), axis=0, keepdims=True)
    place_row = owner_row * SLOT + rank_row
    take_1h[...] = jnp.where(
        iota((TOK, CAP * DEVICES), 1) == as_column(rank_row) * DEVICES + owner_col, 1.0, 0.0
    ).astype(BF)
    for f in range(4):
        slots_1h[:, f * TOK : (f + 1) * TOK] = jnp.where(
            iota((SLOTS, TOK), 0) == place_row + CAP * f, 1.0, 0.0
        ).astype(BF)
    for load in loads[2:5]:
        load.wait()
    for b in range(4):
        joined_t[b * D : (b + 1) * D, :] = turned(joined[:, b * D : (b + 1) * D]).astype(BF)
    cot_t[...] = turned(cot[...])
    dgated_t[...] = nn(wout[...], cot_t[...].astype(BF))
    for load in loads[5:]:
        load.wait()
    for g in range(4):
        cold_wide[:, g * 128 : (g + 1) * 128] = cold[g * HOT : (g + 1) * HOT, :]

    wait_got(ids_all.at[pl.ds(0, DEVICES - 1)], 0)

    ids = ids_all[:, 0, :]
    asked = (ids // SHIFT) == me
    slot_plus = ((ids % SHIFT) + 1).astype(F32)
    upper = jnp.where(iota((TOK, TOK), 0) < iota((TOK, TOK), 1), 1.0, 0.0).astype(BF)
    earlier = nn(jnp.where(asked, 1.0, 0.0).astype(BF), upper)
    asks = [jnp.where(asked & (earlier == float(c)), slot_plus, 0.0) for c in range(CAP)]
    for c in range(CAP):
        wanted = jnp.sum(asks[c], axis=1, keepdims=True).astype(I32) - 1
        group = jnp.where(wanted < 0, -1, wanted // HOT)
        row = jnp.where(wanted < 0, -1, wanted % HOT)
        chosen = jnp.where(iota((DEVICES, HOT), 1) == row, 1.0, 0.0).astype(BF)
        hot_rows = nn(chosen, hot[...])
        cold_rows = nn(chosen, cold_wide[...])
        for f in range(4):
            part = jnp.where(group == 0, hot_rows[:, f * 128 : (f + 1) * 128], 0.0)
            if f == 0:
                for g in range(4):
                    part = jnp.where(group == g + 1, cold_rows[:, g * 128 : (g + 1) * 128], part)
            pick32[pl.ds(CAP * f + c, DEVICES, stride=SLOT), :] = part
    pick16[...] = pick32[...].astype(BF)

    for to in everyone:
        remote(
            pick16.at[tile(to[0] * N_CP + to[1])], row_in.at[tile(me)], send.at[1], recv.at[1], to
        ).start()
    row_in[tile(me), :] = pick16[tile(me), :]
    req_out[...] = jnp.zeros(req_out.shape, I32)
    for c in range(CAP):
        wanted_row = jnp.sum(asks[c].T, axis=0, keepdims=True)
        req_out[c : c + 1, :] = wanted_row.astype(I32) - 1

    wait_got(row_in.at[pl.ds(0, SLOTS - SLOT)], 1)

    by_rank(row_in, rows_got)
    fetched = nn(take_1h[...], rows_got[...])
    cold_vec = fetched[:, 0:COLD_W]
    cold_embed = nn(cold_vec.astype(BF), proj[...])
    embedded = jnp.where(slot_col < HOT, fetched, cold_embed)
    emb_nat[...] = embedded
    normed, inverse = column_norm(embedded.T)
    normed_t[...] = normed
    inv_ref[...] = jnp.broadcast_to(inverse, inv_ref.shape)
    low = normed.astype(BF)

    def k_rows(h):
        return pl.ds(pl.multiple_of(3 * D + h * HEAD, HEAD), HEAD)

    def v_rows(h):
        return pl.ds(pl.multiple_of(D + h * HEAD, HEAD), HEAD)

    def q_rows(h):
        return pl.ds(pl.multiple_of(2 * D + h * HEAD, HEAD), HEAD)

    def same_half(d):
        h = (head + d) % HEADS
        return h, (dp, 2 * h + (half + h) % 2)

    def project(b):
        hid = nn(joined_t[b * D : (b + 1) * D, :], low)
        hidden_t[b * D : (b + 1) * D, :] = hid
        active_t[b * D : (b + 1) * D, :] = (hid * sigmoid(hid)).astype(BF)

    project(3)
    for dx, dy in plane:
        pcp = cps[dx][dy]
        remote(active_t.at[k_rows(pcp // 2)], k_in.at[cp], send.at[2], recv.at[2], (dp, pcp)).start()
    project(1)
    for dx, dy in plane:
        pcp = cps[dx][dy]
        remote(active_t.at[v_rows(pcp // 2)], v_in.at[cp], send.at[3], recv.at[3], (dp, pcp)).start()
    project(2)
    for d in range(1, HEADS):
        h, to = same_half(d)
        remote(active_t.at[q_rows(h)], q_in.at[head], send.at[4], recv.at[4], to).start()
    k_in[pl.ds(cp, 1)] = active_t[k_rows(head), :].reshape(1, HEAD, TOK)
    v_in[pl.ds(cp, 1)] = active_t[v_rows(head), :].reshape(1, HEAD, TOK)
    q_in[pl.ds(head, 1)] = active_t[q_rows(head), :].reshape(1, HEAD, TOK)
    project(0)
    cold_t[...] = jnp.where(slot_row < HOT, 0.0, cold_vec.T)
    wait_got(k_in.at[pl.ds(0, N_CP - 1)], 2)
    wait_got(v_in.at[pl.ds(0, N_CP - 1)], 3)
    wait_got(q_in.at[pl.ds(0, HEADS - 1)], 4)

    def block_of(i):
        return 4 * (i // 2) + (half if i % 2 == 0 else 3 - half)

    def pair(ref, c):
        return jnp.concatenate([ref[2 * c], ref[2 * c + 1]], axis=1)

    shrink = 0.5 / math.sqrt(HEAD)
    for i in range(HEADS - 1, -1, -1):
        q_nat = (turned(q_in[i]) * shrink).astype(BF)
        sums = jnp.zeros((HEAD, TOK), F32)
        for c in range(i + 1):
            s = nn(q_nat, pair(k_in, c))
            up = 1.0 + jnp.tanh(s)
            w = s * up
            slope = up + w * (2.0 - up)
            if c == i:
                ok = (iota((TOK, CHUNK), 1) + c * CHUNK) <= (
                    iota((TOK, CHUNK), 0) + block_of(i) * TOK
                )
                w = jnp.where(ok, w, 0.0)
                slope = jnp.where(ok, slope, 0.0)
            w = w.astype(BF)
            at = i * (i + 1) // 2 + c
            w_keep[at] = w
            slope_keep[at] = slope
            sums = sums + nt(pair(v_in, c), w)
        att_out[i] = sums.astype(BF)

        @pl.when(head != i)
        def _():
            remote(
                att_out.at[i], att_in.at[rows64(head)], send.at[5], recv.at[5], (dp, block_of(i))
            ).start()

    att_in[rows64(head), :] = att_out[pl.ds(head, 1)].reshape(HEAD, TOK)
    wait_got(att_in.at[pl.ds(0, D - HEAD)], 5)

    mixed, inv_mix = column_norm(att_in[...].astype(F32))
    gate = active_t[0:D, :].astype(F32)
    dgated = dgated_t[...]
    da_out[...] = column_norm_back(dgated * gate, mixed, inv_mix).astype(BF)
    for d in range(1, HEADS):
        h, to = same_half(d)
        remote(da_out.at[rows64(h)], da_in.at[head], send.at[6], da_recv.at[head], to).start()
    da_in[pl.ds(head, 1)] = da_out[rows64(head), :].reshape(1, HEAD, TOK)

    sibling = (z * 2 + (1 - core), cp)
    place = (x, y, z)

    def along(dim, d):
        moved = [xs[0], ys[0], zs[0]]
        moved[dim] = (xs, ys, zs)[dim][d]
        return moved[dim], (moved[2] * 2 + core, moved[0] * 4 + moved[1])

    def ar(src, dst, n, stage, k, to):
        return remote(src, dst, ar_send.at[n, stage, k], ar_recv.at[n, stage, k], to)

    def ar_got(ref, n, stage, k):
        ar(ref, ref, n, stage, k, (dp, cp)).wait_recv()

    def ar_sent(ref, n, stage, k):
        ar(ref, ref, n, stage, k, (dp, cp)).wait_send()

    def core_rows(n, c, first, count):
        base, rows = SETS[n][:2]
        return pl.ds(pl.multiple_of(base + c * rows + first, 16), count)

    def set_rows(n, first, count):
        return pl.ds(SETS[n][0] // 2 + first, count)

    def stage0(n, k, first, count):
        ar(
            w_ref.at[core_rows(n, 1 - core, first, count)], r0.at[set_rows(n, first, count)],
            n, 0, k, sibling,
        ).start()

    def stage1(n, k, first, count, colors):
        at = set_rows(n, first, count)
        ar_got(r0.at[at], n, 0, k)
        u1[at, :] = (
            w_ref[core_rows(n, core, first, count), :].astype(F32) + r0[at, :].astype(F32)
        ).astype(BF)
        for color in colors:
            start1(n, color)

    def piece(n, k):
        return pl.ds(SETS[n][3][k], SETS[n][2][k])

    def u1_rows(n, k, a):
        part = SETS[n][2][k]
        return pl.ds(
            pl.multiple_of(SETS[n][0] // 2 + sum(SETS[n][2][:k]) * 4 + a * part, 16), part
        )

    def start1(n, k):
        for d in (2, 1, 3):
            a, to = along(k, d)
            ar(u1.at[u1_rows(n, k, a)], r1.at[d - 1, piece(n, k)], n, 1, k, to).start()

    def stage2(n, k):
        at = piece(n, k)
        ar_got(r1.at[:, at], n, 1, k)
        part = u1[u1_rows(n, k, place[k]), :].astype(F32)
        for d in range(3):
            part = part + r1[d, at, :].astype(F32)
        for b in range(4):
            u2[b, at, :] = part[:, b * 128 : (b + 1) * 128].astype(BF)
        for d in (2, 1, 3):
            b, to = along((k + 1) % 3, d)
            ar(u2.at[b, at], r2.at[d - 1, at], n, 2, k, to).start()

    def stage3(n, k):
        at, rows = piece(n, k), SETS[n][2][k]
        ar_got(r2.at[:, at], n, 2, k)
        b_me, c_me = place[(k + 1) % 3], place[(k + 2) % 3]
        part = u2[pl.ds(b_me, 1), at, :].astype(F32)
        for d in range(3):
            part = part + r2[d : d + 1, at, :].astype(F32)
        r3[pl.ds(c_me, 1), at, :] = part.astype(BF)
        for d in (2, 1, 3):
            _, to = along((k + 2) % 3, d)
            ar(r3.at[c_me, at], r3.at[c_me, at], n, 3, k, to).start()

    def stage4(n, k):
        at = piece(n, k)
        ar_got(r3.at[pl.ds(0, 3), at], n, 3, k)
        b_me = place[(k + 1) % 3]
        part = r3[0:1, at, :].astype(F32)
        for d in range(1, 4):
            part = part + r3[d : d + 1, at, :].astype(F32)
        g2[pl.ds(b_me, 1), at, :] = part.astype(BF)
        for d in (2, 1, 3):
            _, to = along((k + 1) % 3, d)
            ar(g2.at[b_me, at], g2.at[b_me, at], n, 4, k, to).start()

    def stage5(n, k):
        at = piece(n, k)
        ar_got(g2.at[pl.ds(0, 3), at], n, 4, k)
        a_me = place[k]
        for d in (2, 1, 3):
            _, to = along(k, d)
            ar(g2.at[:, at], total.at[core, a_me, :, at], n, 5, k, to).start()
        total[pl.ds(core, 1), pl.ds(a_me, 1), :, at, :] = g2[:, at, :].reshape(
            1, 1, 4, SETS[n][2][k], 128
        )

    def stage6(n, k):
        at = piece(n, k)
        ar_got(total.at[0, pl.ds(0, 3), :, at], n, 5, k)
        ar(total.at[core, :, :, at], total.at[core, :, :, at], n, 6, k, sibling).start()

    def stage7(n, k):
        ar_got(total.at[0, :, :, piece(n, k)], n, 6, k)

    def all_colors(stage, n):
        for k in range(3):
            stage(n, k)

    def settle(n, firsts):
        for k, count in firsts:
            ar_sent(r0.at[pl.ds(0, count)], n, 0, k)
        for k in range(3):
            at = piece(n, k)
            ar_sent(r1.at[:, at], n, 1, k)
            ar_sent(r2.at[:, at], n, 2, k)
            ar_sent(r3.at[pl.ds(0, 3), at], n, 3, k)
            ar_sent(g2.at[pl.ds(0, 3), at], n, 4, k)
            ar_sent(total.at[0, pl.ds(0, 3), :, at], n, 5, k)
            ar_sent(total.at[0, :, :, at], n, 6, k)

    gated = (mixed * gate).astype(BF)
    low = normed_t[...].astype(BF)
    dh_gate = (dgated * mixed * silu_slope(hidden_t[0:D, :])).astype(BF)
    dh_t[0:D, :] = dh_gate
    w_ref[0:D, :] = nt(low, dh_gate).astype(BF)
    w_ref[D : 2 * D, :] = nn(gated, cot[...]).astype(BF)
    stage0(0, 0, 0, D)
    branch = nn(turned(gated).astype(BF), wout[...])
    layer_out[...] = (emb_nat[...] + branch).astype(BF)

    for b in range(N_CP):
        kv_nat[b * TOK : (b + 1) * TOK, :] = turned(
            jnp.concatenate([k_in[b], v_in[b]], axis=0)
        ).astype(BF)

    for i in range(HEADS - 1, -1, -1):

        @pl.when(head != i)
        def _():
            remote(
                da_in.at[i], da_in.at[i], send.at[6], da_recv.at[i], (dp, cp)
            ).wait_recv()

        da_t, q_t = da_in[i], q_in[i]
        da_nat = (turned(da_t) * shrink).astype(BF)
        dq = jnp.zeros((TOK, 2 * HEAD), F32)
        for c in range(i + 1):
            at = i * (i + 1) // 2 + c
            ds = (nn(da_nat, pair(v_in, c)) * slope_keep[at]).astype(BF)
            dq = dq + nn(ds, kv_nat[c * CHUNK : (c + 1) * CHUNK, :])
            dk, dv = nn(q_t, ds), nn(da_t, w_keep[at])
            if i < HEADS - 1:
                dk, dv = dk + dk_acc[c], dv + dv_acc[c]
            if c < i:
                dk_acc[c], dv_acc[c] = dk, dv
        dq_out[i] = dq.T[:HEAD, :].astype(BF)
        dk, dv = dk.astype(BF), dv.astype(BF)
        for b in range(2):
            kb = 2 * i + b
            dk_out[kb] = dk[:, b * TOK : (b + 1) * TOK]
            dv_out[kb] = dv[:, b * TOK : (b + 1) * TOK]

            @pl.when(cp != kb)
            def _():
                remote(
                    dk_out.at[kb], dk_in.at[half, rows64(head)], send.at[7], recv.at[7], (dp, kb)
                ).start()
                remote(
                    dv_out.at[kb], dv_in.at[half, rows64(head)], send.at[8], recv.at[8], (dp, kb)
                ).start()

        @pl.when(head != i)
        def _():
            remote(
                dq_out.at[i], dq_in.at[rows64(head)], send.at[9], recv.at[9], (dp, block_of(i))
            ).start()

        if i == HEADS - 1:
            stage1(0, 0, 0, D, (0, 1, 2))
    all_colors(stage2, 0)
    all_colors(stage3, 0)

    dq_in[rows64(head), :] = dq_out[pl.ds(head, 1)].reshape(HEAD, TOK)
    dk_in[pl.ds(half, 1), rows64(head), :] = dk_out[pl.ds(cp, 1)]
    dv_in[pl.ds(half, 1), rows64(head), :] = dv_out[pl.ds(cp, 1)]
    wait_got(dk_out.at[pl.ds(0, N_CP - 1)], 7)
    wait_got(dv_out.at[pl.ds(0, N_CP - 1)], 8)
    wait_got(dq_in.at[pl.ds(0, D - HEAD)], 9)

    def column_back(b, grad):
        dh = (grad * silu_slope(hidden_t[b * D : (b + 1) * D, :])).astype(BF)
        dh_t[b * D : (b + 1) * D, :] = dh
        grads = nt(low, dh).astype(BF)
        if b == 1:
            w_ref[LATE : LATE + D, :] = grads
        elif b == 2:
            w_ref[LATE + D : LATE + 768, :] = grads[0:256]
            w_ref[LATE + 832 : LATE + 1088, :] = grads[256:512]
        else:
            w_ref[LATE + 1088 : LATE + 1600, :] = grads

    column_back(1, dv_in[0].astype(F32) + dv_in[1].astype(F32))
    column_back(2, dq_in[...].astype(F32))
    column_back(3, dk_in[0].astype(F32) + dk_in[1].astype(F32))
    stage0(1, 0, 0, 768)
    dnormed = nn(joined[...], dh_t[...])
    dembed = column_norm_back(dnormed, normed_t[...], inv_ref[0:1, :]) + cot_t[...]
    exact = lax.Precision.HIGHEST
    stage1(1, 0, 0, 768, (0, 1))
    proj_grads = nt(cold_t[...], dembed, exact).astype(BF)
    w_ref[LATE + 768 : LATE + 832, :] = proj_grads[0:64]
    w_ref[LATE + 1600 : LATE + 1664, :] = proj_grads[64:128]
    stage0(1, 1, 768, 64)

    cold_event = lax.dot_general(
        proj[...].astype(F32), dembed, (((1,), (0,)), ((), ())),
        preferred_element_type=F32, precision=exact,
    )
    is_hot = slot_row < HOT
    for f in range(4):
        part = dembed[f * 128 : (f + 1) * 128, :]
        pack_ref[:, f * TOK : (f + 1) * TOK] = jnp.where(
            is_hot, part, cold_event if f == 0 else 0.0
        ).astype(BF)
    grad_out[...] = nt(slots_1h[...], pack_ref[...]).astype(BF)
    grad_in[tile(me), :] = grad_out[tile(me), :]

    def send_grads(group):
        for to in everyone[group::4]:
            remote(
                grad_out.at[tile(to[0] * N_CP + to[1])], grad_in.at[tile(me)],
                send.at[10], recv.at[10], to,
            ).start()

    stage1(1, 1, 768, 64, (2,))
    all_colors(stage4, 0)
    all_colors(stage2, 1)
    all_colors(stage5, 0)
    all_colors(stage3, 1)
    send_grads(0)
    send_grads(1)
    all_colors(stage4, 1)
    send_grads(2)
    send_grads(3)
    all_colors(stage5, 1)
    all_colors(stage6, 0)

    wait_got(grad_in.at[pl.ds(0, SLOTS - SLOT)], 10)
    by_rank(grad_in, rows_out)

    wait_sent(ids_all.at[pl.ds(0, DEVICES - 1)], 0)
    wait_sent(row_in.at[pl.ds(0, SLOTS - SLOT)], 1)
    wait_sent(k_in.at[pl.ds(0, N_CP - 1)], 2)
    wait_sent(v_in.at[pl.ds(0, N_CP - 1)], 3)
    wait_sent(q_in.at[pl.ds(0, HEADS - 1)], 4)
    wait_sent(att_in.at[pl.ds(0, D - HEAD)], 5)
    wait_sent(da_in.at[pl.ds(0, HEADS - 1)], 6)
    wait_sent(dk_out.at[pl.ds(0, N_CP - 1)], 7)
    wait_sent(dv_out.at[pl.ds(0, N_CP - 1)], 8)
    wait_sent(dq_in.at[pl.ds(0, D - HEAD)], 9)
    wait_sent(grad_in.at[pl.ds(0, SLOTS - SLOT)], 10)
    settle(0, ((0, D),))
    all_colors(stage6, 1)
    all_colors(stage7, 0)
    all_colors(stage7, 1)
    settle(1, ((0, 768), (1, 64)))


def finish_kernel(
    layer, rows, req, sums,
    layer_out, hot_out, cold_out, proj_out, joined_out, wout_out,
    hot_buf, cold_buf, sum_buf, sem,
):
    copies = []

    def put(src, dst):
        copy = pltpu.make_async_copy(src, dst, sem.at[len(copies)])
        copy.start()
        copies.append(copy)

    put(layer, layer_out)
    picked = rows[...]

    def onehot(rows_here, first):
        index = iota((rows_here, DEVICES), 0) + first
        return jnp.concatenate(
            [jnp.where(index == req[c : c + 1, :], 1.0, 0.0).astype(BF) for c in range(CAP)],
            axis=1,
        )

    hot_buf[...] = nn(onehot(HOT, 0), picked)
    put(hot_buf, hot_out)
    low = picked[:, 0:COLD_W]
    for t in range(4):
        part = pl.ds(t * (COLD // 4), COLD // 4)
        cold_buf[part, :] = nn(onehot(COLD // 4, HOT + t * (COLD // 4)), low)
        put(cold_buf.at[part], cold_out.at[part])

    scale = (TOK * DEVICES) ** -0.5
    for core in range(2):
        for n in range(2):
            for k in range(3):
                count, at = SETS[n][2][k], SETS[n][3][k]
                for a in range(4):
                    first = sum(SETS[n][2][:k]) * 4 + a * count
                    for source, target, length in targets(n, core, first, count):
                        for b in range(4):
                            sum_buf[target : target + length, b * 128 : (b + 1) * 128] = (
                                sums[core, a, b, at + source : at + source + length, :].astype(F32)
                                * scale
                            )
        if core == 0:
            for b in (0, 1):
                put(sum_buf.at[pl.ds(b * D, D)], joined_out.at[:, pl.ds(b * D, D)])
    for b in (2, 3):
        put(sum_buf.at[pl.ds(b * D, D)], joined_out.at[:, pl.ds(b * D, D)])
    put(sum_buf.at[pl.ds(4 * D, D)], wout_out)
    put(sum_buf.at[pl.ds(5 * D, COLD_W)], proj_out)
    for copy in copies:
        copy.wait()


def targets(n, core, first, count):
    if n == 0:
        return [(0, (4 * D if core else 0) + first, count)]
    runs = []
    if first < 768:
        length = min(count, 768 - first)
        runs.append((0, D + core * 768 + first, length))
    if first + count > 768:
        start = max(first, 768)
        runs.append((start - first, 5 * D + core * 64 + start - 768, first + count - start))
    return runs


def vmem(n):
    return [pl.BlockSpec(memory_space=pltpu.VMEM)] * n


def anywhere(n):
    return [pl.BlockSpec(memory_space=pl.ANY)] * n


def hbm(n):
    return [pl.BlockSpec(memory_space=pltpu.HBM)] * n


def local(row_owner, slot_row, hot, cold, proj, joined, wout, cot):
    v = pltpu.VMEM
    operands = [row_owner.reshape(1, TOK), slot_row.reshape(1, TOK)]
    operands += [hot, cold, proj, joined, wout, cot]
    operands = [pltpu.with_memory_space_constraint(a, pltpu.HBM) for a in operands]
    layer, rows, req, sums = pl.pallas_call(
        step_kernel,
        out_shape=(
            jax.ShapeDtypeStruct((TOK, D), BF),
            jax.ShapeDtypeStruct((CAP * DEVICES, D), BF),
            jax.ShapeDtypeStruct((8, DEVICES), I32),
            jax.ShapeDtypeStruct((2, 4, 4, PART_ROWS, 128), BF),
        ),
        in_specs=hbm(8),
        out_specs=tuple(vmem(4)),
        scratch_shapes=[
            v((HOT, D), BF), v((COLD, COLD_W), BF), v((HOT, 4 * COLD_W), BF),
            v((COLD_W, D), BF), v((D, 4 * D), BF),
            v((D, D), BF), v((TOK, D), BF), v((1, TOK), I32), v((1, TOK), I32),
            v((1, TOK), I32),
            v((DEVICES, 1, TOK), I32), v((SLOTS, 128), F32), v((SLOTS, 128), BF),
            v((SLOTS, 128), BF), v((TOK, CAP * DEVICES), BF), v((CAP * DEVICES, D), BF),
            v((TOK, D), F32), v((D, TOK), F32), v((8, TOK), F32),
            v((COLD_W, TOK), F32), v((4 * D, D), BF),
            v((4 * D, TOK), F32), v((4 * D, TOK), BF), v((D, TOK), F32), v((D, TOK), F32),
            v((SLOTS, 4 * TOK), BF),
            v((N_CP, HEAD, TOK), BF), v((N_CP, HEAD, TOK), BF), v((HEADS, HEAD, TOK), BF),
            v((N_CP * TOK, 2 * HEAD), BF),
            v((PAIRS, TOK, CHUNK), BF), v((PAIRS, TOK, CHUNK), F32),
            v((HEADS, HEAD, TOK), BF), v((D, TOK), BF), v((D, TOK), BF),
            v((HEADS, HEAD, TOK), BF),
            v((HEADS, HEAD, CHUNK), F32), v((HEADS, HEAD, CHUNK), F32),
            v((HEADS, HEAD, TOK), BF),
            v((N_CP, HEAD, TOK), BF), v((N_CP, HEAD, TOK), BF),
            v((D, TOK), BF), v((2, D, TOK), BF), v((2, D, TOK), BF),
            v((4 * D, TOK), BF), v((128, 4 * TOK), BF),
            v((SLOTS, 128), BF), v((SLOTS, 128), BF),
            v((W_ROWS, D), BF), v((W_ROWS // 2, D), BF), v((W_ROWS // 2, D), BF),
            v((3, PART_ROWS, D), BF), v((4, PART_ROWS, 128), BF),
            v((3, PART_ROWS, 128), BF), v((4, PART_ROWS, 128), BF),
            v((4, PART_ROWS, 128), BF),
            pltpu.SemaphoreType.DMA((11,)), pltpu.SemaphoreType.DMA((11,)),
            pltpu.SemaphoreType.DMA((HEADS,)),
            pltpu.SemaphoreType.DMA((2, 7, 3)), pltpu.SemaphoreType.DMA((2, 7, 3)),
            pltpu.SemaphoreType.DMA((8,)),
        ],
        compiler_params=pltpu.CompilerParams(
            collective_id=0, has_side_effects=True, vmem_limit_bytes=44 << 20
        ),
        name="step",
    )(*operands)
    return pl.pallas_call(
        finish_kernel,
        out_shape=(
            jax.ShapeDtypeStruct((TOK, D), BF),
            jax.ShapeDtypeStruct((HOT, D), F32),
            jax.ShapeDtypeStruct((COLD, COLD_W), F32),
            jax.ShapeDtypeStruct((COLD_W, D), F32),
            jax.ShapeDtypeStruct((D, 4 * D), F32),
            jax.ShapeDtypeStruct((D, D), F32),
        ),
        in_specs=vmem(4),
        out_specs=tuple(hbm(6)),
        scratch_shapes=[
            v((HOT, D), F32), v((COLD, COLD_W), F32), v((W_ROWS, D), F32),
            pltpu.SemaphoreType.DMA((12,)),
        ],
        compiler_params=pltpu.CompilerParams(vmem_limit_bytes=20 << 20),
        name="finish",
    )(layer, rows, req, sums)


def solution(mesh):
    rows = P(("dp", "cp"), None)
    return jax.shard_map(
        local,
        mesh=mesh,
        in_specs=(rows, P(("dp", "cp")), rows, rows, P(), P(), P(), rows),
        out_specs=(rows, rows, rows, P(), P(), P()),
        check_vma=False,
    )
```

```python
import math

import jax
import jax.numpy as jnp
from jax import lax
from jax.experimental import pallas as pl
from jax.experimental.pallas import tpu as pltpu
from jax.sharding import PartitionSpec as P

MESH = pl.DeviceIdType.MESH
BF = jnp.bfloat16
F32 = jnp.float32
I32 = jnp.int32
EPSILON = 1e-05

D = 512
HEADS = 8
HEAD = 64
TOK = 128
CAP = 4
HOT = 512
COLD = 2048
COLD_W = 128
N_DP = 8
N_CP = 16
DEVICES = N_DP * N_CP
SLOT = 16
SLOTS = DEVICES * SLOT
SHIFT = 4096
CHUNK = 256
PAIRS = HEADS * (HEADS + 1) // 2
W_ROWS = 4 * D + D + COLD_W
LATE = 2 * D
SETS = (
    (0, D, 0, D, {0: (48, 0), 1: (48, 48), 2: (32, 96)}),
    (LATE, 832, D, 768, {0: (64, 128), 1: (64, 192), 2: (64, 256)}),
    (LATE + 768, 832, D + 768, 64, {2: (16, 320)}),
)
PART_ROWS = 336


def first_row(n, k):
    return sum(4 * part for color, (part, _) in SETS[n][4].items() if color < k)


FAR_FIRST = sorted(
    (
        (dz, dc, dx, dy)
        for dz in range(4)
        for dc in range(2)
        for dx in range(4)
        for dy in range(4)
        if dz or dc or dx or dy
    ),
    key=lambda o: (-sum(min(v, 4 - v) for v in (o[0], o[2], o[3])), sum(o) * 53 % 7, o),
)


def nn(a, b):
    return jnp.dot(a, b, preferred_element_type=F32)


def nt(a, b, precision=None):
    return lax.dot_general(
        a, b, (((1,), (1,)), ((), ())), preferred_element_type=F32, precision=precision
    )


def sigmoid(v):
    return 0.5 * jnp.tanh(0.5 * v) + 0.5


def silu_slope(v):
    sig = sigmoid(v)
    return sig + v * sig * (1.0 - sig)


def iota(shape, dim):
    return lax.broadcasted_iota(I32, shape, dim)


def turned(v):
    return v.astype(F32).T


def column_norm(v):
    average = jnp.mean(v, axis=0, keepdims=True)
    centred = v - average
    inverse = lax.rsqrt(jnp.mean(centred * centred, axis=0, keepdims=True) + EPSILON)
    return centred * inverse, inverse


def column_norm_back(g, y, inverse):
    first = jnp.mean(g, axis=0, keepdims=True)
    second = jnp.mean(g * y, axis=0, keepdims=True)
    return (g - first - y * second) * inverse


def step_kernel(
    owner_in, slot_in, hot_hbm, cold_hbm, proj_hbm, joined_hbm, wout_hbm, cot_hbm,
    layer_out, rows_out, req_out, total,
    hot, cold, cold_wide, proj, joined, wout, cot, owner_ref, slot_ref, code_row,
    ids_all, pick32, pick16, row_in, take_1h, rows_got, emb_nat, normed_t, inv_ref, cold_t, joined_t,
    hidden_t, active_t, dgated_t, cot_t, slots_1h,
    k_in, v_in, q_in, kv_nat, w_keep, slope_keep, att_out, att_in, da_out, da_in,
    da_nat, da_cat, q_cat, dq_acc, dq_out, dk_out, dv_out, dq_in, dk_in, dv_in, dh_t, pack_ref, grad_out, grad_in,
    w_ref, r0, u1, r1, u2, r2, r3, g2,
    send, recv, da_recv, ar_send, ar_recv, last_recv, local_sem,
):
    dp, cp = lax.axis_index("dp"), lax.axis_index("cp")
    me = dp * N_CP + cp
    z, core, x, y = dp // 2, dp % 2, cp // 4, cp % 4
    head = cp // 2
    half = ((cp + 1) // 2) % 2
    xs, ys, zs = ([(v + d) % 4 for d in range(4)] for v in (x, y, z))
    cores = [core, (core + 1) % 2]
    dps = [[zs[dz] * 2 + cores[dc] for dc in range(2)] for dz in range(4)]
    cps = [[xs[dx] * 4 + ys[dy] for dy in range(4)] for dx in range(4)]
    plane = [(dx, dy) for dx in range(4) for dy in range(4) if dx or dy]
    plane.sort(key=lambda o: (-(min(o[0], 4 - o[0]) + min(o[1], 4 - o[1])), (o[0] * 3 + o[1]) % 4))

    def remote(src, dst, send_sem, recv_sem, to):
        return pltpu.make_async_remote_copy(
            src_ref=src, dst_ref=dst, send_sem=send_sem, recv_sem=recv_sem,
            device_id=to, device_id_type=MESH,
        )

    def wait_sent(ref, i):
        remote(ref, ref, send.at[i], recv.at[i], (dp, cp)).wait_send()

    def wait_got(ref, i):
        remote(ref, ref, send.at[i], recv.at[i], (dp, cp)).wait_recv()

    def rows64(h):
        return pl.ds(pl.multiple_of(h * HEAD, HEAD), HEAD)

    def tile(o):
        return pl.ds(pl.multiple_of(o * SLOT, SLOT), SLOT)

    def by_rank(tiles, rows):
        pick32[...] = tiles[...].astype(F32)
        for c in range(CAP):
            for f in range(4):
                rows[c * DEVICES : (c + 1) * DEVICES, f * 128 : (f + 1) * 128] = pick32[
                    pl.ds(CAP * f + c, DEVICES, stride=SLOT), :
                ].astype(BF)

    barrier = pltpu.get_barrier_semaphore()
    everyone = [(dps[dz][dc], cps[dx][dy]) for dz, dc, dx, dy in FAR_FIRST]
    for to in everyone:
        pl.semaphore_signal(barrier, inc=1, device_id=to, device_id_type=MESH)
    loads = [
        pltpu.make_async_copy(src, dst, local_sem.at[i])
        for i, (src, dst) in enumerate(
            ((owner_in, owner_ref), (slot_in, slot_ref), (joined_hbm, joined), (cot_hbm, cot), (wout_hbm, wout), (hot_hbm, hot),
             (cold_hbm, cold), (proj_hbm, proj))
        )
    ]
    for load in loads:
        load.start()
    for load in loads[:2]:
        load.wait()
    owner_row, slot_row = owner_ref[...], slot_ref[...]
    code_row[...] = owner_row * SHIFT + slot_row
    pl.semaphore_wait(barrier, DEVICES - 1)

    for to in everyone:
        remote(code_row, ids_all.at[me], send.at[0], recv.at[0], to).start()
    ids_all[pl.ds(me, 1)] = code_row[...].reshape(1, 1, TOK)

    diagonal = iota((TOK, TOK), 0) == iota((TOK, TOK), 1)

    def as_column(row):
        picked = jnp.where(diagonal, row.astype(F32), 0.0)
        return jnp.sum(picked, axis=1, keepdims=True).astype(I32)

    owner_col, slot_col = as_column(owner_row), as_column(slot_row)
    before_row = (owner_col == owner_row) & (iota((TOK, TOK), 0) < iota((TOK, TOK), 1))
    rank_row = jnp.sum(jnp.where(before_row, 1, 0), axis=0, keepdims=True)
    place_row = owner_row * SLOT + rank_row
    take_1h[...] = jnp.where(
        iota((TOK, CAP * DEVICES), 1) == as_column(rank_row) * DEVICES + owner_col, 1.0, 0.0
    ).astype(BF)
    for f in range(4):
        slots_1h[:, f * TOK : (f + 1) * TOK] = jnp.where(
            iota((SLOTS, TOK), 0) == place_row + CAP * f, 1.0, 0.0
        ).astype(BF)
    for load in loads[2:5]:
        load.wait()
    for b in range(4):
        joined_t[b * D : (b + 1) * D, :] = turned(joined[:, b * D : (b + 1) * D]).astype(BF)
    cot_t[...] = turned(cot[...])
    dgated_t[...] = nn(wout[...], cot_t[...].astype(BF))
    for load in loads[5:]:
        load.wait()
    for g in range(4):
        cold_wide[:, g * 128 : (g + 1) * 128] = cold[g * HOT : (g + 1) * HOT, :]

    wait_got(ids_all.at[pl.ds(0, DEVICES - 1)], 0)

    ids = ids_all[:, 0, :]
    asked = (ids // SHIFT) == me
    slot_plus = ((ids % SHIFT) + 1).astype(F32)
    upper = jnp.where(iota((TOK, TOK), 0) < iota((TOK, TOK), 1), 1.0, 0.0).astype(BF)
    earlier = nn(jnp.where(asked, 1.0, 0.0).astype(BF), upper)
    asks = [jnp.where(asked & (earlier == float(c)), slot_plus, 0.0) for c in range(CAP)]
    for c in range(CAP):
        wanted = jnp.sum(asks[c], axis=1, keepdims=True).astype(I32) - 1
        group = jnp.where(wanted < 0, -1, wanted // HOT)
        row = jnp.where(wanted < 0, -1, wanted % HOT)
        chosen = jnp.where(iota((DEVICES, HOT), 1) == row, 1.0, 0.0).astype(BF)
        hot_rows = nn(chosen, hot[...])
        cold_rows = nn(chosen, cold_wide[...])
        for f in range(4):
            part = jnp.where(group == 0, hot_rows[:, f * 128 : (f + 1) * 128], 0.0)
            if f == 0:
                for g in range(4):
                    part = jnp.where(group == g + 1, cold_rows[:, g * 128 : (g + 1) * 128], part)
            pick32[pl.ds(CAP * f + c, DEVICES, stride=SLOT), :] = part
    pick16[...] = pick32[...].astype(BF)

    for to in everyone:
        remote(
            pick16.at[tile(to[0] * N_CP + to[1])], row_in.at[tile(me)], send.at[1], recv.at[1], to
        ).start()
    row_in[tile(me), :] = pick16[tile(me), :]
    req_out[...] = jnp.zeros(req_out.shape, I32)
    for c in range(CAP):
        wanted_row = jnp.sum(asks[c].T, axis=0, keepdims=True)
        req_out[c : c + 1, :] = wanted_row.astype(I32) - 1

    wait_got(row_in.at[pl.ds(0, SLOTS - SLOT)], 1)

    by_rank(row_in, rows_got)
    fetched = nn(take_1h[...], rows_got[...])
    cold_vec = fetched[:, 0:COLD_W]
    cold_embed = nn(cold_vec.astype(BF), proj[...])
    embedded = jnp.where(slot_col < HOT, fetched, cold_embed)
    emb_nat[...] = embedded
    normed, inverse = column_norm(embedded.T)
    normed_t[...] = normed
    inv_ref[...] = jnp.broadcast_to(inverse, inv_ref.shape)
    low = normed.astype(BF)

    def k_rows(h):
        return pl.ds(pl.multiple_of(3 * D + h * HEAD, HEAD), HEAD)

    def v_rows(h):
        return pl.ds(pl.multiple_of(D + h * HEAD, HEAD), HEAD)

    def q_rows(h):
        return pl.ds(pl.multiple_of(2 * D + h * HEAD, HEAD), HEAD)

    def same_half(d):
        h = (head + d) % HEADS
        return h, (dp, 2 * h + (half + h) % 2)

    def project(b):
        hid = nn(joined_t[b * D : (b + 1) * D, :], low)
        hidden_t[b * D : (b + 1) * D, :] = hid
        active_t[b * D : (b + 1) * D, :] = (hid * sigmoid(hid)).astype(BF)

    project(3)
    for dx, dy in plane:
        pcp = cps[dx][dy]
        remote(active_t.at[k_rows(pcp // 2)], k_in.at[cp], send.at[2], recv.at[2], (dp, pcp)).start()
    project(1)
    for dx, dy in plane:
        pcp = cps[dx][dy]
        remote(active_t.at[v_rows(pcp // 2)], v_in.at[cp], send.at[3], recv.at[3], (dp, pcp)).start()
    project(2)
    for d in range(1, HEADS):
        h, to = same_half(d)
        remote(active_t.at[q_rows(h)], q_in.at[head], send.at[4], recv.at[4], to).start()
    k_in[pl.ds(cp, 1)] = active_t[k_rows(head), :].reshape(1, HEAD, TOK)
    v_in[pl.ds(cp, 1)] = active_t[v_rows(head), :].reshape(1, HEAD, TOK)
    q_in[pl.ds(head, 1)] = active_t[q_rows(head), :].reshape(1, HEAD, TOK)
    project(0)
    cold_t[...] = jnp.where(slot_row < HOT, 0.0, cold_vec.T)
    wait_got(k_in.at[pl.ds(0, N_CP - 1)], 2)
    wait_got(v_in.at[pl.ds(0, N_CP - 1)], 3)
    wait_got(q_in.at[pl.ds(0, HEADS - 1)], 4)

    def block_of(i):
        return 4 * (i // 2) + (half if i % 2 == 0 else 3 - half)

    def pair(ref, c):
        return jnp.concatenate([ref[2 * c], ref[2 * c + 1]], axis=1)

    def kept(c, i, count):
        at = sum(HEADS - b for b in range(c)) + i - c
        return pl.ds(at * TOK, count * TOK)

    shrink = 0.5 / math.sqrt(HEAD)
    for i in range(HEADS - 1, -1, -1):
        q_nat = (turned(q_in[i]) * shrink).astype(BF)
        sums = jnp.zeros((HEAD, TOK), F32)
        for c in range(i + 1):
            s = nn(q_nat, pair(k_in, c))
            up = 1.0 + jnp.tanh(s)
            w = s * up
            slope = up + w * (2.0 - up)
            if c == i:
                ok = (iota((TOK, CHUNK), 1) + c * CHUNK) <= (
                    iota((TOK, CHUNK), 0) + block_of(i) * TOK
                )
                w = jnp.where(ok, w, 0.0)
                slope = jnp.where(ok, slope, 0.0)
            w = w.astype(BF)
            w_keep[kept(c, i, 1), :] = w
            slope_keep[kept(c, i, 1), :] = slope
            sums = sums + nt(pair(v_in, c), w)
        att_out[i] = sums.astype(BF)

        @pl.when(head != i)
        def _():
            remote(
                att_out.at[i], att_in.at[rows64(head)], send.at[5], recv.at[5], (dp, block_of(i))
            ).start()

    att_in[rows64(head), :] = att_out[pl.ds(head, 1)].reshape(HEAD, TOK)
    wait_got(att_in.at[pl.ds(0, D - HEAD)], 5)

    mixed, inv_mix = column_norm(att_in[...].astype(F32))
    gate = active_t[0:D, :].astype(F32)
    dgated = dgated_t[...]
    da_out[...] = column_norm_back(dgated * gate, mixed, inv_mix).astype(BF)
    for d in range(1, HEADS):
        h, to = same_half(d)
        remote(da_out.at[rows64(h)], da_in.at[head], send.at[6], da_recv.at[head], to).start()
    da_in[pl.ds(head, 1)] = da_out[rows64(head), :].reshape(1, HEAD, TOK)

    sibling = (z * 2 + (1 - core), cp)
    place = (x, y, z)

    def along(dim, d):
        moved = [xs[0], ys[0], zs[0]]
        moved[dim] = (xs, ys, zs)[dim][d]
        return moved[dim], (moved[2] * 2 + core, moved[0] * 4 + moved[1])

    def ar(src, dst, n, stage, k, to):
        return remote(src, dst, ar_send.at[n, stage, k], ar_recv.at[n, stage, k], to)

    def ar_got(ref, n, stage, k):
        ar(ref, ref, n, stage, k, (dp, cp)).wait_recv()

    def ar_sent(ref, n, stage, k):
        ar(ref, ref, n, stage, k, (dp, cp)).wait_send()

    def core_rows(n, c):
        return pl.ds(pl.multiple_of(SETS[n][0] + c * SETS[n][1], 16), SETS[n][3])

    def set_rows(n):
        return pl.ds(SETS[n][2], SETS[n][3])

    def stage0(n):
        ar(w_ref.at[core_rows(n, 1 - core)], r0.at[set_rows(n)], n, 0, 0, sibling).start()

    def piece(n, k):
        part, at = SETS[n][4][k]
        return pl.ds(at, part)

    def u1_rows(n, k, a):
        part = SETS[n][4][k][0]
        return pl.ds(pl.multiple_of(SETS[n][2] + first_row(n, k) + a * part, 16), part)

    def stage1(n):
        at = set_rows(n)
        ar_got(r0.at[at], n, 0, 0)
        u1[at, :] = (w_ref[core_rows(n, core), :].astype(F32) + r0[at, :].astype(F32)).astype(BF)
        for k in SETS[n][4]:
            for d in (2, 1, 3):
                a, to = along(k, d)
                ar(u1.at[u1_rows(n, k, a)], r1.at[d - 1, piece(n, k)], n, 1, k, to).start()

    def stage2(n, k):
        at = piece(n, k)
        ar_got(r1.at[:, at], n, 1, k)
        part = u1[u1_rows(n, k, place[k]), :].astype(F32)
        for d in range(3):
            part = part + r1[d, at, :].astype(F32)
        for b in range(4):
            u2[b, at, :] = part[:, b * 128 : (b + 1) * 128].astype(BF)
        for d in (2, 1, 3):
            b, to = along((k + 1) % 3, d)
            ar(u2.at[b, at], r2.at[d - 1, at], n, 2, k, to).start()

    def stage3(n, k):
        at = piece(n, k)
        ar_got(r2.at[:, at], n, 2, k)
        b_me, c_me = place[(k + 1) % 3], place[(k + 2) % 3]
        part = u2[pl.ds(b_me, 1), at, :].astype(F32)
        for d in range(3):
            part = part + r2[d : d + 1, at, :].astype(F32)
        r3[pl.ds(c_me, 1), at, :] = part.astype(BF)
        for d in (2, 1, 3):
            _, to = along((k + 2) % 3, d)
            ar(r3.at[c_me, at], r3.at[c_me, at], n, 3, k, to).start()

    def stage4(n, k):
        at = piece(n, k)
        ar_got(r3.at[pl.ds(0, 3), at], n, 3, k)
        b_me = place[(k + 1) % 3]
        part = r3[0:1, at, :].astype(F32)
        for d in range(1, 4):
            part = part + r3[d : d + 1, at, :].astype(F32)
        g2[pl.ds(b_me, 1), at, :] = part.astype(BF)
        for d in (2, 1, 3):
            _, to = along((k + 1) % 3, d)
            ar(g2.at[b_me, at], g2.at[b_me, at], n, 4, k, to).start()

    def to_sibling(n, k, a):
        held = total.at[core, a, :, piece(n, k)]
        ar(held, held, n, 6, k, sibling).start()

    def stage5(n, k):
        at = piece(n, k)
        ar_got(g2.at[pl.ds(0, 3), at], n, 4, k)
        a_me = place[k]
        for d in (2, 1, 3):
            _, to = along(k, d)
            remote(
                g2.at[:, at], total.at[core, a_me, :, at],
                ar_send.at[n, 5, k], last_recv.at[n, k, d - 1], to,
            ).start()
        total[pl.ds(core, 1), pl.ds(a_me, 1), :, at, :] = g2[:, at, :].reshape(
            1, 1, 4, SETS[n][4][k][0], 128
        )
        to_sibling(n, k, a_me)

    def stage6(n):
        for d in (1, 3, 2):
            for k in SETS[n][4]:
                a, _ = along(k, 4 - d)
                held = total.at[core, a, :, piece(n, k)]
                remote(
                    held, held, ar_send.at[n, 5, k], last_recv.at[n, k, d - 1], (dp, cp)
                ).wait_recv()
                to_sibling(n, k, a)

    def stage7(n, k):
        ar_got(total.at[0, :, :, piece(n, k)], n, 6, k)

    def all_colors(stage, n):
        for k in SETS[n][4]:
            stage(n, k)

    def settle(n):
        ar_sent(r0.at[set_rows(n)], n, 0, 0)
        for k in SETS[n][4]:
            at = piece(n, k)
            ar_sent(r1.at[:, at], n, 1, k)
            ar_sent(r2.at[:, at], n, 2, k)
            ar_sent(r3.at[pl.ds(0, 3), at], n, 3, k)
            ar_sent(g2.at[pl.ds(0, 3), at], n, 4, k)
            ar_sent(total.at[0, pl.ds(0, 3), :, at], n, 5, k)
            ar_sent(total.at[0, :, :, at], n, 6, k)

    gated = (mixed * gate).astype(BF)
    low = normed_t[...].astype(BF)
    dh_gate = (dgated * mixed * silu_slope(hidden_t[0:D, :])).astype(BF)
    dh_t[0:D, :] = dh_gate
    w_ref[0:D, :] = nt(low, dh_gate).astype(BF)
    w_ref[D : 2 * D, :] = nn(gated, cot[...]).astype(BF)
    stage0(0)
    branch = nn(turned(gated).astype(BF), wout[...])
    layer_out[...] = (emb_nat[...] + branch).astype(BF)

    for i in range(HEADS):
        q_cat[:, i * TOK : (i + 1) * TOK] = q_in[i]
    for b in range(N_CP):
        kv_nat[b * TOK : (b + 1) * TOK, :] = turned(
            jnp.concatenate([k_in[b], v_in[b]], axis=0)
        ).astype(BF)

    for c in range(HEADS - 1, -1, -1):

        @pl.when(head != c)
        def _():
            remote(
                da_in.at[c], da_in.at[c], send.at[6], da_recv.at[c], (dp, cp)
            ).wait_recv()

        da_nat[c * TOK : (c + 1) * TOK, :] = (turned(da_in[c]) * shrink).astype(BF)
        da_cat[:, c * TOK : (c + 1) * TOK] = da_in[c]
        values, keys_values = pair(v_in, c), kv_nat[c * CHUNK : (c + 1) * CHUNK, :]
        dk = jnp.zeros((HEAD, CHUNK), F32)
        dv = jnp.zeros((HEAD, CHUNK), F32)
        for first, last in ((c, HEADS),) if c else ((HEADS // 2, HEADS), (0, HEADS // 2)):
            rows = slice(first * TOK, last * TOK)
            at = kept(c, first, last - first)
            ds = (nn(da_nat[rows, :], values) * slope_keep[at, :]).astype(BF)
            dq = nn(ds, keys_values)
            dk = dk + nn(q_cat[:, rows], ds)
            dv = dv + nn(da_cat[:, rows], w_keep[at, :])
            if c < HEADS - 1:
                after = slice(max(first, c + 1) * TOK, last * TOK)
                dq_acc[after, :] += dq[after.start - first * TOK :, :]
            if first == c:
                dq_acc[c * TOK : (c + 1) * TOK, :] = dq[0:TOK, :]
            if c == 0:
                for i in range(last - 1, first - 1, -1):
                    dq_out[i] = dq_acc[i * TOK : (i + 1) * TOK, :].T[:HEAD, :].astype(BF)

                    @pl.when(head != i)
                    def _():
                        remote(
                            dq_out.at[i], dq_in.at[rows64(head)], send.at[9], recv.at[9],
                            (dp, block_of(i)),
                        ).start()

        dk, dv = dk.astype(BF), dv.astype(BF)
        for b in range(2):
            kb = 2 * c + b
            dk_out[kb] = dk[:, b * TOK : (b + 1) * TOK]
            dv_out[kb] = dv[:, b * TOK : (b + 1) * TOK]

            @pl.when(cp != kb)
            def _():
                remote(
                    dk_out.at[kb], dk_in.at[half, rows64(head)], send.at[7], recv.at[7], (dp, kb)
                ).start()
                remote(
                    dv_out.at[kb], dv_in.at[half, rows64(head)], send.at[8], recv.at[8], (dp, kb)
                ).start()

    stage1(0)

    dq_in[rows64(head), :] = dq_out[pl.ds(head, 1)].reshape(HEAD, TOK)
    dk_in[pl.ds(half, 1), rows64(head), :] = dk_out[pl.ds(cp, 1)]
    dv_in[pl.ds(half, 1), rows64(head), :] = dv_out[pl.ds(cp, 1)]
    wait_got(dk_out.at[pl.ds(0, N_CP - 1)], 7)
    wait_got(dv_out.at[pl.ds(0, N_CP - 1)], 8)
    wait_got(dq_in.at[pl.ds(0, D - HEAD)], 9)

    def column_back(b, grad):
        dh = (grad * silu_slope(hidden_t[b * D : (b + 1) * D, :])).astype(BF)
        dh_t[b * D : (b + 1) * D, :] = dh
        grads = nt(low, dh).astype(BF)
        if b == 1:
            w_ref[LATE : LATE + D, :] = grads
        elif b == 2:
            w_ref[LATE + D : LATE + 768, :] = grads[0:256]
            w_ref[LATE + 832 : LATE + 1088, :] = grads[256:512]
        else:
            w_ref[LATE + 1088 : LATE + 1600, :] = grads

    column_back(1, dv_in[0].astype(F32) + dv_in[1].astype(F32))
    column_back(2, dq_in[...].astype(F32))
    column_back(3, dk_in[0].astype(F32) + dk_in[1].astype(F32))
    stage0(1)
    all_colors(stage2, 0)
    dnormed = nn(joined[...], dh_t[...])
    dembed = column_norm_back(dnormed, normed_t[...], inv_ref[0:1, :]) + cot_t[...]
    exact = lax.Precision.HIGHEST
    stage1(1)
    proj_grads = nt(cold_t[...], dembed, exact).astype(BF)
    w_ref[LATE + 768 : LATE + 832, :] = proj_grads[0:64]
    w_ref[LATE + 1600 : LATE + 1664, :] = proj_grads[64:128]
    stage0(2)

    cold_event = lax.dot_general(
        proj[...].astype(F32), dembed, (((1,), (0,)), ((), ())),
        preferred_element_type=F32, precision=exact,
    )
    is_hot = slot_row < HOT
    for f in range(4):
        part = dembed[f * 128 : (f + 1) * 128, :]
        pack_ref[:, f * TOK : (f + 1) * TOK] = jnp.where(
            is_hot, part, cold_event if f == 0 else 0.0
        ).astype(BF)
    grad_out[...] = nt(slots_1h[...], pack_ref[...]).astype(BF)
    grad_in[tile(me), :] = grad_out[tile(me), :]

    def send_grads(group):
        for to in everyone[group::4]:
            remote(
                grad_out.at[tile(to[0] * N_CP + to[1])], grad_in.at[tile(me)],
                send.at[10], recv.at[10], to,
            ).start()

    stage1(2)
    all_colors(stage3, 0)
    all_colors(stage2, 1)
    all_colors(stage2, 2)
    all_colors(stage4, 0)
    send_grads(0)
    send_grads(1)
    all_colors(stage3, 1)
    all_colors(stage3, 2)
    all_colors(stage5, 0)
    send_grads(2)
    all_colors(stage4, 1)
    all_colors(stage4, 2)
    send_grads(3)
    all_colors(stage5, 1)
    all_colors(stage5, 2)
    stage6(0)
    stage6(1)
    stage6(2)

    wait_got(grad_in.at[pl.ds(0, SLOTS - SLOT)], 10)
    by_rank(grad_in, rows_out)

    wait_sent(ids_all.at[pl.ds(0, DEVICES - 1)], 0)
    wait_sent(row_in.at[pl.ds(0, SLOTS - SLOT)], 1)
    wait_sent(k_in.at[pl.ds(0, N_CP - 1)], 2)
    wait_sent(v_in.at[pl.ds(0, N_CP - 1)], 3)
    wait_sent(q_in.at[pl.ds(0, HEADS - 1)], 4)
    wait_sent(att_in.at[pl.ds(0, D - HEAD)], 5)
    wait_sent(da_in.at[pl.ds(0, HEADS - 1)], 6)
    wait_sent(dk_out.at[pl.ds(0, N_CP - 1)], 7)
    wait_sent(dv_out.at[pl.ds(0, N_CP - 1)], 8)
    wait_sent(dq_in.at[pl.ds(0, D - HEAD)], 9)
    wait_sent(grad_in.at[pl.ds(0, SLOTS - SLOT)], 10)
    settle(0)
    for n in range(3):
        all_colors(stage7, n)
    settle(1)
    settle(2)


def finish_kernel(
    layer, rows, req, sums,
    layer_out, hot_out, cold_out, proj_out, joined_out, wout_out,
    hot_buf, cold_buf, sum_buf, sem,
):
    copies = []

    def put(src, dst):
        copy = pltpu.make_async_copy(src, dst, sem.at[len(copies)])
        copy.start()
        copies.append(copy)

    put(layer, layer_out)
    picked = rows[...]

    def onehot(rows_here, first):
        index = iota((rows_here, DEVICES), 0) + first
        return jnp.concatenate(
            [jnp.where(index == req[c : c + 1, :], 1.0, 0.0).astype(BF) for c in range(CAP)],
            axis=1,
        )

    hot_buf[...] = nn(onehot(HOT, 0), picked)
    put(hot_buf, hot_out)
    low = picked[:, 0:COLD_W]
    for t in range(4):
        part = pl.ds(t * (COLD // 4), COLD // 4)
        cold_buf[part, :] = nn(onehot(COLD // 4, HOT + t * (COLD // 4)), low)
        put(cold_buf.at[part], cold_out.at[part])

    scale = (TOK * DEVICES) ** -0.5
    for core in range(2):
        for n in range(3):
            home = (4 * D * core, D + 768 * core, 5 * D + 64 * core)[n]
            for k, (count, at) in SETS[n][4].items():
                for a in range(4):
                    top = home + first_row(n, k) + a * count
                    for b in range(4):
                        sum_buf[top : top + count, b * 128 : (b + 1) * 128] = (
                            sums[core, a, b, at : at + count, :].astype(F32) * scale
                        )
        if core == 0:
            for b in (0, 1):
                put(sum_buf.at[pl.ds(b * D, D)], joined_out.at[:, pl.ds(b * D, D)])
    for b in (2, 3):
        put(sum_buf.at[pl.ds(b * D, D)], joined_out.at[:, pl.ds(b * D, D)])
    put(sum_buf.at[pl.ds(4 * D, D)], wout_out)
    put(sum_buf.at[pl.ds(5 * D, COLD_W)], proj_out)
    for copy in copies:
        copy.wait()


def vmem(n):
    return [pl.BlockSpec(memory_space=pltpu.VMEM)] * n


def anywhere(n):
    return [pl.BlockSpec(memory_space=pl.ANY)] * n


def hbm(n):
    return [pl.BlockSpec(memory_space=pltpu.HBM)] * n


def local(row_owner, slot_row, hot, cold, proj, joined, wout, cot):
    v = pltpu.VMEM
    operands = [row_owner.reshape(1, TOK), slot_row.reshape(1, TOK)]
    operands += [hot, cold, proj, joined, wout, cot]
    operands = [pltpu.with_memory_space_constraint(a, pltpu.HBM) for a in operands]
    layer, rows, req, sums = pl.pallas_call(
        step_kernel,
        out_shape=(
            jax.ShapeDtypeStruct((TOK, D), BF),
            jax.ShapeDtypeStruct((CAP * DEVICES, D), BF),
            jax.ShapeDtypeStruct((8, DEVICES), I32),
            jax.ShapeDtypeStruct((2, 4, 4, PART_ROWS, 128), BF),
        ),
        in_specs=hbm(8),
        out_specs=tuple(vmem(4)),
        scratch_shapes=[
            v((HOT, D), BF), v((COLD, COLD_W), BF), v((HOT, 4 * COLD_W), BF),
            v((COLD_W, D), BF), v((D, 4 * D), BF),
            v((D, D), BF), v((TOK, D), BF), v((1, TOK), I32), v((1, TOK), I32),
            v((1, TOK), I32),
            v((DEVICES, 1, TOK), I32), v((SLOTS, 128), F32), v((SLOTS, 128), BF),
            v((SLOTS, 128), BF), v((TOK, CAP * DEVICES), BF), v((CAP * DEVICES, D), BF),
            v((TOK, D), F32), v((D, TOK), F32), v((8, TOK), F32),
            v((COLD_W, TOK), F32), v((4 * D, D), BF),
            v((4 * D, TOK), F32), v((4 * D, TOK), BF), v((D, TOK), F32), v((D, TOK), F32),
            v((SLOTS, 4 * TOK), BF),
            v((N_CP, HEAD, TOK), BF), v((N_CP, HEAD, TOK), BF), v((HEADS, HEAD, TOK), BF),
            v((N_CP * TOK, 2 * HEAD), BF),
            v((PAIRS * TOK, CHUNK), BF), v((PAIRS * TOK, CHUNK), F32),
            v((HEADS, HEAD, TOK), BF), v((D, TOK), BF), v((D, TOK), BF),
            v((HEADS, HEAD, TOK), BF),
            v((HEADS * TOK, HEAD), BF), v((HEAD, HEADS * TOK), BF), v((HEAD, HEADS * TOK), BF),
            v((HEADS * TOK, 2 * HEAD), F32),
            v((HEADS, HEAD, TOK), BF),
            v((N_CP, HEAD, TOK), BF), v((N_CP, HEAD, TOK), BF),
            v((D, TOK), BF), v((2, D, TOK), BF), v((2, D, TOK), BF),
            v((4 * D, TOK), BF), v((128, 4 * TOK), BF),
            v((SLOTS, 128), BF), v((SLOTS, 128), BF),
            v((W_ROWS, D), BF), v((W_ROWS // 2, D), BF), v((W_ROWS // 2, D), BF),
            v((3, PART_ROWS, D), BF), v((4, PART_ROWS, 128), BF),
            v((3, PART_ROWS, 128), BF), v((4, PART_ROWS, 128), BF),
            v((4, PART_ROWS, 128), BF),
            pltpu.SemaphoreType.DMA((11,)), pltpu.SemaphoreType.DMA((11,)),
            pltpu.SemaphoreType.DMA((HEADS,)),
            pltpu.SemaphoreType.DMA((3, 7, 3)), pltpu.SemaphoreType.DMA((3, 7, 3)),
            pltpu.SemaphoreType.DMA((3, 3, 3)),
            pltpu.SemaphoreType.DMA((8,)),
        ],
        compiler_params=pltpu.CompilerParams(
            collective_id=0, has_side_effects=True, vmem_limit_bytes=44 << 20
        ),
        name="step",
    )(*operands)
    return pl.pallas_call(
        finish_kernel,
        out_shape=(
            jax.ShapeDtypeStruct((TOK, D), BF),
            jax.ShapeDtypeStruct((HOT, D), F32),
            jax.ShapeDtypeStruct((COLD, COLD_W), F32),
            jax.ShapeDtypeStruct((COLD_W, D), F32),
            jax.ShapeDtypeStruct((D, 4 * D), F32),
            jax.ShapeDtypeStruct((D, D), F32),
        ),
        in_specs=vmem(4),
        out_specs=tuple(hbm(6)),
        scratch_shapes=[
            v((HOT, D), F32), v((COLD, COLD_W), F32), v((W_ROWS, D), F32),
            pltpu.SemaphoreType.DMA((12,)),
        ],
        compiler_params=pltpu.CompilerParams(vmem_limit_bytes=20 << 20),
        name="finish",
    )(layer, rows, req, sums)


def solution(mesh):
    rows = P(("dp", "cp"), None)
    return jax.shard_map(
        local,
        mesh=mesh,
        in_specs=(rows, P(("dp", "cp")), rows, rows, P(), P(), P(), rows),
        out_specs=(rows, rows, rows, P(), P(), P()),
        check_vma=False,
    )
```

```python
import math

import jax
import jax.numpy as jnp
from jax import lax
from jax.experimental import pallas as pl
from jax.experimental.pallas import tpu as pltpu
from jax.sharding import PartitionSpec as P

MESH = pl.DeviceIdType.MESH
BF = jnp.bfloat16
F32 = jnp.float32
I32 = jnp.int32
EPSILON = 1e-05

D = 512
HEADS = 8
HEAD = 64
TOK = 128
CAP = 4
HOT = 512
COLD = 2048
COLD_W = 128
N_DP = 8
N_CP = 16
DEVICES = N_DP * N_CP
SLOT = 16
SLOTS = DEVICES * SLOT
SHIFT = 4096
CHUNK = 256
PAIRS = HEADS * (HEADS + 1) // 2
W_ROWS = 4 * D + D + COLD_W
LATE = 2 * D
SETS = (
    (0, D, 0, D, {0: (48, 0), 1: (48, 48), 2: (32, 96)}),
    (LATE, 832, D, 768, {0: (64, 128), 1: (64, 192), 2: (64, 256)}),
    (LATE + 768, 832, D + 768, 64, {2: (16, 320)}),
)
PART_ROWS = 336


def first_row(n, k):
    return sum(4 * part for color, (part, _) in SETS[n][4].items() if color < k)


FAR_FIRST = sorted(
    (
        (dz, dc, dx, dy)
        for dz in range(4)
        for dc in range(2)
        for dx in range(4)
        for dy in range(4)
        if dz or dc or dx or dy
    ),
    key=lambda o: (-sum(min(v, 4 - v) for v in (o[0], o[2], o[3])), sum(o) * 53 % 7, o),
)


def nn(a, b):
    return jnp.dot(a, b, preferred_element_type=F32)


def nt(a, b, precision=None):
    return lax.dot_general(
        a, b, (((1,), (1,)), ((), ())), preferred_element_type=F32, precision=precision
    )


def sigmoid(v):
    return 0.5 * jnp.tanh(0.5 * v) + 0.5


def silu_slope(v):
    sig = sigmoid(v)
    return sig + v * sig * (1.0 - sig)


def iota(shape, dim):
    return lax.broadcasted_iota(I32, shape, dim)


def turned(v):
    return v.astype(F32).T


def column_norm(v):
    average = jnp.mean(v, axis=0, keepdims=True)
    centred = v - average
    inverse = lax.rsqrt(jnp.mean(centred * centred, axis=0, keepdims=True) + EPSILON)
    return centred * inverse, inverse


def column_norm_back(g, y, inverse):
    first = jnp.mean(g, axis=0, keepdims=True)
    second = jnp.mean(g * y, axis=0, keepdims=True)
    return (g - first - y * second) * inverse


def step_kernel(
    owner_in, slot_in, hot_hbm, cold_hbm, proj_hbm, joined_hbm, wout_hbm, cot_hbm,
    layer_out, hot_sum, cold_sum, total,
    hot, cold, cold_wide, proj, joined, wout, cot, owner_ref, slot_ref, code_row,
    ids_all, pick32, pick16, row_in, take_1h, rows_got, emb_nat, normed_t, inv_ref, cold_t, joined_t,
    hidden_t, active_t, dgated_t, cot_t, slots_1h,
    k_in, v_in, q_in, kv_nat, w_keep, slope_keep, att_out, att_in, da_out, da_in,
    da_nat, da_cat, q_cat, dq_acc, dq_out, dk_out, dv_out, dq_in, dk_in, dv_in, dh_t, pack_ref, grad_out, grad_in, req,
    w_ref, r0, u1, r1, u2, r2, r3, g2,
    send, recv, da_recv, ar_send, ar_recv, last_recv, local_sem,
):
    dp, cp = lax.axis_index("dp"), lax.axis_index("cp")
    me = dp * N_CP + cp
    z, core, x, y = dp // 2, dp % 2, cp // 4, cp % 4
    head = cp // 2
    half = ((cp + 1) // 2) % 2
    xs, ys, zs = ([(v + d) % 4 for d in range(4)] for v in (x, y, z))
    cores = [core, (core + 1) % 2]
    dps = [[zs[dz] * 2 + cores[dc] for dc in range(2)] for dz in range(4)]
    cps = [[xs[dx] * 4 + ys[dy] for dy in range(4)] for dx in range(4)]
    plane = [(dx, dy) for dx in range(4) for dy in range(4) if dx or dy]
    plane.sort(key=lambda o: (-(min(o[0], 4 - o[0]) + min(o[1], 4 - o[1])), (o[0] * 3 + o[1]) % 4))

    def remote(src, dst, send_sem, recv_sem, to):
        return pltpu.make_async_remote_copy(
            src_ref=src, dst_ref=dst, send_sem=send_sem, recv_sem=recv_sem,
            device_id=to, device_id_type=MESH,
        )

    def wait_sent(ref, i):
        remote(ref, ref, send.at[i], recv.at[i], (dp, cp)).wait_send()

    def wait_got(ref, i):
        remote(ref, ref, send.at[i], recv.at[i], (dp, cp)).wait_recv()

    def rows64(h):
        return pl.ds(pl.multiple_of(h * HEAD, HEAD), HEAD)

    def tile(o):
        return pl.ds(pl.multiple_of(o * SLOT, SLOT), SLOT)

    def by_rank(tiles, rows):
        pick32[...] = tiles[...].astype(F32)
        for c in range(CAP):
            for f in range(4):
                rows[c * DEVICES : (c + 1) * DEVICES, f * 128 : (f + 1) * 128] = pick32[
                    pl.ds(CAP * f + c, DEVICES, stride=SLOT), :
                ].astype(BF)

    barrier = pltpu.get_barrier_semaphore()
    everyone = [(dps[dz][dc], cps[dx][dy]) for dz, dc, dx, dy in FAR_FIRST]
    for to in everyone:
        pl.semaphore_signal(barrier, inc=1, device_id=to, device_id_type=MESH)
    loads = [
        pltpu.make_async_copy(src, dst, local_sem.at[i])
        for i, (src, dst) in enumerate(
            ((owner_in, owner_ref), (slot_in, slot_ref), (joined_hbm, joined), (cot_hbm, cot), (wout_hbm, wout), (hot_hbm, hot),
             (cold_hbm, cold), (proj_hbm, proj))
        )
    ]
    for load in loads:
        load.start()
    for load in loads[:2]:
        load.wait()
    owner_row, slot_row = owner_ref[...], slot_ref[...]
    code_row[...] = owner_row * SHIFT + slot_row
    pl.semaphore_wait(barrier, DEVICES - 1)

    for to in everyone:
        remote(code_row, ids_all.at[me], send.at[0], recv.at[0], to).start()
    ids_all[pl.ds(me, 1)] = code_row[...].reshape(1, 1, TOK)

    diagonal = iota((TOK, TOK), 0) == iota((TOK, TOK), 1)

    def as_column(row):
        picked = jnp.where(diagonal, row.astype(F32), 0.0)
        return jnp.sum(picked, axis=1, keepdims=True).astype(I32)

    owner_col, slot_col = as_column(owner_row), as_column(slot_row)
    before_row = (owner_col == owner_row) & (iota((TOK, TOK), 0) < iota((TOK, TOK), 1))
    rank_row = jnp.sum(jnp.where(before_row, 1, 0), axis=0, keepdims=True)
    place_row = owner_row * SLOT + rank_row
    take_1h[...] = jnp.where(
        iota((TOK, CAP * DEVICES), 1) == as_column(rank_row) * DEVICES + owner_col, 1.0, 0.0
    ).astype(BF)
    for f in range(4):
        slots_1h[:, f * TOK : (f + 1) * TOK] = jnp.where(
            iota((SLOTS, TOK), 0) == place_row + CAP * f, 1.0, 0.0
        ).astype(BF)
    for load in loads[2:5]:
        load.wait()
    for b in range(4):
        joined_t[b * D : (b + 1) * D, :] = turned(joined[:, b * D : (b + 1) * D]).astype(BF)
    cot_t[...] = turned(cot[...])
    dgated_t[...] = nn(wout[...], cot_t[...].astype(BF))
    for load in loads[5:]:
        load.wait()
    for g in range(4):
        cold_wide[:, g * 128 : (g + 1) * 128] = cold[g * HOT : (g + 1) * HOT, :]

    wait_got(ids_all.at[pl.ds(0, DEVICES - 1)], 0)

    ids = ids_all[:, 0, :]
    asked = (ids // SHIFT) == me
    slot_plus = ((ids % SHIFT) + 1).astype(F32)
    upper = jnp.where(iota((TOK, TOK), 0) < iota((TOK, TOK), 1), 1.0, 0.0).astype(BF)
    earlier = nn(jnp.where(asked, 1.0, 0.0).astype(BF), upper)
    asks = [jnp.where(asked & (earlier == float(c)), slot_plus, 0.0) for c in range(CAP)]
    wanted = jnp.concatenate([jnp.sum(ask, axis=1, keepdims=True) for ask in asks], axis=0)
    wanted = wanted.astype(I32) - 1
    group = jnp.where(wanted < 0, -1, wanted // HOT)
    row = jnp.where(wanted < 0, -1, wanted % HOT)
    chosen = jnp.where(iota((CAP * DEVICES, HOT), 1) == row, 1.0, 0.0).astype(BF)
    hot_rows = nn(chosen, hot[...])
    cold_rows = nn(chosen, cold_wide[...])
    for f in range(4):
        part = jnp.where(group == 0, hot_rows[:, f * 128 : (f + 1) * 128], 0.0)
        if f == 0:
            for g in range(4):
                part = jnp.where(group == g + 1, cold_rows[:, g * 128 : (g + 1) * 128], part)
        for c in range(CAP):
            pick32[pl.ds(CAP * f + c, DEVICES, stride=SLOT), :] = part[
                c * DEVICES : (c + 1) * DEVICES, :
            ]
    pick16[...] = pick32[...].astype(BF)

    for to in everyone:
        remote(
            pick16.at[tile(to[0] * N_CP + to[1])], row_in.at[tile(me)], send.at[1], recv.at[1], to
        ).start()
    row_in[tile(me), :] = pick16[tile(me), :]
    for c in range(CAP):
        wanted_row = jnp.sum(asks[c].T, axis=0, keepdims=True)
        req[c : c + 1, :] = wanted_row.astype(I32) - 1

    wait_got(row_in.at[pl.ds(0, SLOTS - SLOT)], 1)

    by_rank(row_in, rows_got)
    fetched = nn(take_1h[...], rows_got[...])
    cold_vec = fetched[:, 0:COLD_W]
    cold_embed = nn(cold_vec.astype(BF), proj[...])
    embedded = jnp.where(slot_col < HOT, fetched, cold_embed)
    emb_nat[...] = embedded
    normed, inverse = column_norm(embedded.T)
    normed_t[...] = normed
    inv_ref[...] = jnp.broadcast_to(inverse, inv_ref.shape)
    low = normed.astype(BF)

    def k_rows(h):
        return pl.ds(pl.multiple_of(3 * D + h * HEAD, HEAD), HEAD)

    def v_rows(h):
        return pl.ds(pl.multiple_of(D + h * HEAD, HEAD), HEAD)

    def q_rows(h):
        return pl.ds(pl.multiple_of(2 * D + h * HEAD, HEAD), HEAD)

    def same_half(d):
        h = (head + d) % HEADS
        return h, (dp, 2 * h + (half + h) % 2)

    def project(b):
        hid = nn(joined_t[b * D : (b + 1) * D, :], low)
        hidden_t[b * D : (b + 1) * D, :] = hid
        active_t[b * D : (b + 1) * D, :] = (hid * sigmoid(hid)).astype(BF)

    project(3)
    for dx, dy in plane:
        pcp = cps[dx][dy]
        remote(active_t.at[k_rows(pcp // 2)], k_in.at[cp], send.at[2], recv.at[2], (dp, pcp)).start()
    project(1)
    for dx, dy in plane:
        pcp = cps[dx][dy]
        remote(active_t.at[v_rows(pcp // 2)], v_in.at[cp], send.at[3], recv.at[3], (dp, pcp)).start()
    project(2)
    for d in range(1, HEADS):
        h, to = same_half(d)
        remote(active_t.at[q_rows(h)], q_in.at[head], send.at[4], recv.at[4], to).start()
    k_in[pl.ds(cp, 1)] = active_t[k_rows(head), :].reshape(1, HEAD, TOK)
    v_in[pl.ds(cp, 1)] = active_t[v_rows(head), :].reshape(1, HEAD, TOK)
    q_in[pl.ds(head, 1)] = active_t[q_rows(head), :].reshape(1, HEAD, TOK)
    project(0)
    cold_t[...] = jnp.where(slot_row < HOT, 0.0, cold_vec.T)
    wait_got(k_in.at[pl.ds(0, N_CP - 1)], 2)
    wait_got(v_in.at[pl.ds(0, N_CP - 1)], 3)
    wait_got(q_in.at[pl.ds(0, HEADS - 1)], 4)

    def block_of(i):
        return 4 * (i // 2) + (half if i % 2 == 0 else 3 - half)

    def pair(ref, c):
        return jnp.concatenate([ref[2 * c], ref[2 * c + 1]], axis=1)

    def kept(c, i, count):
        at = sum(HEADS - b for b in range(c)) + i - c
        return pl.ds(at * TOK, count * TOK)

    shrink = 0.5 / math.sqrt(HEAD)
    def attend(i):
        q_nat = (turned(q_in[i]) * shrink).astype(BF)
        sums = jnp.zeros((HEAD, TOK), F32)
        for c in range(i + 1):
            s = nn(q_nat, pair(k_in, c))
            up = 1.0 + jnp.tanh(s)
            w = s * up
            slope = up + w * (2.0 - up)
            if c == i:
                ok = (iota((TOK, CHUNK), 1) + c * CHUNK) <= (
                    iota((TOK, CHUNK), 0) + block_of(i) * TOK
                )
                w = jnp.where(ok, w, 0.0)
                slope = jnp.where(ok, slope, 0.0)
            w = w.astype(BF)
            w_keep[kept(c, i, 1), :] = w
            slope_keep[kept(c, i, 1), :] = slope
            sums = sums + nt(pair(v_in, c), w)
        att_out[i] = sums.astype(BF)

    for group in ((7, 6, 5), (4, 3, 2, 1, 0)):
        for i in group:
            attend(i)
        for i in group:

            @pl.when(head != i)
            def _():
                remote(
                    att_out.at[i], att_in.at[rows64(head)], send.at[5], recv.at[5],
                    (dp, block_of(i)),
                ).start()

    att_in[rows64(head), :] = att_out[pl.ds(head, 1)].reshape(HEAD, TOK)
    wait_got(att_in.at[pl.ds(0, D - HEAD)], 5)

    mixed, inv_mix = column_norm(att_in[...].astype(F32))
    gate = active_t[0:D, :].astype(F32)
    dgated = dgated_t[...]
    da_out[...] = column_norm_back(dgated * gate, mixed, inv_mix).astype(BF)
    for d in range(1, HEADS):
        h, to = same_half(d)
        remote(da_out.at[rows64(h)], da_in.at[head], send.at[6], da_recv.at[head], to).start()
    da_in[pl.ds(head, 1)] = da_out[rows64(head), :].reshape(1, HEAD, TOK)

    sibling = (z * 2 + (1 - core), cp)
    place = (x, y, z)

    def along(dim, d):
        moved = [xs[0], ys[0], zs[0]]
        moved[dim] = (xs, ys, zs)[dim][d]
        return moved[dim], (moved[2] * 2 + core, moved[0] * 4 + moved[1])

    def ar(src, dst, n, stage, k, to):
        return remote(src, dst, ar_send.at[n, stage, k], ar_recv.at[n, stage, k], to)

    def ar_got(ref, n, stage, k):
        ar(ref, ref, n, stage, k, (dp, cp)).wait_recv()

    def ar_sent(ref, n, stage, k):
        ar(ref, ref, n, stage, k, (dp, cp)).wait_send()

    def core_rows(n, c):
        return pl.ds(pl.multiple_of(SETS[n][0] + c * SETS[n][1], 16), SETS[n][3])

    def set_rows(n):
        return pl.ds(SETS[n][2], SETS[n][3])

    def stage0(n):
        ar(w_ref.at[core_rows(n, 1 - core)], r0.at[set_rows(n)], n, 0, 0, sibling).start()

    def piece(n, k):
        part, at = SETS[n][4][k]
        return pl.ds(at, part)

    def u1_rows(n, k, a):
        part = SETS[n][4][k][0]
        return pl.ds(pl.multiple_of(SETS[n][2] + first_row(n, k) + a * part, 16), part)

    def stage1(n):
        at = set_rows(n)
        ar_got(r0.at[at], n, 0, 0)
        u1[at, :] = (w_ref[core_rows(n, core), :].astype(F32) + r0[at, :].astype(F32)).astype(BF)
        for k in SETS[n][4]:
            for d in (2, 1, 3):
                a, to = along(k, d)
                ar(u1.at[u1_rows(n, k, a)], r1.at[d - 1, piece(n, k)], n, 1, k, to).start()

    def stage2(n, k):
        at = piece(n, k)
        ar_got(r1.at[:, at], n, 1, k)
        part = u1[u1_rows(n, k, place[k]), :].astype(F32)
        for d in range(3):
            part = part + r1[d, at, :].astype(F32)
        for b in range(4):
            u2[b, at, :] = part[:, b * 128 : (b + 1) * 128].astype(BF)
        for d in (2, 1, 3):
            b, to = along((k + 1) % 3, d)
            ar(u2.at[b, at], r2.at[d - 1, at], n, 2, k, to).start()

    def stage3(n, k):
        at = piece(n, k)
        ar_got(r2.at[:, at], n, 2, k)
        b_me, c_me = place[(k + 1) % 3], place[(k + 2) % 3]
        part = u2[pl.ds(b_me, 1), at, :].astype(F32)
        for d in range(3):
            part = part + r2[d : d + 1, at, :].astype(F32)
        r3[pl.ds(c_me, 1), at, :] = part.astype(BF)
        for d in (2, 1, 3):
            _, to = along((k + 2) % 3, d)
            ar(r3.at[c_me, at], r3.at[c_me, at], n, 3, k, to).start()

    def stage4(n, k):
        at = piece(n, k)
        ar_got(r3.at[pl.ds(0, 3), at], n, 3, k)
        b_me = place[(k + 1) % 3]
        part = r3[0:1, at, :].astype(F32)
        for d in range(1, 4):
            part = part + r3[d : d + 1, at, :].astype(F32)
        g2[pl.ds(b_me, 1), at, :] = part.astype(BF)
        for d in (2, 1, 3):
            _, to = along((k + 1) % 3, d)
            ar(g2.at[b_me, at], g2.at[b_me, at], n, 4, k, to).start()

    def to_sibling(n, k, a):
        held = total.at[core, a, :, piece(n, k)]
        ar(held, held, n, 6, k, sibling).start()

    def stage5(n, k):
        at = piece(n, k)
        ar_got(g2.at[pl.ds(0, 3), at], n, 4, k)
        a_me = place[k]
        for d in (2, 1, 3):
            _, to = along(k, d)
            remote(
                g2.at[:, at], total.at[core, a_me, :, at],
                ar_send.at[n, 5, k], last_recv.at[n, k, d - 1], to,
            ).start()
        total[pl.ds(core, 1), pl.ds(a_me, 1), :, at, :] = g2[:, at, :].reshape(
            1, 1, 4, SETS[n][4][k][0], 128
        )
        to_sibling(n, k, a_me)

    def stage6(n):
        for d in (1, 3, 2):
            for k in SETS[n][4]:
                a, _ = along(k, 4 - d)
                held = total.at[core, a, :, piece(n, k)]
                remote(
                    held, held, ar_send.at[n, 5, k], last_recv.at[n, k, d - 1], (dp, cp)
                ).wait_recv()
                to_sibling(n, k, a)

    def stage7(n, k):
        ar_got(total.at[0, :, :, piece(n, k)], n, 6, k)

    def all_colors(stage, n):
        for k in SETS[n][4]:
            stage(n, k)

    def settle(n):
        ar_sent(r0.at[set_rows(n)], n, 0, 0)
        for k in SETS[n][4]:
            at = piece(n, k)
            ar_sent(r1.at[:, at], n, 1, k)
            ar_sent(r2.at[:, at], n, 2, k)
            ar_sent(r3.at[pl.ds(0, 3), at], n, 3, k)
            ar_sent(g2.at[pl.ds(0, 3), at], n, 4, k)
            ar_sent(total.at[0, pl.ds(0, 3), :, at], n, 5, k)
            ar_sent(total.at[0, :, :, at], n, 6, k)

    gated = (mixed * gate).astype(BF)
    low = normed_t[...].astype(BF)
    dh_gate = (dgated * mixed * silu_slope(hidden_t[0:D, :])).astype(BF)
    dh_t[0:D, :] = dh_gate
    w_ref[0:D, :] = nt(low, dh_gate).astype(BF)
    w_ref[D : 2 * D, :] = nn(gated, cot[...]).astype(BF)
    stage0(0)
    branch = nn(turned(gated).astype(BF), wout[...])
    layer_out[...] = (emb_nat[...] + branch).astype(BF)

    for i in range(HEADS):
        q_cat[:, i * TOK : (i + 1) * TOK] = q_in[i]
    for b in range(N_CP):
        kv_nat[b * TOK : (b + 1) * TOK, :] = turned(
            jnp.concatenate([k_in[b], v_in[b]], axis=0)
        ).astype(BF)

    def backward(c):
        da_nat[c * TOK : (c + 1) * TOK, :] = (turned(da_in[c]) * shrink).astype(BF)
        da_cat[:, c * TOK : (c + 1) * TOK] = da_in[c]
        rows = slice(c * TOK, HEADS * TOK)
        at = kept(c, c, HEADS - c)
        ds = (nn(da_nat[rows, :], pair(v_in, c)) * slope_keep[at, :]).astype(BF)
        dk = nn(q_cat[:, rows], ds).astype(BF)
        dv = nn(da_cat[:, rows], w_keep[at, :]).astype(BF)
        for b in range(2):
            dk_out[2 * c + b] = dk[:, b * TOK : (b + 1) * TOK]
            dv_out[2 * c + b] = dv[:, b * TOK : (b + 1) * TOK]
        dq = nn(ds, kv_nat[c * CHUNK : (c + 1) * CHUNK, :])
        if c < HEADS - 1:
            dq_acc[(c + 1) * TOK :, :] += dq[TOK:, :]
        dq_acc[c * TOK : (c + 1) * TOK, :] = dq[0:TOK, :]

    for group in ((7, 6, 5), (4, 3), (2, 1), (0,)):
        for c in group:

            @pl.when(head != c)
            def _():
                remote(
                    da_in.at[c], da_in.at[c], send.at[6], da_recv.at[c], (dp, cp)
                ).wait_recv()

        for c in group:
            backward(c)
        if group == (0,):
            for i in range(HEADS):
                dq_out[i] = dq_acc[i * TOK : (i + 1) * TOK, :].T[:HEAD, :].astype(BF)
        if group == (7, 6, 5):
            stage1(0)
        for kb in [2 * c + b for c in group for b in range(2)]:

            @pl.when(cp != kb)
            def _():
                remote(
                    dk_out.at[kb], dk_in.at[half, rows64(head)], send.at[7], recv.at[7], (dp, kb)
                ).start()
                remote(
                    dv_out.at[kb], dv_in.at[half, rows64(head)], send.at[8], recv.at[8], (dp, kb)
                ).start()

    for i in range(HEADS):

        @pl.when(head != i)
        def _():
            remote(
                dq_out.at[i], dq_in.at[rows64(head)], send.at[9], recv.at[9], (dp, block_of(i))
            ).start()

    all_colors(stage2, 0)

    dq_in[rows64(head), :] = dq_out[pl.ds(head, 1)].reshape(HEAD, TOK)
    dk_in[pl.ds(half, 1), rows64(head), :] = dk_out[pl.ds(cp, 1)]
    dv_in[pl.ds(half, 1), rows64(head), :] = dv_out[pl.ds(cp, 1)]
    wait_got(dk_out.at[pl.ds(0, N_CP - 1)], 7)
    wait_got(dv_out.at[pl.ds(0, N_CP - 1)], 8)
    wait_got(dq_in.at[pl.ds(0, D - HEAD)], 9)

    def column_back(b, grad):
        dh = (grad * silu_slope(hidden_t[b * D : (b + 1) * D, :])).astype(BF)
        dh_t[b * D : (b + 1) * D, :] = dh
        grads = nt(low, dh).astype(BF)
        if b == 1:
            w_ref[LATE : LATE + D, :] = grads
        elif b == 2:
            w_ref[LATE + D : LATE + 768, :] = grads[0:256]
            w_ref[LATE + 832 : LATE + 1088, :] = grads[256:512]
        else:
            w_ref[LATE + 1088 : LATE + 1600, :] = grads

    column_back(1, dv_in[0].astype(F32) + dv_in[1].astype(F32))
    column_back(2, dq_in[...].astype(F32))
    column_back(3, dk_in[0].astype(F32) + dk_in[1].astype(F32))
    stage0(1)
    dnormed = nn(joined[...], dh_t[...])
    dembed = column_norm_back(dnormed, normed_t[...], inv_ref[0:1, :]) + cot_t[...]
    exact = lax.Precision.HIGHEST
    all_colors(stage3, 0)
    stage1(1)
    proj_grads = nt(cold_t[...], dembed, exact).astype(BF)
    w_ref[LATE + 768 : LATE + 832, :] = proj_grads[0:64]
    w_ref[LATE + 1600 : LATE + 1664, :] = proj_grads[64:128]
    stage0(2)

    cold_event = lax.dot_general(
        proj[...].astype(F32), dembed, (((1,), (0,)), ((), ())),
        preferred_element_type=F32, precision=exact,
    )
    is_hot = slot_row < HOT
    for f in range(4):
        part = dembed[f * 128 : (f + 1) * 128, :]
        pack_ref[:, f * TOK : (f + 1) * TOK] = jnp.where(
            is_hot, part, cold_event if f == 0 else 0.0
        ).astype(BF)
    grad_out[...] = nt(slots_1h[...], pack_ref[...]).astype(BF)
    grad_in[tile(me), :] = grad_out[tile(me), :]

    def send_grads(group):
        for to in everyone[group::4]:
            remote(
                grad_out.at[tile(to[0] * N_CP + to[1])], grad_in.at[tile(me)],
                send.at[10], recv.at[10], to,
            ).start()

    stage1(2)
    all_colors(stage4, 0)
    all_colors(stage2, 1)
    all_colors(stage2, 2)
    all_colors(stage5, 0)
    send_grads(0)
    all_colors(stage3, 1)
    all_colors(stage3, 2)
    send_grads(1)
    send_grads(2)
    all_colors(stage4, 1)
    all_colors(stage4, 2)
    send_grads(3)
    all_colors(stage5, 1)
    all_colors(stage5, 2)
    stage6(0)
    stage6(1)
    stage6(2)

    wait_got(grad_in.at[pl.ds(0, SLOTS - SLOT)], 10)
    by_rank(grad_in, rows_got)

    def onehot(rows_here, first):
        index = iota((rows_here, DEVICES), 0) + first
        return jnp.concatenate(
            [jnp.where(index == req[c : c + 1, :], 1.0, 0.0).astype(BF) for c in range(CAP)],
            axis=1,
        )

    hot_sum[...] = nn(onehot(HOT, 0), rows_got[...])
    for t in range(4):
        part = slice(t * HOT, (t + 1) * HOT)
        cold_sum[part, :] = nn(onehot(HOT, HOT + t * HOT), rows_got[:, 0:COLD_W])

    wait_sent(ids_all.at[pl.ds(0, DEVICES - 1)], 0)
    wait_sent(row_in.at[pl.ds(0, SLOTS - SLOT)], 1)
    wait_sent(k_in.at[pl.ds(0, N_CP - 1)], 2)
    wait_sent(v_in.at[pl.ds(0, N_CP - 1)], 3)
    wait_sent(q_in.at[pl.ds(0, HEADS - 1)], 4)
    wait_sent(att_in.at[pl.ds(0, D - HEAD)], 5)
    wait_sent(da_in.at[pl.ds(0, HEADS - 1)], 6)
    wait_sent(dk_out.at[pl.ds(0, N_CP - 1)], 7)
    wait_sent(dv_out.at[pl.ds(0, N_CP - 1)], 8)
    wait_sent(dq_in.at[pl.ds(0, D - HEAD)], 9)
    wait_sent(grad_in.at[pl.ds(0, SLOTS - SLOT)], 10)
    settle(0)
    for n in range(3):
        all_colors(stage7, n)
    settle(1)
    settle(2)


def finish_kernel(
    layer, hot_sum, cold_sum, sums,
    layer_out, hot_out, cold_out, proj_out, joined_out, wout_out,
    sum_buf, sem,
):
    copies = []

    def put(src, dst):
        copy = pltpu.make_async_copy(src, dst, sem.at[len(copies)])
        copy.start()
        copies.append(copy)

    put(layer, layer_out)
    put(hot_sum, hot_out)
    put(cold_sum, cold_out)
    scale = (TOK * DEVICES) ** -0.5

    def scaled(n, core):
        home = (4 * D * core, D + 768 * core, 5 * D + 64 * core)[n]
        for k, (count, at) in SETS[n][4].items():
            for a in range(4):
                top = home + first_row(n, k) + a * count
                for b in range(4):
                    sum_buf[top : top + count, b * 128 : (b + 1) * 128] = (
                        sums[core, a, b, at : at + count, :].astype(F32) * scale
                    )

    def put_joined(b):
        put(sum_buf.at[pl.ds(b * D, D)], joined_out.at[:, pl.ds(b * D, D)])

    scaled(0, 0)
    put_joined(0)
    scaled(1, 0)
    put_joined(1)
    scaled(1, 1)
    put_joined(2)
    put_joined(3)
    scaled(0, 1)
    put(sum_buf.at[pl.ds(4 * D, D)], wout_out)
    scaled(2, 0)
    scaled(2, 1)
    put(sum_buf.at[pl.ds(5 * D, COLD_W)], proj_out)
    for copy in copies:
        copy.wait()


def vmem(n):
    return [pl.BlockSpec(memory_space=pltpu.VMEM)] * n


def anywhere(n):
    return [pl.BlockSpec(memory_space=pl.ANY)] * n


def hbm(n):
    return [pl.BlockSpec(memory_space=pltpu.HBM)] * n


def local(row_owner, slot_row, hot, cold, proj, joined, wout, cot):
    v = pltpu.VMEM
    operands = [row_owner.reshape(1, TOK), slot_row.reshape(1, TOK)]
    operands += [hot, cold, proj, joined, wout, cot]
    operands = [pltpu.with_memory_space_constraint(a, pltpu.HBM) for a in operands]
    layer, hot_sum, cold_sum, sums = pl.pallas_call(
        step_kernel,
        out_shape=(
            jax.ShapeDtypeStruct((TOK, D), BF),
            jax.ShapeDtypeStruct((HOT, D), F32),
            jax.ShapeDtypeStruct((COLD, COLD_W), F32),
            jax.ShapeDtypeStruct((2, 4, 4, PART_ROWS, 128), BF),
        ),
        in_specs=hbm(8),
        out_specs=tuple(vmem(4)),
        scratch_shapes=[
            v((HOT, D), BF), v((COLD, COLD_W), BF), v((HOT, 4 * COLD_W), BF),
            v((COLD_W, D), BF), v((D, 4 * D), BF),
            v((D, D), BF), v((TOK, D), BF), v((1, TOK), I32), v((1, TOK), I32),
            v((1, TOK), I32),
            v((DEVICES, 1, TOK), I32), v((SLOTS, 128), F32), v((SLOTS, 128), BF),
            v((SLOTS, 128), BF), v((TOK, CAP * DEVICES), BF), v((CAP * DEVICES, D), BF),
            v((TOK, D), F32), v((D, TOK), F32), v((8, TOK), F32),
            v((COLD_W, TOK), F32), v((4 * D, D), BF),
            v((4 * D, TOK), F32), v((4 * D, TOK), BF), v((D, TOK), F32), v((D, TOK), F32),
            v((SLOTS, 4 * TOK), BF),
            v((N_CP, HEAD, TOK), BF), v((N_CP, HEAD, TOK), BF), v((HEADS, HEAD, TOK), BF),
            v((N_CP * TOK, 2 * HEAD), BF),
            v((PAIRS * TOK, CHUNK), BF), v((PAIRS * TOK, CHUNK), F32),
            v((HEADS, HEAD, TOK), BF), v((D, TOK), BF), v((D, TOK), BF),
            v((HEADS, HEAD, TOK), BF),
            v((HEADS * TOK, HEAD), BF), v((HEAD, HEADS * TOK), BF), v((HEAD, HEADS * TOK), BF),
            v((HEADS * TOK, 2 * HEAD), F32),
            v((HEADS, HEAD, TOK), BF),
            v((N_CP, HEAD, TOK), BF), v((N_CP, HEAD, TOK), BF),
            v((D, TOK), BF), v((2, D, TOK), BF), v((2, D, TOK), BF),
            v((4 * D, TOK), BF), v((128, 4 * TOK), BF),
            v((SLOTS, 128), BF), v((SLOTS, 128), BF), v((8, DEVICES), I32),
            v((W_ROWS, D), BF), v((W_ROWS // 2, D), BF), v((W_ROWS // 2, D), BF),
            v((3, PART_ROWS, D), BF), v((4, PART_ROWS, 128), BF),
            v((3, PART_ROWS, 128), BF), v((4, PART_ROWS, 128), BF),
            v((4, PART_ROWS, 128), BF),
            pltpu.SemaphoreType.DMA((11,)), pltpu.SemaphoreType.DMA((11,)),
            pltpu.SemaphoreType.DMA((HEADS,)),
            pltpu.SemaphoreType.DMA((3, 7, 3)), pltpu.SemaphoreType.DMA((3, 7, 3)),
            pltpu.SemaphoreType.DMA((3, 3, 3)),
            pltpu.SemaphoreType.DMA((8,)),
        ],
        compiler_params=pltpu.CompilerParams(
            collective_id=0, has_side_effects=True, vmem_limit_bytes=44 << 20
        ),
        name="step",
    )(*operands)
    return pl.pallas_call(
        finish_kernel,
        out_shape=(
            jax.ShapeDtypeStruct((TOK, D), BF),
            jax.ShapeDtypeStruct((HOT, D), F32),
            jax.ShapeDtypeStruct((COLD, COLD_W), F32),
            jax.ShapeDtypeStruct((COLD_W, D), F32),
            jax.ShapeDtypeStruct((D, 4 * D), F32),
            jax.ShapeDtypeStruct((D, D), F32),
        ),
        in_specs=vmem(4),
        out_specs=tuple(hbm(6)),
        scratch_shapes=[
            v((W_ROWS, D), F32),
            pltpu.SemaphoreType.DMA((9,)),
        ],
        compiler_params=pltpu.CompilerParams(vmem_limit_bytes=20 << 20),
        name="finish",
    )(layer, hot_sum, cold_sum, sums)


def solution(mesh):
    rows = P(("dp", "cp"), None)
    return jax.shard_map(
        local,
        mesh=mesh,
        in_specs=(rows, P(("dp", "cp")), rows, rows, P(), P(), P(), rows),
        out_specs=(rows, rows, rows, P(), P(), P()),
        check_vma=False,
    )
```

```python
import math

import jax
import jax.numpy as jnp
from jax import lax
from jax.experimental import pallas as pl
from jax.experimental.pallas import tpu as pltpu
from jax.sharding import PartitionSpec as P

MESH = pl.DeviceIdType.MESH
BF = jnp.bfloat16
F32 = jnp.float32
I32 = jnp.int32
EPSILON = 1e-05

D = 512
HEADS = 8
HEAD = 64
TOK = 128
CAP = 4
HOT = 512
COLD = 2048
COLD_W = 128
N_DP = 8
N_CP = 16
DEVICES = N_DP * N_CP
SLOT = 16
SLOTS = DEVICES * SLOT
BITS = 12
SHIFT = 1 << BITS
CHUNK = 256
PAIRS = HEADS * (HEADS + 1) // 2
W_ROWS = 4 * D + D + COLD_W
LATE = 2 * D
SETS = (
    (0, D, 0, D, {0: (48, 0), 1: (48, 48), 2: (32, 96)}),
    (LATE, 832, D, 768, {0: (64, 128), 1: (64, 192), 2: (64, 256)}),
    (LATE + 768, 832, D + 768, 64, {2: (16, 320)}),
)
PART_ROWS = 336
SENT_KIB = 2 * 4 * (DEVICES - 1) + 16 * (4 * (N_CP - 1) + 4 * (HEADS - 1))


def first_row(n, k):
    return sum(4 * part for color, (part, _) in SETS[n][4].items() if color < k)


FAR_FIRST = sorted(
    (
        (dz, dc, dx, dy)
        for dz in range(4)
        for dc in range(2)
        for dx in range(4)
        for dy in range(4)
        if dz or dc or dx or dy
    ),
    key=lambda o: (-sum(min(v, 4 - v) for v in (o[0], o[2], o[3])), sum(o) * 53 % 7, o),
)


def nn(a, b):
    return jnp.dot(a, b, preferred_element_type=F32)


def nt(a, b, precision=None):
    return lax.dot_general(
        a, b, (((1,), (1,)), ((), ())), preferred_element_type=F32, precision=precision
    )


def sigmoid(v):
    return 0.5 * jnp.tanh(0.5 * v) + 0.5


def silu_slope(v):
    sig = sigmoid(v)
    return sig + v * sig * (1.0 - sig)


def iota(shape, dim):
    return lax.broadcasted_iota(I32, shape, dim)


def turned(v):
    return v.astype(F32).T


def column_norm(v):
    average = jnp.mean(v, axis=0, keepdims=True)
    centred = v - average
    inverse = lax.rsqrt(jnp.mean(centred * centred, axis=0, keepdims=True) + EPSILON)
    return centred * inverse, inverse


def column_norm_back(g, y, inverse):
    first = jnp.mean(g, axis=0, keepdims=True)
    second = jnp.mean(g * y, axis=0, keepdims=True)
    return (g - first - y * second) * inverse


def step_kernel(
    owner_in, slot_in, hot_hbm, cold_hbm, proj_hbm, joined_hbm, wout_hbm, cot_hbm,
    layer_out, hot_sum, cold_sum, total,
    hot, cold, cold_wide, proj, joined, wout, cot, owner_ref, slot_ref, code_row,
    ids_all, pick32, pick16, row_in, take_1h, rows_got, emb_nat, normed_t, inv_ref, cold_t, joined_t,
    hidden_t, active_t, dgated_t, cot_t, slots_1h,
    k_in, v_in, q_in, kv_nat, w_keep, slope_keep, att_out, att_in, da_out, da_in,
    da_nat, da_cat, q_cat, dq_acc, dq_out, dk_out, dv_out, dq_in, dk_in, dv_in, dh_t, pack_ref, grad_out, grad_in, named,
    w_ref, r0, u1, r1, u2, r2, r3, g2,
    send, recv, da_recv, ar_send, ar_recv, last_recv, local_sem,
):
    dp, cp = lax.axis_index("dp"), lax.axis_index("cp")
    me = dp * N_CP + cp
    z, core, x, y = dp // 2, dp % 2, cp // 4, cp % 4
    head = cp // 2
    half = ((cp + 1) // 2) % 2
    xs, ys, zs = ([(v + d) % 4 for d in range(4)] for v in (x, y, z))
    cores = [core, (core + 1) % 2]
    dps = [[zs[dz] * 2 + cores[dc] for dc in range(2)] for dz in range(4)]
    cps = [[xs[dx] * 4 + ys[dy] for dy in range(4)] for dx in range(4)]
    plane = [(dx, dy) for dx in range(4) for dy in range(4) if dx or dy]
    plane.sort(key=lambda o: (-(min(o[0], 4 - o[0]) + min(o[1], 4 - o[1])), (o[0] * 3 + o[1]) % 4))

    def remote(src, dst, send_sem, recv_sem, to):
        return pltpu.make_async_remote_copy(
            src_ref=src, dst_ref=dst, send_sem=send_sem, recv_sem=recv_sem,
            device_id=to, device_id_type=MESH,
        )

    def wait_got(ref, i):
        remote(ref, ref, send.at[0], recv.at[i], (dp, cp)).wait_recv()

    def rows64(h):
        return pl.ds(pl.multiple_of(h * HEAD, HEAD), HEAD)

    def tile(o):
        return pl.ds(pl.multiple_of(o * SLOT, SLOT), SLOT)

    def by_rank(tiles, rows):
        pick32[...] = tiles[...].astype(F32)
        for c in range(CAP):
            for f in range(4):
                rows[c * DEVICES : (c + 1) * DEVICES, f * 128 : (f + 1) * 128] = pick32[
                    pl.ds(CAP * f + c, DEVICES, stride=SLOT), :
                ].astype(BF)

    barrier = pltpu.get_barrier_semaphore()
    everyone = [(dps[dz][dc], cps[dx][dy]) for dz, dc, dx, dy in FAR_FIRST]
    for to in everyone:
        pl.semaphore_signal(barrier, inc=1, device_id=to, device_id_type=MESH)
    loads = [
        pltpu.make_async_copy(src, dst, local_sem.at[i])
        for i, (src, dst) in enumerate(
            ((owner_in, owner_ref), (slot_in, slot_ref), (joined_hbm, joined), (cot_hbm, cot), (wout_hbm, wout), (hot_hbm, hot),
             (cold_hbm, cold), (proj_hbm, proj))
        )
    ]
    for load in loads:
        load.start()
    for load in loads[:2]:
        load.wait()
    owner_row, slot_row = owner_ref[...], slot_ref[...]
    code_row[...] = owner_row * SHIFT + slot_row
    pl.semaphore_wait(barrier, DEVICES - 1)

    for to in everyone:
        remote(code_row, ids_all.at[me], send.at[0], recv.at[0], to).start()
    ids_all[pl.ds(me, 1)] = code_row[...].reshape(1, 1, TOK)

    diagonal = iota((TOK, TOK), 0) == iota((TOK, TOK), 1)

    def as_column(row):
        picked = jnp.where(diagonal, row.astype(F32), 0.0)
        return jnp.sum(picked, axis=1, keepdims=True).astype(I32)

    owner_col, slot_col = as_column(owner_row), as_column(slot_row)
    before_row = (owner_col == owner_row) & (iota((TOK, TOK), 0) < iota((TOK, TOK), 1))
    rank_row = jnp.sum(jnp.where(before_row, 1, 0), axis=0, keepdims=True)
    place_row = owner_row * SLOT + rank_row
    take_1h[...] = jnp.where(
        iota((TOK, CAP * DEVICES), 1) == as_column(rank_row) * DEVICES + owner_col, 1.0, 0.0
    ).astype(BF)
    for f in range(4):
        slots_1h[:, f * TOK : (f + 1) * TOK] = jnp.where(
            iota((SLOTS, TOK), 0) == place_row + CAP * f, 1.0, 0.0
        ).astype(BF)
    for load in loads[2:5]:
        load.wait()
    for b in range(4):
        joined_t[b * D : (b + 1) * D, :] = turned(joined[:, b * D : (b + 1) * D]).astype(BF)
    cot_t[...] = turned(cot[...])
    dgated_t[...] = nn(wout[...], cot_t[...].astype(BF))
    for load in loads[5:]:
        load.wait()
    for g in range(4):
        cold_wide[:, g * 128 : (g + 1) * 128] = cold[g * HOT : (g + 1) * HOT, :]

    wait_got(ids_all.at[pl.ds(0, DEVICES - 1)], 0)

    ids = ids_all[:, 0, :]
    asked = (ids >> BITS) == me
    slot_plus = ((ids & (SHIFT - 1)) + 1).astype(F32)
    upper = jnp.where(iota((TOK, TOK), 0) < iota((TOK, TOK), 1), 1.0, 0.0).astype(BF)
    earlier = nn(jnp.where(asked, 1.0, 0.0).astype(BF), upper)
    asks = [jnp.where(asked & (earlier == float(c)), slot_plus, 0.0) for c in range(CAP)]
    wanted = jnp.concatenate([jnp.sum(ask, axis=1, keepdims=True) for ask in asks], axis=0)
    wanted = wanted.astype(I32) - 1
    group = wanted >> 9
    row = jnp.where(wanted < 0, -1, wanted & (HOT - 1))
    chosen = jnp.where(iota((CAP * DEVICES, HOT), 1) == row, 1.0, 0.0).astype(BF)
    hot_rows = nn(chosen, hot[...])
    cold_rows = nn(chosen, cold_wide[...])
    for f in range(4):
        part = jnp.where(group == 0, hot_rows[:, f * 128 : (f + 1) * 128], 0.0)
        if f == 0:
            for g in range(4):
                part = jnp.where(group == g + 1, cold_rows[:, g * 128 : (g + 1) * 128], part)
        for c in range(CAP):
            pick32[pl.ds(CAP * f + c, DEVICES, stride=SLOT), :] = part[
                c * DEVICES : (c + 1) * DEVICES, :
            ]
    pick16[...] = pick32[...].astype(BF)

    for to in everyone:
        remote(
            pick16.at[tile(to[0] * N_CP + to[1])], row_in.at[tile(me)], send.at[1], recv.at[1], to
        ).start()
    row_in[tile(me), :] = pick16[tile(me), :]
    for c in range(CAP):
        wanted_row = jnp.sum(asks[c].T, axis=0, keepdims=True)
        named[:, c * DEVICES : (c + 1) * DEVICES] = jnp.where(
            iota((HOT + COLD, DEVICES), 0) == wanted_row.astype(I32) - 1, 1.0, 0.0
        ).astype(BF)

    wait_got(row_in.at[pl.ds(0, SLOTS - SLOT)], 1)

    by_rank(row_in, rows_got)
    fetched = nn(take_1h[...], rows_got[...])
    cold_vec = fetched[:, 0:COLD_W]
    cold_embed = nn(cold_vec.astype(BF), proj[...])
    embedded = jnp.where(slot_col < HOT, fetched, cold_embed)
    emb_nat[...] = embedded
    normed, inverse = column_norm(embedded.T)
    normed_t[...] = normed
    inv_ref[...] = jnp.broadcast_to(inverse, inv_ref.shape)
    low = normed.astype(BF)

    def k_rows(h):
        return pl.ds(pl.multiple_of(3 * D + h * HEAD, HEAD), HEAD)

    def v_rows(h):
        return pl.ds(pl.multiple_of(D + h * HEAD, HEAD), HEAD)

    def q_rows(h):
        return pl.ds(pl.multiple_of(2 * D + h * HEAD, HEAD), HEAD)

    def same_half(d):
        h = (head + d) % HEADS
        return h, (dp, 2 * h + (half + h) % 2)

    def project(b):
        hid = nn(joined_t[b * D : (b + 1) * D, :], low)
        hidden_t[b * D : (b + 1) * D, :] = hid
        active_t[b * D : (b + 1) * D, :] = (hid * sigmoid(hid)).astype(BF)

    project(3)
    for dx, dy in plane:
        pcp = cps[dx][dy]
        remote(active_t.at[k_rows(pcp // 2)], k_in.at[cp], send.at[1], recv.at[2], (dp, pcp)).start()
    project(1)
    for dx, dy in plane:
        pcp = cps[dx][dy]
        remote(active_t.at[v_rows(pcp // 2)], v_in.at[cp], send.at[1], recv.at[3], (dp, pcp)).start()
    project(2)
    for d in range(1, HEADS):
        h, to = same_half(d)
        remote(active_t.at[q_rows(h)], q_in.at[head], send.at[1], recv.at[4], to).start()
    k_in[pl.ds(cp, 1)] = active_t[k_rows(head), :].reshape(1, HEAD, TOK)
    v_in[pl.ds(cp, 1)] = active_t[v_rows(head), :].reshape(1, HEAD, TOK)
    q_in[pl.ds(head, 1)] = active_t[q_rows(head), :].reshape(1, HEAD, TOK)
    project(0)
    cold_t[...] = jnp.where(slot_row < HOT, 0.0, cold_vec.T)
    wait_got(k_in.at[pl.ds(0, N_CP - 1)], 2)
    wait_got(v_in.at[pl.ds(0, N_CP - 1)], 3)
    wait_got(q_in.at[pl.ds(0, HEADS - 1)], 4)

    def block_of(i):
        return 4 * (i // 2) + (half if i % 2 == 0 else 3 - half)

    def pair(ref, c):
        return jnp.concatenate([ref[2 * c], ref[2 * c + 1]], axis=1)

    def kept(c, i, count):
        at = sum(HEADS - b for b in range(c)) + i - c
        return pl.ds(at * TOK, count * TOK)

    shrink = 0.5 / math.sqrt(HEAD)
    def attend(i):
        q_nat = (turned(q_in[i]) * shrink).astype(BF)
        sums = jnp.zeros((HEAD, TOK), F32)
        for c in range(i + 1):
            s = nn(q_nat, pair(k_in, c))
            up = 1.0 + jnp.tanh(s)
            w = s * up
            slope = up + w * (2.0 - up)
            if c == i:
                ok = (iota((TOK, CHUNK), 1) + c * CHUNK) <= (
                    iota((TOK, CHUNK), 0) + block_of(i) * TOK
                )
                w = jnp.where(ok, w, 0.0)
                slope = jnp.where(ok, slope, 0.0)
            w = w.astype(BF)
            w_keep[kept(c, i, 1), :] = w
            slope_keep[kept(c, i, 1), :] = slope
            sums = sums + nt(pair(v_in, c), w)
        att_out[i] = sums.astype(BF)

    for group in ((7, 6, 5), (4, 3, 2, 1, 0)):
        for i in group:
            attend(i)
        for i in group:

            @pl.when(head != i)
            def _():
                remote(
                    att_out.at[i], att_in.at[rows64(head)], send.at[1], recv.at[5],
                    (dp, block_of(i)),
                ).start()

    att_in[rows64(head), :] = att_out[pl.ds(head, 1)].reshape(HEAD, TOK)
    wait_got(att_in.at[pl.ds(0, D - HEAD)], 5)

    mixed, inv_mix = column_norm(att_in[...].astype(F32))
    gate = active_t[0:D, :].astype(F32)
    dgated = dgated_t[...]
    da_out[...] = column_norm_back(dgated * gate, mixed, inv_mix).astype(BF)
    for d in range(1, HEADS):
        h, to = same_half(d)
        remote(da_out.at[rows64(h)], da_in.at[head], send.at[1], da_recv.at[head], to).start()
    da_in[pl.ds(head, 1)] = da_out[rows64(head), :].reshape(1, HEAD, TOK)

    sibling = (z * 2 + (1 - core), cp)
    place = (x, y, z)

    def along(dim, d):
        moved = [xs[0], ys[0], zs[0]]
        moved[dim] = (xs, ys, zs)[dim][d]
        return moved[dim], (moved[2] * 2 + core, moved[0] * 4 + moved[1])

    def ar(src, dst, n, stage, k, to):
        at = (0, 14, 28)[n]
        if stage in (1, 2, 3, 4):
            at += stage if n == 2 else 3 * stage - 2 + k
        elif stage == 6:
            at += 5 if n == 2 else 13
        return remote(src, dst, ar_send.at[n], ar_recv.at[at], to)

    def ar_got(ref, n, stage, k):
        ar(ref, ref, n, stage, k, (dp, cp)).wait_recv()

    def core_rows(n, c):
        return pl.ds(pl.multiple_of(SETS[n][0] + c * SETS[n][1], 16), SETS[n][3])

    def set_rows(n):
        return pl.ds(SETS[n][2], SETS[n][3])

    def stage0(n):
        ar(w_ref.at[core_rows(n, 1 - core)], r0.at[set_rows(n)], n, 0, 0, sibling).start()

    def piece(n, k):
        part, at = SETS[n][4][k]
        return pl.ds(at, part)

    def u1_rows(n, k, a):
        part = SETS[n][4][k][0]
        return pl.ds(pl.multiple_of(SETS[n][2] + first_row(n, k) + a * part, 16), part)

    def stage1(n):
        at = set_rows(n)
        ar_got(r0.at[at], n, 0, 0)
        u1[at, :] = (w_ref[core_rows(n, core), :].astype(F32) + r0[at, :].astype(F32)).astype(BF)
        for k in SETS[n][4]:
            for d in (2, 1, 3):
                a, to = along(k, d)
                ar(u1.at[u1_rows(n, k, a)], r1.at[d - 1, piece(n, k)], n, 1, k, to).start()

    def stage2(n, k):
        at = piece(n, k)
        ar_got(r1.at[:, at], n, 1, k)
        part = u1[u1_rows(n, k, place[k]), :].astype(F32)
        for d in range(3):
            part = part + r1[d, at, :].astype(F32)
        for b in range(4):
            u2[b, at, :] = part[:, b * 128 : (b + 1) * 128].astype(BF)
        for d in (2, 1, 3):
            b, to = along((k + 1) % 3, d)
            ar(u2.at[b, at], r2.at[d - 1, at], n, 2, k, to).start()

    def stage3(n, k):
        at = piece(n, k)
        ar_got(r2.at[:, at], n, 2, k)
        b_me, c_me = place[(k + 1) % 3], place[(k + 2) % 3]
        part = u2[pl.ds(b_me, 1), at, :].astype(F32)
        for d in range(3):
            part = part + r2[d : d + 1, at, :].astype(F32)
        r3[pl.ds(c_me, 1), at, :] = part.astype(BF)
        for d in (2, 1, 3):
            _, to = along((k + 2) % 3, d)
            ar(r3.at[c_me, at], r3.at[c_me, at], n, 3, k, to).start()

    def stage4(n, k):
        at = piece(n, k)
        ar_got(r3.at[pl.ds(0, 3), at], n, 3, k)
        b_me = place[(k + 1) % 3]
        part = r3[0:1, at, :].astype(F32)
        for d in range(1, 4):
            part = part + r3[d : d + 1, at, :].astype(F32)
        g2[pl.ds(b_me, 1), at, :] = part.astype(BF)
        for d in (2, 1, 3):
            _, to = along((k + 1) % 3, d)
            ar(g2.at[b_me, at], g2.at[b_me, at], n, 4, k, to).start()

    def to_sibling(n, k, a):
        held = total.at[core, a, :, piece(n, k)]
        ar(held, held, n, 6, k, sibling).start()

    def stage5(n, k):
        at = piece(n, k)
        ar_got(g2.at[pl.ds(0, 3), at], n, 4, k)
        a_me = place[k]
        for d in (2, 1, 3):
            _, to = along(k, d)
            remote(
                g2.at[:, at], total.at[core, a_me, :, at],
                ar_send.at[n], last_recv.at[n, d - 1], to,
            ).start()
        total[pl.ds(core, 1), pl.ds(a_me, 1), :, at, :] = g2[:, at, :].reshape(
            1, 1, 4, SETS[n][4][k][0], 128
        )
        to_sibling(n, k, a_me)

    def set_pieces(n):
        return pl.ds(min(at for _, at in SETS[n][4].values()), SETS[n][3] // 4)

    def stage6(n):
        for d in (1, 3, 2):
            held = total.at[0, 0, :, set_pieces(n)]
            remote(held, held, ar_send.at[n], last_recv.at[n, d - 1], (dp, cp)).wait_recv()
            for k in SETS[n][4]:
                to_sibling(n, k, along(k, 4 - d)[0])

    def stage7(n):
        ar_got(total.at[0, :, :, set_pieces(n)], n, 6, 0)

    def all_colors(stage, n):
        for k in SETS[n][4]:
            stage(n, k)

    def settle(n):
        kib = SETS[n][3] * 65 // 16
        sent = pick32.at[pl.ds(0, 2 * kib)] if n == 2 else slope_keep.at[pl.ds(0, kib)]
        remote(sent, sent, ar_send.at[n], ar_recv.at[0], (dp, cp)).wait_send()

    gated = (mixed * gate).astype(BF)
    low = normed_t[...].astype(BF)
    dh_gate = (dgated * mixed * silu_slope(hidden_t[0:D, :])).astype(BF)
    dh_t[0:D, :] = dh_gate
    w_ref[0:D, :] = nt(low, dh_gate).astype(BF)
    w_ref[D : 2 * D, :] = nn(gated, cot[...]).astype(BF)
    stage0(0)
    branch = nn(turned(gated).astype(BF), wout[...])
    layer_out[...] = (emb_nat[...] + branch).astype(BF)

    for i in range(HEADS):
        q_cat[:, i * TOK : (i + 1) * TOK] = q_in[i]
    for b in range(N_CP):
        kv_nat[b * TOK : (b + 1) * TOK, :] = turned(
            jnp.concatenate([k_in[b], v_in[b]], axis=0)
        ).astype(BF)

    def backward(c):
        da_nat[c * TOK : (c + 1) * TOK, :] = (turned(da_in[c]) * shrink).astype(BF)
        da_cat[:, c * TOK : (c + 1) * TOK] = da_in[c]
        rows = slice(c * TOK, HEADS * TOK)
        at = kept(c, c, HEADS - c)
        ds = (nn(da_nat[rows, :], pair(v_in, c)) * slope_keep[at, :]).astype(BF)
        dk = nn(q_cat[:, rows], ds).astype(BF)
        dv = nn(da_cat[:, rows], w_keep[at, :]).astype(BF)
        for b in range(2):
            dk_out[2 * c + b] = dk[:, b * TOK : (b + 1) * TOK]
            dv_out[2 * c + b] = dv[:, b * TOK : (b + 1) * TOK]
        dq = nn(ds, kv_nat[c * CHUNK : (c + 1) * CHUNK, :])
        if c < HEADS - 1:
            dq_acc[(c + 1) * TOK :, :] += dq[TOK:, :]
        dq_acc[c * TOK : (c + 1) * TOK, :] = dq[0:TOK, :]

    for group in ((7, 6, 5), (4, 3), (2, 1), (0,)):
        for c in group:

            @pl.when(head != c)
            def _():
                remote(
                    da_in.at[c], da_in.at[c], send.at[1], da_recv.at[c], (dp, cp)
                ).wait_recv()

        for c in group:
            backward(c)
        if group == (0,):
            for i in range(HEADS):
                dq_out[i] = dq_acc[i * TOK : (i + 1) * TOK, :].T[:HEAD, :].astype(BF)
        if group == (7, 6, 5):
            stage1(0)
        for kb in [2 * c + b for c in group for b in range(2)]:

            @pl.when(cp != kb)
            def _():
                remote(
                    dk_out.at[kb], dk_in.at[half, rows64(head)], send.at[1], recv.at[7], (dp, kb)
                ).start()
                remote(
                    dv_out.at[kb], dv_in.at[half, rows64(head)], send.at[1], recv.at[8], (dp, kb)
                ).start()

    for i in range(HEADS):

        @pl.when(head != i)
        def _():
            remote(
                dq_out.at[i], dq_in.at[rows64(head)], send.at[1], recv.at[9], (dp, block_of(i))
            ).start()

    all_colors(stage2, 0)

    dq_in[rows64(head), :] = dq_out[pl.ds(head, 1)].reshape(HEAD, TOK)
    dk_in[pl.ds(half, 1), rows64(head), :] = dk_out[pl.ds(cp, 1)]
    dv_in[pl.ds(half, 1), rows64(head), :] = dv_out[pl.ds(cp, 1)]
    wait_got(dk_out.at[pl.ds(0, N_CP - 1)], 7)
    wait_got(dv_out.at[pl.ds(0, N_CP - 1)], 8)
    wait_got(dq_in.at[pl.ds(0, D - HEAD)], 9)

    def column_back(b, grad):
        dh = (grad * silu_slope(hidden_t[b * D : (b + 1) * D, :])).astype(BF)
        dh_t[b * D : (b + 1) * D, :] = dh
        grads = nt(low, dh).astype(BF)
        if b == 1:
            w_ref[LATE : LATE + D, :] = grads
        elif b == 2:
            w_ref[LATE + D : LATE + 768, :] = grads[0:256]
            w_ref[LATE + 832 : LATE + 1088, :] = grads[256:512]
        else:
            w_ref[LATE + 1088 : LATE + 1600, :] = grads

    column_back(1, dv_in[0].astype(F32) + dv_in[1].astype(F32))
    column_back(2, dq_in[...].astype(F32))
    column_back(3, dk_in[0].astype(F32) + dk_in[1].astype(F32))
    stage0(1)
    dnormed = nn(joined[...], dh_t[...])
    dembed = column_norm_back(dnormed, normed_t[...], inv_ref[0:1, :]) + cot_t[...]
    exact = lax.Precision.HIGHEST
    all_colors(stage3, 0)
    stage1(1)
    proj_grads = nt(cold_t[...], dembed, exact).astype(BF)
    w_ref[LATE + 768 : LATE + 832, :] = proj_grads[0:64]
    w_ref[LATE + 1600 : LATE + 1664, :] = proj_grads[64:128]
    stage0(2)

    cold_event = lax.dot_general(
        proj[...].astype(F32), dembed, (((1,), (0,)), ((), ())),
        preferred_element_type=F32, precision=exact,
    )
    is_hot = slot_row < HOT
    for f in range(4):
        part = dembed[f * 128 : (f + 1) * 128, :]
        pack_ref[:, f * TOK : (f + 1) * TOK] = jnp.where(
            is_hot, part, cold_event if f == 0 else 0.0
        ).astype(BF)
    grad_out[...] = nt(slots_1h[...], pack_ref[...]).astype(BF)
    grad_in[tile(me), :] = grad_out[tile(me), :]

    def send_grads(group):
        for to in everyone[group::4]:
            remote(
                grad_out.at[tile(to[0] * N_CP + to[1])], grad_in.at[tile(me)],
                send.at[1], recv.at[10], to,
            ).start()

    stage1(2)
    all_colors(stage4, 0)
    send_grads(0)
    all_colors(stage2, 1)
    all_colors(stage2, 2)
    all_colors(stage5, 0)
    all_colors(stage3, 1)
    all_colors(stage3, 2)
    send_grads(1)
    send_grads(2)
    all_colors(stage4, 1)
    all_colors(stage4, 2)
    send_grads(3)
    all_colors(stage5, 1)
    all_colors(stage5, 2)
    stage6(0)
    stage6(1)
    stage6(2)

    wait_got(grad_in.at[pl.ds(0, SLOTS - SLOT)], 10)
    by_rank(grad_in, rows_got)

    hot_sum[...] = nn(named[0:HOT, :], rows_got[...])
    cold_sum[...] = nn(named[HOT:, :], rows_got[:, 0:COLD_W])

    sent = ids_all.at[pl.ds(0, DEVICES - 1)]
    remote(sent, sent, send.at[0], recv.at[0], (dp, cp)).wait_send()
    sent = slope_keep.at[pl.ds(0, SENT_KIB)]
    remote(sent, sent, send.at[1], recv.at[0], (dp, cp)).wait_send()
    settle(0)
    for n in range(3):
        stage7(n)
    settle(1)
    settle(2)


def finish_kernel(
    layer, hot_sum, cold_sum, sums,
    layer_out, hot_out, cold_out, proj_out, joined_out, wout_out,
    sum_buf, sem,
):
    copies = []

    def put(src, dst):
        copy = pltpu.make_async_copy(src, dst, sem.at[len(copies)])
        copy.start()
        copies.append(copy)

    put(layer, layer_out)
    put(hot_sum, hot_out)
    put(cold_sum, cold_out)
    scale = (TOK * DEVICES) ** -0.5

    def scaled(n, core):
        home = (4 * D * core, D + 768 * core, 5 * D + 64 * core)[n]
        for k, (count, at) in SETS[n][4].items():
            for a in range(4):
                top = home + first_row(n, k) + a * count
                for b in range(4):
                    sum_buf[top : top + count, b * 128 : (b + 1) * 128] = (
                        sums[core, a, b, at : at + count, :].astype(F32) * scale
                    )

    def put_joined(b):
        put(sum_buf.at[pl.ds(b * D, D)], joined_out.at[:, pl.ds(b * D, D)])

    scaled(0, 0)
    put_joined(0)
    scaled(1, 0)
    put_joined(1)
    scaled(1, 1)
    put_joined(2)
    put_joined(3)
    scaled(0, 1)
    put(sum_buf.at[pl.ds(4 * D, D)], wout_out)
    scaled(2, 0)
    scaled(2, 1)
    put(sum_buf.at[pl.ds(5 * D, COLD_W)], proj_out)
    for copy in copies:
        copy.wait()


def vmem(n):
    return [pl.BlockSpec(memory_space=pltpu.VMEM)] * n


def anywhere(n):
    return [pl.BlockSpec(memory_space=pl.ANY)] * n


def hbm(n):
    return [pl.BlockSpec(memory_space=pltpu.HBM)] * n


def local(row_owner, slot_row, hot, cold, proj, joined, wout, cot):
    v = pltpu.VMEM
    operands = [row_owner.reshape(1, TOK), slot_row.reshape(1, TOK)]
    operands += [hot, cold, proj, joined, wout, cot]
    operands = [pltpu.with_memory_space_constraint(a, pltpu.HBM) for a in operands]
    layer, hot_sum, cold_sum, sums = pl.pallas_call(
        step_kernel,
        out_shape=(
            jax.ShapeDtypeStruct((TOK, D), BF),
            jax.ShapeDtypeStruct((HOT, D), F32),
            jax.ShapeDtypeStruct((COLD, COLD_W), F32),
            jax.ShapeDtypeStruct((2, 4, 4, PART_ROWS, 128), BF),
        ),
        in_specs=hbm(8),
        out_specs=tuple(vmem(4)),
        scratch_shapes=[
            v((HOT, D), BF), v((COLD, COLD_W), BF), v((HOT, 4 * COLD_W), BF),
            v((COLD_W, D), BF), v((D, 4 * D), BF),
            v((D, D), BF), v((TOK, D), BF), v((1, TOK), I32), v((1, TOK), I32),
            v((1, TOK), I32),
            v((DEVICES, 1, TOK), I32), v((SLOTS, 128), F32), v((SLOTS, 128), BF),
            v((SLOTS, 128), BF), v((TOK, CAP * DEVICES), BF), v((CAP * DEVICES, D), BF),
            v((TOK, D), F32), v((D, TOK), F32), v((8, TOK), F32),
            v((COLD_W, TOK), F32), v((4 * D, D), BF),
            v((4 * D, TOK), F32), v((4 * D, TOK), BF), v((D, TOK), F32), v((D, TOK), F32),
            v((SLOTS, 4 * TOK), BF),
            v((N_CP, HEAD, TOK), BF), v((N_CP, HEAD, TOK), BF), v((HEADS, HEAD, TOK), BF),
            v((N_CP * TOK, 2 * HEAD), BF),
            v((PAIRS * TOK, CHUNK), BF), v((PAIRS * TOK, CHUNK), F32),
            v((HEADS, HEAD, TOK), BF), v((D, TOK), BF), v((D, TOK), BF),
            v((HEADS, HEAD, TOK), BF),
            v((HEADS * TOK, HEAD), BF), v((HEAD, HEADS * TOK), BF), v((HEAD, HEADS * TOK), BF),
            v((HEADS * TOK, 2 * HEAD), F32),
            v((HEADS, HEAD, TOK), BF),
            v((N_CP, HEAD, TOK), BF), v((N_CP, HEAD, TOK), BF),
            v((D, TOK), BF), v((2, D, TOK), BF), v((2, D, TOK), BF),
            v((4 * D, TOK), BF), v((128, 4 * TOK), BF),
            v((SLOTS, 128), BF), v((SLOTS, 128), BF), v((HOT + COLD, CAP * DEVICES), BF),
            v((W_ROWS, D), BF), v((W_ROWS // 2, D), BF), v((W_ROWS // 2, D), BF),
            v((3, PART_ROWS, D), BF), v((4, PART_ROWS, 128), BF),
            v((3, PART_ROWS, 128), BF), v((4, PART_ROWS, 128), BF),
            v((4, PART_ROWS, 128), BF),
            pltpu.SemaphoreType.DMA((2,)), pltpu.SemaphoreType.DMA((11,)),
            pltpu.SemaphoreType.DMA((HEADS,)),
            pltpu.SemaphoreType.DMA((3,)), pltpu.SemaphoreType.DMA((34,)),
            pltpu.SemaphoreType.DMA((3, 3)),
            pltpu.SemaphoreType.DMA((8,)),
        ],
        compiler_params=pltpu.CompilerParams(
            collective_id=0, has_side_effects=True, vmem_limit_bytes=44 << 20
        ),
        name="step",
    )(*operands)
    return pl.pallas_call(
        finish_kernel,
        out_shape=(
            jax.ShapeDtypeStruct((TOK, D), BF),
            jax.ShapeDtypeStruct((HOT, D), F32),
            jax.ShapeDtypeStruct((COLD, COLD_W), F32),
            jax.ShapeDtypeStruct((COLD_W, D), F32),
            jax.ShapeDtypeStruct((D, 4 * D), F32),
            jax.ShapeDtypeStruct((D, D), F32),
        ),
        in_specs=vmem(4),
        out_specs=tuple(hbm(6)),
        scratch_shapes=[
            v((W_ROWS, D), F32),
            pltpu.SemaphoreType.DMA((9,)),
        ],
        compiler_params=pltpu.CompilerParams(vmem_limit_bytes=20 << 20),
        name="finish",
    )(layer, hot_sum, cold_sum, sums)


def solution(mesh):
    rows = P(("dp", "cp"), None)
    return jax.shard_map(
        local,
        mesh=mesh,
        in_specs=(rows, P(("dp", "cp")), rows, rows, P(), P(), P(), rows),
        out_specs=(rows, rows, rows, P(), P(), P()),
        check_vma=False,
    )
```

```python
import math

import jax
import jax.numpy as jnp
from jax import lax
from jax.experimental import pallas as pl
from jax.experimental.pallas import tpu as pltpu
from jax.sharding import PartitionSpec as P

MESH = pl.DeviceIdType.MESH
BF = jnp.bfloat16
F32 = jnp.float32
I32 = jnp.int32
EPSILON = 1e-05

D = 512
HEADS = 8
HEAD = 64
TOK = 128
CAP = 4
HOT = 512
COLD = 2048
COLD_W = 128
N_DP = 8
N_CP = 16
DEVICES = N_DP * N_CP
SLOT = 16
SLOTS = DEVICES * SLOT
BITS = 12
SHIFT = 1 << BITS
CHUNK = 256
PAIRS = HEADS * (HEADS + 1) // 2
W_ROWS = 4 * D + D + COLD_W
LATE = 2 * D
SETS = (
    (0, D, 0, D, {0: (48, 0), 1: (48, 48), 2: (32, 96)}),
    (LATE, 832, D, 768, {0: (64, 128), 1: (64, 192), 2: (64, 256)}),
    (LATE + 768, 832, D + 768, 64, {2: (16, 320)}),
)
PART_ROWS = 336
SENT_KIB = 2 * 4 * (DEVICES - 1) + 16 * (4 * (N_CP - 1) + 4 * (HEADS - 1))


def first_row(n, k):
    return sum(4 * part for color, (part, _) in SETS[n][4].items() if color < k)


FAR_FIRST = sorted(
    (
        (dz, dc, dx, dy)
        for dz in range(4)
        for dc in range(2)
        for dx in range(4)
        for dy in range(4)
        if dz or dc or dx or dy
    ),
    key=lambda o: (-sum(min(v, 4 - v) for v in (o[0], o[2], o[3])), sum(o) * 53 % 7, o),
)


def nn(a, b):
    return jnp.dot(a, b, preferred_element_type=F32)


def nt(a, b, precision=None):
    return lax.dot_general(
        a, b, (((1,), (1,)), ((), ())), preferred_element_type=F32, precision=precision
    )


def sigmoid(v):
    return 0.5 * jnp.tanh(0.5 * v) + 0.5


def silu_slope(v):
    sig = sigmoid(v)
    return sig + v * sig * (1.0 - sig)


def iota(shape, dim):
    return lax.broadcasted_iota(I32, shape, dim)


def turned(v):
    return v.astype(F32).T


def column_norm(v):
    average = jnp.mean(v, axis=0, keepdims=True)
    centred = v - average
    inverse = lax.rsqrt(jnp.mean(centred * centred, axis=0, keepdims=True) + EPSILON)
    return centred * inverse, inverse


def column_norm_back(g, y, inverse):
    first = jnp.mean(g, axis=0, keepdims=True)
    second = jnp.mean(g * y, axis=0, keepdims=True)
    return (g - first - y * second) * inverse


def step_kernel(
    owner_in, slot_in, hot_hbm, cold_hbm, proj_hbm, joined_hbm, wout_hbm, cot_hbm,
    layer_out, hot_sum, cold_sum, total,
    hot, cold, cold_wide, proj, joined, wout, cot, owner_ref, slot_ref, code_row,
    ids_all, pick32, pick16, row_in, take_1h, rows_got, emb_nat, normed_t, inv_ref, cold_t, joined_t,
    hidden_t, active_t, dgated_t, cot_t, slots_1h,
    k_in, v_in, q_in, kv_nat, w_keep, slope_keep, att_out, att_in, da_out, da_in,
    da_nat, da_cat, q_cat, dq_acc, dq_out, dk_out, dv_out, dq_in, dk_in, dv_in, dh_t, pack_ref, grad_out, grad_in, named,
    w_ref, r0, u1, r1, u2, r2, r3, g2,
    send, recv, da_recv, ar_send, ar_recv, last_recv, local_sem,
):
    dp, cp = lax.axis_index("dp"), lax.axis_index("cp")
    me = dp * N_CP + cp
    z, core, x, y = dp // 2, dp % 2, cp // 4, cp % 4
    head = cp // 2
    half = ((cp + 1) // 2) % 2
    xs, ys, zs = ([(v + d) % 4 for d in range(4)] for v in (x, y, z))
    cores = [core, (core + 1) % 2]
    dps = [[zs[dz] * 2 + cores[dc] for dc in range(2)] for dz in range(4)]
    cps = [[xs[dx] * 4 + ys[dy] for dy in range(4)] for dx in range(4)]
    plane = [(dx, dy) for dx in range(4) for dy in range(4) if dx or dy]
    plane.sort(key=lambda o: (-(min(o[0], 4 - o[0]) + min(o[1], 4 - o[1])), (o[0] * 3 + o[1]) % 4))

    def remote(src, dst, send_sem, recv_sem, to):
        return pltpu.make_async_remote_copy(
            src_ref=src, dst_ref=dst, send_sem=send_sem, recv_sem=recv_sem,
            device_id=to, device_id_type=MESH,
        )

    def wait_got(ref, i):
        remote(ref, ref, send.at[0], recv.at[i], (dp, cp)).wait_recv()

    def rows64(h):
        return pl.ds(pl.multiple_of(h * HEAD, HEAD), HEAD)

    def tile(o):
        return pl.ds(pl.multiple_of(o * SLOT, SLOT), SLOT)

    def by_rank(tiles, rows):
        pick32[...] = tiles[...].astype(F32)
        for c in range(CAP):
            for f in range(4):
                rows[c * DEVICES : (c + 1) * DEVICES, f * 128 : (f + 1) * 128] = pick32[
                    pl.ds(CAP * f + c, DEVICES, stride=SLOT), :
                ].astype(BF)

    barrier = pltpu.get_barrier_semaphore()
    everyone = [(dps[dz][dc], cps[dx][dy]) for dz, dc, dx, dy in FAR_FIRST]
    for to in everyone:
        pl.semaphore_signal(barrier, inc=1, device_id=to, device_id_type=MESH)
    loads = [
        pltpu.make_async_copy(src, dst, local_sem.at[i])
        for i, (src, dst) in enumerate(
            ((owner_in, owner_ref), (slot_in, slot_ref), (joined_hbm, joined), (cot_hbm, cot), (wout_hbm, wout), (hot_hbm, hot),
             (cold_hbm, cold), (proj_hbm, proj))
        )
    ]
    for load in loads:
        load.start()
    for load in loads[:2]:
        load.wait()
    owner_row, slot_row = owner_ref[...], slot_ref[...]
    code_row[...] = owner_row * SHIFT + slot_row
    pl.semaphore_wait(barrier, DEVICES - 1)

    for to in everyone:
        remote(code_row, ids_all.at[me], send.at[0], recv.at[0], to).start()
    ids_all[pl.ds(me, 1)] = code_row[...].reshape(1, 1, TOK)

    diagonal = iota((TOK, TOK), 0) == iota((TOK, TOK), 1)

    def as_column(row):
        picked = jnp.where(diagonal, row.astype(F32), 0.0)
        return jnp.sum(picked, axis=1, keepdims=True).astype(I32)

    owner_col, slot_col = as_column(owner_row), as_column(slot_row)
    before_row = (owner_col == owner_row) & (iota((TOK, TOK), 0) < iota((TOK, TOK), 1))
    rank_row = jnp.sum(jnp.where(before_row, 1, 0), axis=0, keepdims=True)
    place_row = owner_row * SLOT + rank_row
    take_1h[...] = jnp.where(
        iota((TOK, CAP * DEVICES), 1) == as_column(rank_row) * DEVICES + owner_col, 1.0, 0.0
    ).astype(BF)
    for f in range(4):
        slots_1h[:, f * TOK : (f + 1) * TOK] = jnp.where(
            iota((SLOTS, TOK), 0) == place_row + CAP * f, 1.0, 0.0
        ).astype(BF)
    for load in loads[2:5]:
        load.wait()
    for b in range(4):
        joined_t[b * D : (b + 1) * D, :] = turned(joined[:, b * D : (b + 1) * D]).astype(BF)
    cot_t[...] = turned(cot[...])
    dgated_t[...] = nn(wout[...], cot_t[...].astype(BF))
    for load in loads[5:]:
        load.wait()
    for g in range(4):
        cold_wide[:, g * 128 : (g + 1) * 128] = cold[g * HOT : (g + 1) * HOT, :]

    wait_got(ids_all.at[pl.ds(0, DEVICES - 1)], 0)

    ids = ids_all[:, 0, :]
    asked = (ids >> BITS) == me
    slot_plus = ((ids & (SHIFT - 1)) + 1).astype(F32)
    upper = jnp.where(iota((TOK, TOK), 0) < iota((TOK, TOK), 1), 1.0, 0.0).astype(BF)
    earlier = nn(jnp.where(asked, 1.0, 0.0).astype(BF), upper)
    asks = [jnp.where(asked & (earlier == float(c)), slot_plus, 0.0) for c in range(CAP)]
    wanted = jnp.concatenate([jnp.sum(ask, axis=1, keepdims=True) for ask in asks], axis=0)
    wanted = wanted.astype(I32) - 1
    group = wanted >> 9
    row = jnp.where(wanted < 0, -1, wanted & (HOT - 1))
    chosen = jnp.where(iota((CAP * DEVICES, HOT), 1) == row, 1.0, 0.0).astype(BF)
    hot_rows = nn(chosen, hot[...])
    cold_rows = nn(chosen, cold_wide[...])
    for f in range(4):
        part = jnp.where(group == 0, hot_rows[:, f * 128 : (f + 1) * 128], 0.0)
        if f == 0:
            for g in range(4):
                part = jnp.where(group == g + 1, cold_rows[:, g * 128 : (g + 1) * 128], part)
        for c in range(CAP):
            pick32[pl.ds(CAP * f + c, DEVICES, stride=SLOT), :] = part[
                c * DEVICES : (c + 1) * DEVICES, :
            ]
    pick16[...] = pick32[...].astype(BF)

    for to in everyone:
        remote(
            pick16.at[tile(to[0] * N_CP + to[1])], row_in.at[tile(me)], send.at[1], recv.at[1], to
        ).start()
    row_in[tile(me), :] = pick16[tile(me), :]
    for c in range(CAP):
        wanted_row = jnp.sum(asks[c].T, axis=0, keepdims=True)
        named[:, c * DEVICES : (c + 1) * DEVICES] = jnp.where(
            iota((HOT + COLD, DEVICES), 0) == wanted_row.astype(I32) - 1, 1.0, 0.0
        ).astype(BF)

    wait_got(row_in.at[pl.ds(0, SLOTS - SLOT)], 1)

    by_rank(row_in, rows_got)
    fetched = nn(take_1h[...], rows_got[...])
    cold_vec = fetched[:, 0:COLD_W]
    cold_embed = nn(cold_vec.astype(BF), proj[...])
    embedded = jnp.where(slot_col < HOT, fetched, cold_embed)
    emb_nat[...] = embedded
    normed, inverse = column_norm(embedded.T)
    normed_t[...] = normed
    inv_ref[...] = jnp.broadcast_to(inverse, inv_ref.shape)
    low = normed.astype(BF)

    def k_rows(h):
        return pl.ds(pl.multiple_of(3 * D + h * HEAD, HEAD), HEAD)

    def v_rows(h):
        return pl.ds(pl.multiple_of(D + h * HEAD, HEAD), HEAD)

    def q_rows(h):
        return pl.ds(pl.multiple_of(2 * D + h * HEAD, HEAD), HEAD)

    def same_half(d):
        h = (head + d) % HEADS
        return h, (dp, 2 * h + (half + h) % 2)

    def project(b):
        hid = nn(joined_t[b * D : (b + 1) * D, :], low)
        hidden_t[b * D : (b + 1) * D, :] = hid
        active_t[b * D : (b + 1) * D, :] = (hid * sigmoid(hid)).astype(BF)

    project(3)
    for dx, dy in plane:
        pcp = cps[dx][dy]
        remote(active_t.at[k_rows(pcp // 2)], k_in.at[cp], send.at[1], recv.at[2], (dp, pcp)).start()
    project(1)
    for dx, dy in plane:
        pcp = cps[dx][dy]
        remote(active_t.at[v_rows(pcp // 2)], v_in.at[cp], send.at[1], recv.at[3], (dp, pcp)).start()
    project(2)
    for d in range(1, HEADS):
        h, to = same_half(d)
        remote(active_t.at[q_rows(h)], q_in.at[head], send.at[1], recv.at[4], to).start()
    k_in[pl.ds(cp, 1)] = active_t[k_rows(head), :].reshape(1, HEAD, TOK)
    v_in[pl.ds(cp, 1)] = active_t[v_rows(head), :].reshape(1, HEAD, TOK)
    q_in[pl.ds(head, 1)] = active_t[q_rows(head), :].reshape(1, HEAD, TOK)
    project(0)
    cold_t[...] = jnp.where(slot_row < HOT, 0.0, cold_vec.T)
    wait_got(k_in.at[pl.ds(0, N_CP - 1)], 2)
    wait_got(v_in.at[pl.ds(0, N_CP - 1)], 3)
    wait_got(q_in.at[pl.ds(0, HEADS - 1)], 4)

    def block_of(i):
        return 4 * (i // 2) + (half if i % 2 == 0 else 3 - half)

    def pair(ref, c):
        return jnp.concatenate([ref[2 * c], ref[2 * c + 1]], axis=1)

    def kept(c, i, count):
        at = sum(HEADS - b for b in range(c)) + i - c
        return pl.ds(at * TOK, count * TOK)

    shrink = 0.5 / math.sqrt(HEAD)
    def attend(i):
        q_nat = (turned(q_in[i]) * shrink).astype(BF)
        sums = jnp.zeros((HEAD, TOK), F32)
        for c in range(i + 1):
            s = nn(q_nat, pair(k_in, c))
            up = 1.0 + jnp.tanh(s)
            w = s * up
            slope = up + w * (2.0 - up)
            if c == i:
                ok = (iota((TOK, CHUNK), 1) + c * CHUNK) <= (
                    iota((TOK, CHUNK), 0) + block_of(i) * TOK
                )
                w = jnp.where(ok, w, 0.0)
                slope = jnp.where(ok, slope, 0.0)
            w = w.astype(BF)
            w_keep[kept(c, i, 1), :] = w
            slope_keep[kept(c, i, 1), :] = slope
            sums = sums + nt(pair(v_in, c), w)
        att_out[i] = sums.astype(BF)

    for group in ((7, 6, 5), (4, 3, 2, 1, 0)):
        for i in group:
            attend(i)
        for i in group:

            @pl.when(head != i)
            def _():
                remote(
                    att_out.at[i], att_in.at[rows64(head)], send.at[1], recv.at[5],
                    (dp, block_of(i)),
                ).start()

    att_in[rows64(head), :] = att_out[pl.ds(head, 1)].reshape(HEAD, TOK)
    wait_got(att_in.at[pl.ds(0, D - HEAD)], 5)

    mixed, inv_mix = column_norm(att_in[...].astype(F32))
    gate = active_t[0:D, :].astype(F32)
    dgated = dgated_t[...]
    da_out[...] = column_norm_back(dgated * gate, mixed, inv_mix).astype(BF)
    for d in range(1, HEADS):
        h, to = same_half(d)
        remote(da_out.at[rows64(h)], da_in.at[head], send.at[1], da_recv.at[head], to).start()
    da_in[pl.ds(head, 1)] = da_out[rows64(head), :].reshape(1, HEAD, TOK)

    sibling = (z * 2 + (1 - core), cp)
    place = (x, y, z)

    def along(dim, d):
        moved = [xs[0], ys[0], zs[0]]
        moved[dim] = (xs, ys, zs)[dim][d]
        return moved[dim], (moved[2] * 2 + core, moved[0] * 4 + moved[1])

    def ar(src, dst, n, stage, k, to):
        at = (0, 14, 28)[n]
        if stage in (1, 2, 3, 4):
            at += stage if n == 2 else 3 * stage - 2 + k
        elif stage == 6:
            at += 5 if n == 2 else 13
        return remote(src, dst, ar_send.at[n], ar_recv.at[at], to)

    def ar_got(ref, n, stage, k):
        ar(ref, ref, n, stage, k, (dp, cp)).wait_recv()

    def core_rows(n, c):
        return pl.ds(pl.multiple_of(SETS[n][0] + c * SETS[n][1], 16), SETS[n][3])

    def set_rows(n):
        return pl.ds(SETS[n][2], SETS[n][3])

    def stage0(n):
        ar(w_ref.at[core_rows(n, 1 - core)], r0.at[set_rows(n)], n, 0, 0, sibling).start()

    def piece(n, k):
        part, at = SETS[n][4][k]
        return pl.ds(at, part)

    def u1_rows(n, k, a):
        part = SETS[n][4][k][0]
        return pl.ds(pl.multiple_of(SETS[n][2] + first_row(n, k) + a * part, 16), part)

    def stage1(n):
        at = set_rows(n)
        ar_got(r0.at[at], n, 0, 0)
        u1[at, :] = (w_ref[core_rows(n, core), :].astype(F32) + r0[at, :].astype(F32)).astype(BF)
        for k in SETS[n][4]:
            for d in (2, 1, 3):
                a, to = along(k, d)
                ar(u1.at[u1_rows(n, k, a)], r1.at[d - 1, piece(n, k)], n, 1, k, to).start()

    def stage2(n, k):
        at = piece(n, k)
        ar_got(r1.at[:, at], n, 1, k)
        part = u1[u1_rows(n, k, place[k]), :].astype(F32)
        for d in range(3):
            part = part + r1[d, at, :].astype(F32)
        for b in range(4):
            u2[b, at, :] = part[:, b * 128 : (b + 1) * 128].astype(BF)
        for d in (2, 1, 3):
            b, to = along((k + 1) % 3, d)
            ar(u2.at[b, at], r2.at[d - 1, at], n, 2, k, to).start()

    def stage3(n, k):
        at = piece(n, k)
        ar_got(r2.at[:, at], n, 2, k)
        b_me, c_me = place[(k + 1) % 3], place[(k + 2) % 3]
        part = u2[pl.ds(b_me, 1), at, :].astype(F32)
        for d in range(3):
            part = part + r2[d : d + 1, at, :].astype(F32)
        r3[pl.ds(c_me, 1), at, :] = part.astype(BF)
        for d in (2, 1, 3):
            _, to = along((k + 2) % 3, d)
            ar(r3.at[c_me, at], r3.at[c_me, at], n, 3, k, to).start()

    def stage4(n, k):
        at = piece(n, k)
        ar_got(r3.at[pl.ds(0, 3), at], n, 3, k)
        b_me = place[(k + 1) % 3]
        part = r3[0:1, at, :].astype(F32)
        for d in range(1, 4):
            part = part + r3[d : d + 1, at, :].astype(F32)
        g2[pl.ds(b_me, 1), at, :] = part.astype(BF)
        for d in (2, 1, 3):
            _, to = along((k + 1) % 3, d)
            ar(g2.at[b_me, at], g2.at[b_me, at], n, 4, k, to).start()

    def to_sibling(n, k, a):
        held = total.at[core, a, :, piece(n, k)]
        ar(held, held, n, 6, k, sibling).start()

    def stage5(n, k):
        at = piece(n, k)
        ar_got(g2.at[pl.ds(0, 3), at], n, 4, k)
        a_me = place[k]
        for d in (2, 1, 3):
            _, to = along(k, d)
            remote(
                g2.at[:, at], total.at[core, a_me, :, at],
                ar_send.at[n], last_recv.at[n, d - 1], to,
            ).start()
        total[pl.ds(core, 1), pl.ds(a_me, 1), :, at, :] = g2[:, at, :].reshape(
            1, 1, 4, SETS[n][4][k][0], 128
        )
        to_sibling(n, k, a_me)

    def set_pieces(n):
        return pl.ds(min(at for _, at in SETS[n][4].values()), SETS[n][3] // 4)

    def stage6(n):
        for d in (1, 3, 2):
            held = total.at[0, 0, :, set_pieces(n)]
            remote(held, held, ar_send.at[n], last_recv.at[n, d - 1], (dp, cp)).wait_recv()
            for k in SETS[n][4]:
                to_sibling(n, k, along(k, 4 - d)[0])

    def stage7(n):
        ar_got(total.at[0, :, :, set_pieces(n)], n, 6, 0)

    def all_colors(stage, n):
        for k in SETS[n][4]:
            stage(n, k)

    def settle(n):
        kib = SETS[n][3] * 65 // 16
        sent = pick32.at[pl.ds(0, 2 * kib)] if n == 2 else slope_keep.at[pl.ds(0, kib)]
        remote(sent, sent, ar_send.at[n], ar_recv.at[0], (dp, cp)).wait_send()

    gated = (mixed * gate).astype(BF)
    low = normed_t[...].astype(BF)
    dh_gate = (dgated * mixed * silu_slope(hidden_t[0:D, :])).astype(BF)
    dh_t[0:D, :] = dh_gate
    w_ref[0:D, :] = nt(low, dh_gate).astype(BF)
    w_ref[D : 2 * D, :] = nn(gated, cot[...]).astype(BF)
    stage0(0)
    branch = nn(turned(gated).astype(BF), wout[...])
    layer_out[...] = (emb_nat[...] + branch).astype(BF)

    for i in range(HEADS):
        q_cat[:, i * TOK : (i + 1) * TOK] = q_in[i]
    for b in range(N_CP):
        kv_nat[b * TOK : (b + 1) * TOK, :] = turned(
            jnp.concatenate([k_in[b], v_in[b]], axis=0)
        ).astype(BF)

    def backward(c):
        da_nat[c * TOK : (c + 1) * TOK, :] = (turned(da_in[c]) * shrink).astype(BF)
        da_cat[:, c * TOK : (c + 1) * TOK] = da_in[c]
        rows = slice(c * TOK, HEADS * TOK)
        at = kept(c, c, HEADS - c)
        ds = (nn(da_nat[rows, :], pair(v_in, c)) * slope_keep[at, :]).astype(BF)
        dk = nn(q_cat[:, rows], ds).astype(BF)
        dv = nn(da_cat[:, rows], w_keep[at, :]).astype(BF)
        for b in range(2):
            dk_out[2 * c + b] = dk[:, b * TOK : (b + 1) * TOK]
            dv_out[2 * c + b] = dv[:, b * TOK : (b + 1) * TOK]
        dq = nn(ds, kv_nat[c * CHUNK : (c + 1) * CHUNK, :])
        if c < HEADS - 1:
            dq_acc[(c + 1) * TOK :, :] += dq[TOK:, :]
        dq_acc[c * TOK : (c + 1) * TOK, :] = dq[0:TOK, :]

    for group in ((7, 6, 5), (4, 3), (2, 1), (0,)):
        for c in group:

            @pl.when(head != c)
            def _():
                remote(
                    da_in.at[c], da_in.at[c], send.at[1], da_recv.at[c], (dp, cp)
                ).wait_recv()

        for c in group:
            backward(c)
        if group == (0,):
            for i in range(HEADS):
                dq_out[i] = dq_acc[i * TOK : (i + 1) * TOK, :].T[:HEAD, :].astype(BF)
        if group == (7, 6, 5):
            stage1(0)
        for kb in [2 * c + b for c in group for b in range(2)]:

            @pl.when(cp != kb)
            def _():
                remote(
                    dk_out.at[kb], dk_in.at[half, rows64(head)], send.at[1], recv.at[7], (dp, kb)
                ).start()
                remote(
                    dv_out.at[kb], dv_in.at[half, rows64(head)], send.at[1], recv.at[8], (dp, kb)
                ).start()

    for i in range(HEADS):

        @pl.when(head != i)
        def _():
            remote(
                dq_out.at[i], dq_in.at[rows64(head)], send.at[1], recv.at[9], (dp, block_of(i))
            ).start()

    all_colors(stage2, 0)

    dq_in[rows64(head), :] = dq_out[pl.ds(head, 1)].reshape(HEAD, TOK)
    dk_in[pl.ds(half, 1), rows64(head), :] = dk_out[pl.ds(cp, 1)]
    dv_in[pl.ds(half, 1), rows64(head), :] = dv_out[pl.ds(cp, 1)]
    wait_got(dk_out.at[pl.ds(0, N_CP - 1)], 7)
    wait_got(dv_out.at[pl.ds(0, N_CP - 1)], 8)
    wait_got(dq_in.at[pl.ds(0, D - HEAD)], 9)

    def column_back(b, grad):
        dh = (grad * silu_slope(hidden_t[b * D : (b + 1) * D, :])).astype(BF)
        dh_t[b * D : (b + 1) * D, :] = dh
        grads = nt(low, dh).astype(BF)
        if b == 1:
            w_ref[LATE : LATE + D, :] = grads
        elif b == 2:
            w_ref[LATE + D : LATE + 768, :] = grads[0:256]
            w_ref[LATE + 832 : LATE + 1088, :] = grads[256:512]
        else:
            w_ref[LATE + 1088 : LATE + 1600, :] = grads

    column_back(1, dv_in[0].astype(F32) + dv_in[1].astype(F32))
    column_back(2, dq_in[...].astype(F32))
    column_back(3, dk_in[0].astype(F32) + dk_in[1].astype(F32))
    stage0(1)
    dnormed = nn(joined[...], dh_t[...])
    dembed = column_norm_back(dnormed, normed_t[...], inv_ref[0:1, :]) + cot_t[...]
    exact = lax.Precision.HIGHEST
    all_colors(stage3, 0)
    stage1(1)
    proj_grads = nt(cold_t[...], dembed, exact).astype(BF)
    w_ref[LATE + 768 : LATE + 832, :] = proj_grads[0:64]
    w_ref[LATE + 1600 : LATE + 1664, :] = proj_grads[64:128]
    stage0(2)

    cold_event = lax.dot_general(
        proj[...].astype(F32), dembed, (((1,), (0,)), ((), ())),
        preferred_element_type=F32, precision=exact,
    )
    is_hot = slot_row < HOT
    for f in range(4):
        part = dembed[f * 128 : (f + 1) * 128, :]
        pack_ref[:, f * TOK : (f + 1) * TOK] = jnp.where(
            is_hot, part, cold_event if f == 0 else 0.0
        ).astype(BF)
    grad_out[...] = nt(slots_1h[...], pack_ref[...]).astype(BF)
    grad_in[tile(me), :] = grad_out[tile(me), :]

    def send_grads(group):
        for to in everyone[group::4]:
            remote(
                grad_out.at[tile(to[0] * N_CP + to[1])], grad_in.at[tile(me)],
                send.at[1], recv.at[10], to,
            ).start()

    stage1(2)
    all_colors(stage4, 0)
    send_grads(0)
    send_grads(1)
    all_colors(stage2, 1)
    all_colors(stage2, 2)
    all_colors(stage5, 0)
    all_colors(stage3, 1)
    all_colors(stage3, 2)
    send_grads(2)
    all_colors(stage4, 1)
    all_colors(stage4, 2)
    send_grads(3)
    all_colors(stage5, 1)
    all_colors(stage5, 2)
    stage6(0)
    stage6(1)
    stage6(2)

    wait_got(grad_in.at[pl.ds(0, SLOTS - SLOT)], 10)
    by_rank(grad_in, rows_got)

    hot_sum[...] = nn(named[0:HOT, :], rows_got[...])
    cold_sum[...] = nn(named[HOT:, :], rows_got[:, 0:COLD_W])

    sent = ids_all.at[pl.ds(0, DEVICES - 1)]
    remote(sent, sent, send.at[0], recv.at[0], (dp, cp)).wait_send()
    sent = slope_keep.at[pl.ds(0, SENT_KIB)]
    remote(sent, sent, send.at[1], recv.at[0], (dp, cp)).wait_send()
    settle(0)
    for n in range(3):
        stage7(n)
    settle(1)
    settle(2)


def finish_kernel(
    layer, hot_sum, cold_sum, sums,
    layer_out, hot_out, cold_out, proj_out, joined_out, wout_out,
    sum_buf, sem,
):
    copies = []

    def put(src, dst):
        copy = pltpu.make_async_copy(src, dst, sem.at[len(copies)])
        copy.start()
        copies.append(copy)

    put(layer, layer_out)
    put(hot_sum, hot_out)
    put(cold_sum, cold_out)
    scale = (TOK * DEVICES) ** -0.5

    def scaled(n, core):
        home = (4 * D * core, D + 768 * core, 5 * D + 64 * core)[n]
        for k, (count, at) in SETS[n][4].items():
            for a in range(4):
                top = home + first_row(n, k) + a * count
                for b in range(4):
                    sum_buf[top : top + count, b * 128 : (b + 1) * 128] = (
                        sums[core, a, b, at : at + count, :].astype(F32) * scale
                    )

    def put_joined(b):
        put(sum_buf.at[pl.ds(b * D, D)], joined_out.at[:, pl.ds(b * D, D)])

    scaled(0, 0)
    put_joined(0)
    scaled(1, 0)
    put_joined(1)
    scaled(1, 1)
    put_joined(2)
    put_joined(3)
    scaled(0, 1)
    put(sum_buf.at[pl.ds(4 * D, D)], wout_out)
    scaled(2, 0)
    scaled(2, 1)
    put(sum_buf.at[pl.ds(5 * D, COLD_W)], proj_out)
    for copy in copies:
        copy.wait()


def vmem(n):
    return [pl.BlockSpec(memory_space=pltpu.VMEM)] * n


def anywhere(n):
    return [pl.BlockSpec(memory_space=pl.ANY)] * n


def hbm(n):
    return [pl.BlockSpec(memory_space=pltpu.HBM)] * n


def local(row_owner, slot_row, hot, cold, proj, joined, wout, cot):
    v = pltpu.VMEM
    operands = [row_owner.reshape(1, TOK), slot_row.reshape(1, TOK)]
    operands += [hot, cold, proj, joined, wout, cot]
    operands = [pltpu.with_memory_space_constraint(a, pltpu.HBM) for a in operands]
    layer, hot_sum, cold_sum, sums = pl.pallas_call(
        step_kernel,
        out_shape=(
            jax.ShapeDtypeStruct((TOK, D), BF),
            jax.ShapeDtypeStruct((HOT, D), F32),
            jax.ShapeDtypeStruct((COLD, COLD_W), F32),
            jax.ShapeDtypeStruct((2, 4, 4, PART_ROWS, 128), BF),
        ),
        in_specs=hbm(8),
        out_specs=tuple(vmem(4)),
        scratch_shapes=[
            v((HOT, D), BF), v((COLD, COLD_W), BF), v((HOT, 4 * COLD_W), BF),
            v((COLD_W, D), BF), v((D, 4 * D), BF),
            v((D, D), BF), v((TOK, D), BF), v((1, TOK), I32), v((1, TOK), I32),
            v((1, TOK), I32),
            v((DEVICES, 1, TOK), I32), v((SLOTS, 128), F32), v((SLOTS, 128), BF),
            v((SLOTS, 128), BF), v((TOK, CAP * DEVICES), BF), v((CAP * DEVICES, D), BF),
            v((TOK, D), F32), v((D, TOK), F32), v((8, TOK), F32),
            v((COLD_W, TOK), F32), v((4 * D, D), BF),
            v((4 * D, TOK), F32), v((4 * D, TOK), BF), v((D, TOK), F32), v((D, TOK), F32),
            v((SLOTS, 4 * TOK), BF),
            v((N_CP, HEAD, TOK), BF), v((N_CP, HEAD, TOK), BF), v((HEADS, HEAD, TOK), BF),
            v((N_CP * TOK, 2 * HEAD), BF),
            v((PAIRS * TOK, CHUNK), BF), v((PAIRS * TOK, CHUNK), F32),
            v((HEADS, HEAD, TOK), BF), v((D, TOK), BF), v((D, TOK), BF),
            v((HEADS, HEAD, TOK), BF),
            v((HEADS * TOK, HEAD), BF), v((HEAD, HEADS * TOK), BF), v((HEAD, HEADS * TOK), BF),
            v((HEADS * TOK, 2 * HEAD), F32),
            v((HEADS, HEAD, TOK), BF),
            v((N_CP, HEAD, TOK), BF), v((N_CP, HEAD, TOK), BF),
            v((D, TOK), BF), v((2, D, TOK), BF), v((2, D, TOK), BF),
            v((4 * D, TOK), BF), v((128, 4 * TOK), BF),
            v((SLOTS, 128), BF), v((SLOTS, 128), BF), v((HOT + COLD, CAP * DEVICES), BF),
            v((W_ROWS, D), BF), v((W_ROWS // 2, D), BF), v((W_ROWS // 2, D), BF),
            v((3, PART_ROWS, D), BF), v((4, PART_ROWS, 128), BF),
            v((3, PART_ROWS, 128), BF), v((4, PART_ROWS, 128), BF),
            v((4, PART_ROWS, 128), BF),
            pltpu.SemaphoreType.DMA((2,)), pltpu.SemaphoreType.DMA((11,)),
            pltpu.SemaphoreType.DMA((HEADS,)),
            pltpu.SemaphoreType.DMA((3,)), pltpu.SemaphoreType.DMA((34,)),
            pltpu.SemaphoreType.DMA((3, 3)),
            pltpu.SemaphoreType.DMA((8,)),
        ],
        compiler_params=pltpu.CompilerParams(
            collective_id=0, has_side_effects=True, vmem_limit_bytes=44 << 20
        ),
        name="step",
    )(*operands)
    return pl.pallas_call(
        finish_kernel,
        out_shape=(
            jax.ShapeDtypeStruct((TOK, D), BF),
            jax.ShapeDtypeStruct((HOT, D), F32),
            jax.ShapeDtypeStruct((COLD, COLD_W), F32),
            jax.ShapeDtypeStruct((COLD_W, D), F32),
            jax.ShapeDtypeStruct((D, 4 * D), F32),
            jax.ShapeDtypeStruct((D, D), F32),
        ),
        in_specs=vmem(4),
        out_specs=tuple(hbm(6)),
        scratch_shapes=[
            v((W_ROWS, D), F32),
            pltpu.SemaphoreType.DMA((9,)),
        ],
        compiler_params=pltpu.CompilerParams(vmem_limit_bytes=20 << 20),
        name="finish",
    )(layer, hot_sum, cold_sum, sums)


def solution(mesh):
    rows = P(("dp", "cp"), None)
    return jax.shard_map(
        local,
        mesh=mesh,
        in_specs=(rows, P(("dp", "cp")), rows, rows, P(), P(), P(), rows),
        out_specs=(rows, rows, rows, P(), P(), P()),
        check_vma=False,
    )
```
